128 devices in a mesh: dp: 1, cpo: 2 (over core), cp: 64 (over z, y, x).
Axes of the slice: x: 4, y: 4, z: 4, core: 2. Of those that a mesh axis runs over, the one named last changes fastest.
Arguments:
- queries: bfloat16 [65536, 2, 128], P(('dp', 'cpo', 'cp'))
- keys: bfloat16 [65536, 128], P(('dp', 'cpo', 'cp'))
- values: bfloat16 [65536, 128], P(('dp', 'cpo', 'cp'))
- attn_out: bfloat16 [65536, 2, 128], P(('dp', 'cpo', 'cp'))
- logsumexp: float32 [65536, 2], P(('dp', 'cpo', 'cp'))
- d_out: bfloat16 [65536, 2, 128], P(('dp', 'cpo', 'cp'))
- cu_seqlens: int32 [174], P('dp')
Outputs:
- output 1: bfloat16 [65536, 2, 128], P(('dp', 'cpo', 'cp'))
- output 2: bfloat16 [65536, 128], P(('dp', 'cpo', 'cp'))
- output 3: bfloat16 [65536, 128], P(('dp', 'cpo', 'cp'))
All inputs are finite; a program needn't handle non-finite values.
Results may differ from the reference program's by a relative error of at most 0.00131.
Values are sent between devices in bfloat16 or wider.
A program may use at most 1 GiB of HBM per device.

```python
import jax
import jax.numpy as jnp
from jax import lax

CHUNK = 512
GROUP = 128
QHEADS = 2
HEAD_DIM = 128
HOPS = 3
QROWS = 64
SEQ = GROUP * CHUNK
NCUT_RAND = GROUP
NCUT_GRID = GROUP // 3 + 2


def doc_ids(bounds, positions):
    found = jnp.searchsorted(bounds[1:], positions, side="right").astype(jnp.int32)
    return jnp.where((positions >= 0) & (positions < SEQ), found, -1)


def draw_bounds(key):
    key_phase, key_slot, key_cuts = jax.random.split(key, 3)
    span_len = HOPS * CHUNK
    phase = jax.random.randint(key_phase, (), 0, span_len, dtype=jnp.int32)
    grid_cuts = jnp.minimum(phase + span_len * jnp.arange(NCUT_GRID, dtype=jnp.int32), SEQ)
    slot_count = (SEQ - phase) // span_len
    slot = jax.random.randint(key_slot, (), 0, slot_count, dtype=jnp.int32)
    long_start = phase + span_len * slot
    free_cuts = jax.random.randint(key_cuts, (NCUT_RAND,), 1, SEQ, dtype=jnp.int32)
    inside = (free_cuts > long_start) & (free_cuts < long_start + span_len)
    free_cuts = jnp.where(inside, 0, free_cuts)
    every_cut = jnp.concatenate([jnp.zeros((1,), jnp.int32), grid_cuts, free_cuts, jnp.full((1,), SEQ, jnp.int32)])
    return jnp.sort(every_cut).astype(jnp.int32)


def attend_forward(queries, keys, values, ids):
    scale = HEAD_DIM ** -0.5
    span_len = HOPS * CHUNK
    width = span_len + QROWS
    key_pad = jnp.concatenate([jnp.zeros((span_len, HEAD_DIM), jnp.float32), keys.astype(jnp.float32)])
    val_pad = jnp.concatenate([jnp.zeros((span_len, HEAD_DIM), jnp.float32), values.astype(jnp.float32)])
    id_pad = jnp.concatenate([jnp.full((span_len,), -1, jnp.int32), ids])

    def block_fwd(start):
        q_blk = lax.dynamic_slice_in_dim(queries, start, QROWS).astype(jnp.float32)
        id_q = lax.dynamic_slice_in_dim(ids, start, QROWS)
        pos_q = start + jnp.arange(QROWS, dtype=jnp.int32)
        k_blk = lax.dynamic_slice_in_dim(key_pad, start, width)
        v_blk = lax.dynamic_slice_in_dim(val_pad, start, width)
        id_k = lax.dynamic_slice_in_dim(id_pad, start, width)
        pos_k = start - span_len + jnp.arange(width, dtype=jnp.int32)
        keep = (id_q[:, None] == id_k[None, :]) & (pos_k[None, :] <= pos_q[:, None])
        scores = scale * jnp.einsum("qgd,kd->qgk", q_blk, k_blk)
        scores = jnp.where(keep[:, None, :], scores, -1e30)
        top_val = jnp.max(scores, axis=-1, keepdims=True)
        exp_scores = jnp.where(keep[:, None, :], jnp.exp(scores - top_val), 0.0)
        denom = jnp.sum(exp_scores, axis=-1, keepdims=True)
        out_blk = jnp.einsum("qgk,kd->qgd", exp_scores, v_blk) / denom
        return out_blk.astype(jnp.bfloat16), (top_val + jnp.log(denom))[:, :, 0]

    starts = jnp.arange(SEQ // QROWS, dtype=jnp.int32) * QROWS
    out_all, lse_all = lax.map(block_fwd, starts)
    return out_all.reshape(SEQ, QHEADS, HEAD_DIM), lse_all.reshape(SEQ, QHEADS)


def setup_inputs(seed: int = 0, part: int = 0) -> dict:
    part_key = jax.random.fold_in(jax.random.key(seed), part)
    key_q, key_k, key_v, key_do, key_b = jax.random.split(part_key, 5)
    queries = jax.random.normal(key_q, (SEQ, QHEADS, HEAD_DIM), jnp.float32).astype(jnp.bfloat16)
    keys = jax.random.normal(key_k, (SEQ, HEAD_DIM), jnp.float32).astype(jnp.bfloat16)
    values = jax.random.normal(key_v, (SEQ, HEAD_DIM), jnp.float32).astype(jnp.bfloat16)
    d_out = jax.random.normal(key_do, (SEQ, QHEADS, HEAD_DIM), jnp.float32).astype(jnp.bfloat16)
    cu_seqlens = draw_bounds(key_b)
    ids = doc_ids(cu_seqlens, jnp.arange(SEQ, dtype=jnp.int32))
    attn_out, logsumexp = attend_forward(queries, keys, values, ids)
    return {"queries": queries, "keys": keys, "values": values, "attn_out": attn_out, "logsumexp": logsumexp, "d_out": d_out, "cu_seqlens": cu_seqlens}


def reference(queries, keys, values, attn_out, logsumexp, d_out, cu_seqlens):
    scale = HEAD_DIM ** -0.5
    span_len = HOPS * CHUNK
    width = span_len + QROWS
    ids = doc_ids(cu_seqlens, jnp.arange(SEQ, dtype=jnp.int32))
    id_pad = jnp.concatenate([jnp.full((span_len,), -1, jnp.int32), ids])
    key_pad = jnp.concatenate([jnp.zeros((span_len, HEAD_DIM), keys.dtype), keys])
    val_pad = jnp.concatenate([jnp.zeros((span_len, HEAD_DIM), values.dtype), values])
    row_dot = jnp.sum(d_out.astype(jnp.float32) * attn_out.astype(jnp.float32), axis=-1)

    def block_bwd(carry, start):
        dk_acc, dv_acc = carry
        q_blk = lax.dynamic_slice_in_dim(queries, start, QROWS).astype(jnp.float32)
        do_blk = lax.dynamic_slice_in_dim(d_out, start, QROWS).astype(jnp.float32)
        lse_blk = lax.dynamic_slice_in_dim(logsumexp, start, QROWS)
        dot_blk = lax.dynamic_slice_in_dim(row_dot, start, QROWS)
        id_q = lax.dynamic_slice_in_dim(ids, start, QROWS)
        pos_q = start + jnp.arange(QROWS, dtype=jnp.int32)
        k_blk = lax.dynamic_slice_in_dim(key_pad, start, width).astype(jnp.float32)
        v_blk = lax.dynamic_slice_in_dim(val_pad, start, width).astype(jnp.float32)
        id_k = lax.dynamic_slice_in_dim(id_pad, start, width)
        pos_k = start - span_len + jnp.arange(width, dtype=jnp.int32)
        keep = (id_q[:, None] == id_k[None, :]) & (pos_k[None, :] <= pos_q[:, None])
        scores = scale * jnp.einsum("qgd,kd->qgk", q_blk, k_blk)
        p_mat = jnp.where(keep[:, None, :], jnp.exp(scores - lse_blk[:, :, None]), 0.0)
        p_low = p_mat.astype(jnp.bfloat16).astype(jnp.float32)
        dp_mat = jnp.einsum("qgd,kd->qgk", do_blk, v_blk)
        ds_mat = (p_mat * (dp_mat - dot_blk[:, :, None])).astype(jnp.bfloat16).astype(jnp.float32)
        dq_blk = scale * jnp.einsum("qgk,kd->qgd", ds_mat, k_blk)
        dk_part = jnp.einsum("qgk,qgd->kd", ds_mat, q_blk)
        dv_part = jnp.einsum("qgk,qgd->kd", p_low, do_blk)
        dk_acc = lax.dynamic_update_slice_in_dim(dk_acc, lax.dynamic_slice_in_dim(dk_acc, start, width) + dk_part, start, axis=0)
        dv_acc = lax.dynamic_update_slice_in_dim(dv_acc, lax.dynamic_slice_in_dim(dv_acc, start, width) + dv_part, start, axis=0)
        return (dk_acc, dv_acc), dq_blk.astype(jnp.bfloat16)

    init = (jnp.zeros((SEQ + span_len, HEAD_DIM), jnp.float32), jnp.zeros((SEQ + span_len, HEAD_DIM), jnp.float32))
    starts = jnp.arange(SEQ // QROWS, dtype=jnp.int32) * QROWS
    (dk_acc, dv_acc), dq_all = lax.scan(block_bwd, init, starts)
    d_queries = dq_all.reshape(SEQ, QHEADS, HEAD_DIM)
    d_keys = (scale * dk_acc[span_len:]).astype(jnp.bfloat16)
    d_values = dv_acc[span_len:].astype(jnp.bfloat16)
    return d_queries, d_keys, d_values
```

```python
import functools
import math

import jax
import jax.numpy as jnp
from jax import lax
from jax.experimental import pallas as pl
from jax.experimental.pallas import tpu as pltpu
from jax.sharding import PartitionSpec as P

MESH = pl.DeviceIdType.MESH
HOPS = 3
CHUNKS = 4
LOG2E = math.log2(math.e)
NT = (((1,), (1,)), ((), ()))
NN = (((1,), (0,)), ((), ()))


def dot(lhs, rhs, dims):
    return lax.dot_general(lhs, rhs, dims, preferred_element_type=jnp.float32)


def backward_kernel(sizes, q_hbm, k_hbm, v_hbm, o_hbm, do_hbm, lse_ref, cu_ref, dq_hbm, dk_hbm, dv_hbm,
                    kv_own, kv_in, qd_own, qd_in, o_buf, ld_own, ld_in, starts, key_t, dq_t, dk_acc, dv_acc,
                    dq_buf, dk_buf, dv_buf, load_sem, store_sem,
                    kv_send, kv_recv, qd_send, qd_recv, ld_send, ld_recv):
    outer, inner, rows, heads, head = sizes
    group = outer * inner
    scale = head ** -0.5
    span = rows // CHUNKS
    lanes = span * heads
    bounds = cu_ref.shape[1]
    rank = lax.axis_index("cpo") * inner + lax.axis_index("cp")

    def device(index):
        return (0, index // inner, index % inner)

    right = device((rank + 1) % group)
    left = device((rank + group - 1) % group)

    loads = [
        pltpu.make_async_copy(k_hbm, kv_own.at[0], load_sem.at[0]),
        pltpu.make_async_copy(v_hbm, kv_own.at[1], load_sem.at[1]),
        pltpu.make_async_copy(q_hbm, qd_own.at[0], load_sem.at[2]),
        pltpu.make_async_copy(do_hbm, qd_own.at[1], load_sem.at[3]),
        pltpu.make_async_copy(o_hbm, o_buf, load_sem.at[4]),
    ]
    for load in loads:
        load.start()

    barrier = pltpu.get_barrier_semaphore()
    for peer in (left, right):
        pl.semaphore_signal(barrier, inc=1, device_id=peer, device_id_type=MESH)
    pl.semaphore_wait(barrier, 2)

    def kv_copy(hop, chunk):
        source = kv_own if hop == 0 else kv_in.at[hop - 1]
        part = pl.ds(chunk * span, span)
        return pltpu.make_async_remote_copy(
            src_ref=source.at[:, part], dst_ref=kv_in.at[hop, :, part],
            send_sem=kv_send.at[hop, chunk], recv_sem=kv_recv.at[hop, chunk],
            device_id=right, device_id_type=MESH)

    def qd_copy(hop, chunk):
        source = qd_own if hop == 0 else qd_in.at[hop - 1]
        part = pl.ds(chunk * lanes, lanes)
        return pltpu.make_async_remote_copy(
            src_ref=source.at[:, part], dst_ref=qd_in.at[hop, :, part],
            send_sem=qd_send.at[hop, chunk], recv_sem=qd_recv.at[hop, chunk],
            device_id=left, device_id_type=MESH)

    def ld_copy(hop):
        source = ld_own if hop == 0 else ld_in.at[hop - 1]
        return pltpu.make_async_remote_copy(
            src_ref=source, dst_ref=ld_in.at[hop],
            send_sem=ld_send.at[hop], recv_sem=ld_recv.at[hop],
            device_id=left, device_id_type=MESH)

    loads[0].wait()
    loads[1].wait()
    for chunk in range(CHUNKS):
        kv_copy(0, chunk).start()
    loads[2].wait()
    loads[3].wait()
    for chunk in range(CHUNKS):
        qd_copy(0, chunk).start()
    loads[4].wait()

    ld_own[0:1, :] = lse_ref[...] * LOG2E
    for part in range(rows * heads // head):
        piece = slice(part * head, (part + 1) * head)
        prod = qd_own[1, piece, :].astype(jnp.float32) * o_buf[piece, :].astype(jnp.float32)
        ld_own[1:2, piece] = jnp.sum(prod.T, axis=0, keepdims=True)

    first = (rank * rows).astype(jnp.float32)
    cuts = cu_ref[...].astype(jnp.float32)
    padded = -(-bounds // head) * head
    cut_cols = []
    for base in range(0, padded, head):
        width = min(head, bounds - base)
        row = cuts[:, base:base + width]
        if width < head:
            row = jnp.concatenate([row, jnp.zeros((1, head - width), jnp.float32)], axis=1)
        cut_cols.append(jnp.broadcast_to(row, (head, head)).T - first)
    lane = lax.broadcasted_iota(jnp.int32, (1, head), 1)

    def fill_starts(step, _):
        lane_base = pl.multiple_of((step % (rows * heads // head)) * head, head)
        hop = step // (rows * heads // head)
        token = ((lane + lane_base) // heads + hop * rows).astype(jnp.float32)
        best = jnp.full((head, head), -1e9, jnp.float32)
        for col in cut_cols:
            best = jnp.maximum(best, jnp.where(col <= token, col, -1e9))
        starts[hop, :, pl.ds(lane_base, head)] = jnp.max(best, axis=0, keepdims=True)
        return 0

    lax.fori_loop(0, (HOPS + 1) * rows * heads // head, fill_starts, 0)

    dk_acc[...] = jnp.zeros_like(dk_acc)
    dv_acc[...] = jnp.zeros_like(dv_acc)
    dq_t[...] = jnp.zeros_like(dq_t)

    def tile(kv, k_from, k_to, qd, ld, chunk, key_shift, start_slot, q_side, k_side):
        part = slice(chunk * lanes, (chunk + 1) * lanes)
        key_rows = slice(k_from, k_to)
        keys, vals = kv[0, key_rows, :], kv[1, key_rows, :]
        qry, dout = qd[0, part, :], qd[1, part, :]
        score = dot(keys, qry, NT)
        grad = dot(vals, dout, NT)
        lse, row_dot = ld[0:1, part], ld[1:2, part]
        start = starts[start_slot, :, part]
        key_pos = lax.broadcasted_iota(jnp.int32, (k_to - k_from, lanes), 0).astype(jnp.float32)
        keep = key_pos >= start - float(key_shift * rows + k_from)
        if q_side and k_side:
            token = lax.broadcasted_iota(jnp.int32, (1, lanes), 1) // heads + (chunk * span - k_from)
            keep = keep & (key_pos <= token.astype(jnp.float32))
        prob = jnp.where(keep, jnp.exp2(score * (scale * LOG2E) - lse), 0.0)
        dsc = (prob * (grad - row_dot)).astype(jnp.bfloat16)
        if k_side:
            dv_acc[key_rows, :] += dot(prob.astype(jnp.bfloat16), dout, NN)
            dk_acc[key_rows, :] += dot(dsc, qry, NN)
        if q_side:
            dq_t[:, part] += dot(key_t[:, key_rows], dsc, NN)

    key_t[...] = kv_own[0].T
    for chunk in range(CHUNKS):
        tile(kv_own, 0, (chunk + 1) * span, qd_own, ld_own, chunk, 0, 0, True, True)
    ld_copy(0).start()

    def keys_ready(hop):
        key_t[...] = kv_in[hop - 1, 0].T
        for chunk in range(CHUNKS):
            k_from = chunk * span if hop == HOPS else 0
            tile(kv_in.at[hop - 1], k_from, rows, qd_own, ld_own, chunk, -hop, 0, True, False)

    for step in range(HOPS * CHUNKS):
        for index in (2 * step, 2 * step + 1):
            if index < HOPS * CHUNKS:
                hop, chunk = index // CHUNKS, index % CHUNKS
                kv_copy(hop, chunk).wait_recv()
                if hop + 1 < HOPS:
                    kv_copy(hop + 1, chunk).start()
        hop, chunk = step // CHUNKS, step % CHUNKS
        if chunk == 0:
            ld_copy(hop).wait_recv()
            if hop + 1 < HOPS:
                ld_copy(hop + 1).start()
        qd_copy(hop, chunk).wait_recv()
        if hop + 1 < HOPS:
            qd_copy(hop + 1, chunk).start()
        k_from = chunk * span if hop + 1 == HOPS else 0
        tile(kv_own, k_from, rows, qd_in.at[hop], ld_in.at[hop], chunk, 0, hop + 1, False, True)
        if step % 2 == 1 and step // 2 < HOPS:
            keys_ready(step // 2 + 1)
        if step == 2 * HOPS - 1:
            for part in range(rows * heads // head):
                piece = slice(part * head, (part + 1) * head)
                dq_buf[piece, :] = (scale * dq_t[:, piece].T).astype(jnp.bfloat16)
            pltpu.make_async_copy(dq_buf, dq_hbm, store_sem.at[0]).start()

    dk_buf[...] = (scale * dk_acc[...]).astype(jnp.bfloat16)
    dv_buf[...] = dv_acc[...].astype(jnp.bfloat16)
    pltpu.make_async_copy(dk_buf, dk_hbm, store_sem.at[1]).start()
    pltpu.make_async_copy(dv_buf, dv_hbm, store_sem.at[2]).start()
    for hop in range(HOPS):
        for chunk in range(CHUNKS):
            kv_copy(hop, chunk).wait_send()
            qd_copy(hop, chunk).wait_send()
        ld_copy(hop).wait_send()
    pltpu.make_async_copy(dq_buf, dq_hbm, store_sem.at[0]).wait()
    pltpu.make_async_copy(dk_buf, dk_hbm, store_sem.at[1]).wait()
    pltpu.make_async_copy(dv_buf, dv_hbm, store_sem.at[2]).wait()


def solution(mesh):
    outer, inner = mesh.shape["cpo"], mesh.shape["cp"]

    def local(queries, keys, values, attn_out, logsumexp, d_out, cu_seqlens):
        rows, heads, head = queries.shape
        flat = rows * heads
        low, full = jnp.bfloat16, jnp.float32
        any_spec = pl.BlockSpec(memory_space=pl.ANY)
        vmem_spec = pl.BlockSpec(memory_space=pltpu.VMEM)
        dma = pltpu.SemaphoreType.DMA
        d_query, d_key, d_value = pl.pallas_call(
            functools.partial(backward_kernel, (outer, inner, rows, heads, head)),
            out_shape=(jax.ShapeDtypeStruct((flat, head), low), jax.ShapeDtypeStruct((rows, head), low), jax.ShapeDtypeStruct((rows, head), low)),
            in_specs=[any_spec] * 5 + [vmem_spec] * 2,
            out_specs=(any_spec,) * 3,
            scratch_shapes=[
                pltpu.VMEM((2, rows, head), low), pltpu.VMEM((HOPS, 2, rows, head), low),
                pltpu.VMEM((2, flat, head), low), pltpu.VMEM((HOPS, 2, flat, head), low),
                pltpu.VMEM((flat, head), low),
                pltpu.VMEM((2, flat), full), pltpu.VMEM((HOPS, 2, flat), full),
                pltpu.VMEM((HOPS + 1, 1, flat), full),
                pltpu.VMEM((head, rows), low), pltpu.VMEM((head, flat), full),
                pltpu.VMEM((rows, head), full), pltpu.VMEM((rows, head), full),
                pltpu.VMEM((flat, head), low), pltpu.VMEM((rows, head), low), pltpu.VMEM((rows, head), low),
                dma((5,)), dma((3,)),
                dma((HOPS, CHUNKS)), dma((HOPS, CHUNKS)), dma((HOPS, CHUNKS)), dma((HOPS, CHUNKS)), dma((HOPS,)), dma((HOPS,)),
            ],
            compiler_params=pltpu.CompilerParams(collective_id=0, has_side_effects=True),
        )(queries.reshape(flat, head), keys, values, attn_out.reshape(flat, head), d_out.reshape(flat, head),
          logsumexp.reshape(1, flat), cu_seqlens.reshape(1, -1))
        return d_query.reshape(rows, heads, head), d_key, d_value

    seq_spec = P(("dp", "cpo", "cp"))
    return jax.shard_map(local, mesh=mesh, in_specs=(seq_spec,) * 6 + (P("dp"),), out_specs=(seq_spec,) * 3, check_vma=False)
```

```python
import functools
import math

import jax
import jax.numpy as jnp
from jax import lax
from jax.experimental import pallas as pl
from jax.experimental.pallas import tpu as pltpu
from jax.sharding import PartitionSpec as P

MESH = pl.DeviceIdType.MESH
HOPS = 3
CHUNKS = 4
FAR = (1, 2, 3)
VIA = 2
LOG2E = math.log2(math.e)
NT = (((1,), (1,)), ((), ()))
NN = (((1,), (0,)), ((), ()))


def dot(lhs, rhs, dims):
    return lax.dot_general(lhs, rhs, dims, preferred_element_type=jnp.float32)


def backward_kernel(sizes, q_hbm, k_hbm, v_hbm, o_hbm, do_hbm, lse_hbm, cu_hbm, dq_out, dk_out, dv_out,
                    kv_own, kv_in, qd_own, qd_in, qd_via, o_buf, ld_own, ld_in, lse_buf, cu_buf, starts, key_t, dq_t, dk_acc, dv_acc,
                    load_sem, kv_send, kv_recv, qd_send, qd_recv, far_send, far_recv, via_recv, ld_send, ld_recv):
    outer, inner, rows, heads, head, ring = sizes
    group = outer * inner
    scale = head ** -0.5
    span = rows // CHUNKS
    lanes = span * heads
    flat = rows * heads
    bounds = cu_buf.shape[1]
    rank = lax.axis_index("cpo") * inner + lax.axis_index("cp")
    column = rank % ring

    def device(index):
        return (0, index // inner, index % inner)

    loads = [
        pltpu.make_async_copy(k_hbm, kv_own.at[0], load_sem.at[0]),
        pltpu.make_async_copy(v_hbm, kv_own.at[1], load_sem.at[1]),
        pltpu.make_async_copy(q_hbm, qd_own.at[0], load_sem.at[2]),
        pltpu.make_async_copy(do_hbm, qd_own.at[1], load_sem.at[3]),
        pltpu.make_async_copy(o_hbm, o_buf, load_sem.at[4]),
        pltpu.make_async_copy(lse_hbm, lse_buf, load_sem.at[5]),
        pltpu.make_async_copy(cu_hbm, cu_buf, load_sem.at[6]),
    ]
    for load in loads:
        load.start()

    barrier = pltpu.get_barrier_semaphore()
    arrivals = 0
    for step in (-4, -3, -1, 1, 3, 4):
        peer = rank + step
        known = (peer >= 0) & (peer < group)

        @pl.when(known)
        def _():
            pl.semaphore_signal(barrier, inc=1, device_id=device(peer), device_id_type=MESH)

        arrivals = arrivals + jnp.where(known, 1, 0)
    pl.semaphore_wait(barrier, arrivals)

    def kv_copy(hop, chunk):
        source = kv_own if hop == 0 else kv_in.at[hop - 1]
        part = pl.ds(chunk * span, span)
        return pltpu.make_async_remote_copy(
            src_ref=source.at[:, part], dst_ref=kv_in.at[hop, :, part],
            send_sem=kv_send.at[hop, chunk], recv_sem=kv_recv.at[hop, chunk],
            device_id=device(rank + 1), device_id_type=MESH)

    def qd_copy(hop, chunk):
        source = qd_own if hop == 0 else qd_in.at[hop - 1]
        part = pl.ds(chunk * lanes, lanes)
        return pltpu.make_async_remote_copy(
            src_ref=source.at[:, part], dst_ref=qd_in.at[hop, :, part],
            send_sem=qd_send.at[hop, chunk], recv_sem=qd_recv.at[hop, chunk],
            device_id=device(rank - 1), device_id_type=MESH)

    def ld_copy(hop):
        source = ld_own if hop == 0 else ld_in.at[hop - 1]
        return pltpu.make_async_remote_copy(
            src_ref=source, dst_ref=ld_in.at[hop],
            send_sem=ld_send.at[hop], recv_sem=ld_recv.at[hop],
            device_id=device(rank - 1), device_id_type=MESH)

    def far_copy(chunk):
        part = pl.ds(chunk * lanes, lanes)
        return pltpu.make_async_remote_copy(
            src_ref=qd_own.at[:, part], dst_ref=qd_in.at[HOPS - 1, :, part],
            send_sem=far_send.at[chunk], recv_sem=far_recv.at[chunk],
            device_id=device(rank - 3), device_id_type=MESH)

    def via_copy(chunk):
        part = pl.ds(chunk * lanes, lanes)
        return pltpu.make_async_remote_copy(
            src_ref=qd_own.at[:, part], dst_ref=qd_via.at[:, part],
            send_sem=far_send.at[chunk], recv_sem=via_recv.at[chunk],
            device_id=device(rank - 4), device_id_type=MESH)

    def pass_copy(chunk):
        part = pl.ds(chunk * lanes, lanes)
        return pltpu.make_async_remote_copy(
            src_ref=qd_via.at[:, part], dst_ref=qd_in.at[HOPS - 1, :, part],
            send_sem=qd_send.at[HOPS - 1, chunk], recv_sem=far_recv.at[chunk],
            device_id=device(rank + 1), device_id_type=MESH)

    sends_kv = [(rank >= hop) & (rank + 1 < group) for hop in range(HOPS)]
    gets_kv = [rank >= hop + 1 for hop in range(HOPS)]
    sends_qd = [(rank >= 1) & (rank + hop < group) for hop in range(HOPS)]
    gets_qd = [rank + hop + 1 < group for hop in range(HOPS)]
    is_via = column == VIA
    sends_far = (rank >= HOPS) & ~is_via
    sends_via = (rank >= HOPS + 1) & is_via
    passes = is_via & (rank + HOPS + 1 < group)

    loads[0].wait()
    loads[1].wait()

    @pl.when(sends_kv[0])
    def _():
        for chunk in range(CHUNKS):
            kv_copy(0, chunk).start()

    loads[2].wait()
    loads[3].wait()

    @pl.when(sends_qd[0])
    def _():
        qd_copy(0, 0).start()

    @pl.when(sends_via)
    def _():
        for chunk in FAR:
            via_copy(chunk).start()

    loads[4].wait()
    loads[5].wait()
    loads[6].wait()

    row_id = lax.broadcasted_iota(jnp.int32, (head, heads * head), 0)
    lane_id = lax.broadcasted_iota(jnp.int32, (head, heads * head), 1)
    for part in range(rows // head):
        piece = slice(part * head, (part + 1) * head)
        wide = jnp.zeros((head, heads * head), jnp.float32)
        for g in range(heads):
            column_g = jnp.broadcast_to(lse_buf[g:g + 1, piece], (head, head)).T
            wide = jnp.where(lane_id == row_id * heads + g, jnp.concatenate([column_g] * heads, axis=1), wide)
        ld_own[0:1, part * heads * head:(part + 1) * heads * head] = jnp.sum(wide, axis=0, keepdims=True) * LOG2E
    for part in range(flat // head):
        piece = slice(part * head, (part + 1) * head)
        prod = qd_own[1, piece, :].astype(jnp.float32) * o_buf[piece, :].astype(jnp.float32)
        ld_own[1:2, piece] = jnp.sum(prod.T, axis=0, keepdims=True)

    first = (rank * rows).astype(jnp.float32)
    cuts = cu_buf[...].astype(jnp.float32)
    cut_cols = []
    for base in range(0, bounds, head):
        width = min(head, bounds - base)
        row = cuts[:, base:base + width]
        if width < head:
            row = jnp.concatenate([row, jnp.zeros((1, head - width), jnp.float32)], axis=1)
        cut_cols.append(jnp.broadcast_to(row, (head, head)).T - first)
    lane = lax.broadcasted_iota(jnp.int32, (1, head), 1)

    def fill_starts(step, _):
        lane_base = pl.multiple_of((step % (flat // head)) * head, head)
        hop = step // (flat // head)
        token = ((lane + lane_base) // heads + hop * rows).astype(jnp.float32)
        best = jnp.full((head, head), -1e9, jnp.float32)
        for col in cut_cols:
            best = jnp.maximum(best, jnp.where(col <= token, col, -1e9))
        starts[hop, :, pl.ds(lane_base, head)] = jnp.max(best, axis=0, keepdims=True)
        return 0

    lax.fori_loop(0, (HOPS + 1) * flat // head, fill_starts, 0)

    @pl.when(sends_qd[0])
    def _():
        ld_copy(0).start()
        for chunk in range(1, CHUNKS):
            qd_copy(0, chunk).start()

    dk_acc[...] = jnp.zeros_like(dk_acc)
    dv_acc[...] = jnp.zeros_like(dv_acc)
    dq_t[...] = jnp.zeros_like(dq_t)

    def tile(kv, k_from, k_to, qd, ld, chunk, key_shift, start_slot, q_side, k_side):
        part = slice(chunk * lanes, (chunk + 1) * lanes)
        key_rows = slice(k_from, k_to)
        keys, vals = kv[0, key_rows, :], kv[1, key_rows, :]
        qry, dout = qd[0, part, :], qd[1, part, :]
        score = dot(keys, qry, NT)
        grad = dot(vals, dout, NT)
        lse, row_dot = ld[0:1, part], ld[1:2, part]
        start = starts[start_slot, :, part]
        key_pos = lax.broadcasted_iota(jnp.int32, (k_to - k_from, lanes), 0).astype(jnp.float32)
        keep = key_pos >= start - float(key_shift * rows + k_from)
        if q_side and k_side:
            token = lax.broadcasted_iota(jnp.int32, (1, lanes), 1) // heads + (chunk * span - k_from)
            keep = keep & (key_pos <= token.astype(jnp.float32))
        prob = jnp.where(keep, jnp.exp2(score * (scale * LOG2E) - lse), 0.0)
        dsc = (prob * (grad - row_dot)).astype(jnp.bfloat16)
        if k_side:
            dv_acc[key_rows, :] += dot(prob.astype(jnp.bfloat16), dout, NN)
            dk_acc[key_rows, :] += dot(dsc, qry, NN)
        if q_side:
            dq_t[:, part] += dot(key_t[:, key_rows], dsc, NN)

    key_t[...] = kv_own[0].T
    for chunk in range(CHUNKS):
        tile(kv_own, 0, (chunk + 1) * span, qd_own, ld_own, chunk, 0, 0, True, True)

    def keys_arrive(hop, chunks):
        @pl.when(gets_kv[hop])
        def _():
            for chunk in chunks:
                kv_copy(hop, chunk).wait_recv()

        if hop + 1 < HOPS:
            @pl.when(sends_kv[hop + 1])
            def _():
                for chunk in chunks:
                    kv_copy(hop + 1, chunk).start()

    def keys_used(hop):
        @pl.when(gets_kv[hop])
        def _():
            key_t[...] = kv_in[hop, 0].T
            for chunk in range(CHUNKS):
                k_from = chunk * span if hop + 1 == HOPS else 0
                tile(kv_in.at[hop], k_from, rows, qd_own, ld_own, chunk, -hop - 1, 0, True, False)

    def queries_arrive(hop, chunk):
        @pl.when(gets_qd[hop])
        def _():
            if hop + 1 == HOPS and chunk in FAR:
                far_copy(chunk).wait_recv()
            else:
                qd_copy(hop, chunk).wait_recv()

        if hop + 1 < HOPS and not (hop + 2 == HOPS and chunk in FAR):
            @pl.when(sends_qd[hop + 1])
            def _():
                qd_copy(hop + 1, chunk).start()

    def stats_arrive(hop):
        @pl.when(gets_qd[hop])
        def _():
            ld_copy(hop).wait_recv()

        if hop + 1 < HOPS:
            @pl.when(sends_qd[hop + 1])
            def _():
                ld_copy(hop + 1).start()

    def queries_used(hop, chunk):
        @pl.when(gets_qd[hop])
        def _():
            k_from = chunk * span if hop + 1 == HOPS else 0
            tile(kv_own, k_from, rows, qd_in.at[hop], ld_in.at[hop], chunk, 0, hop + 1, False, True)

    for slot in range(2 * CHUNKS):
        if slot < HOPS * CHUNKS // 2:
            keys_arrive(slot // 2, (2 * (slot % 2), 2 * (slot % 2) + 1))
        hop, chunk = slot // CHUNKS, slot % CHUNKS
        queries_arrive(hop, chunk)
        if chunk == 0:
            stats_arrive(hop)
        if slot == CHUNKS - 1:
            @pl.when(sends_far)
            def _():
                for far in FAR:
                    far_copy(far).start()

            @pl.when(passes)
            def _():
                for far in FAR:
                    via_copy(far).wait_recv()
                    pass_copy(far).start()
        queries_used(hop, chunk)
        if slot % 2 == 1 and slot // 2 < HOPS:
            keys_used(slot // 2)
        if slot == 2 * HOPS - 1:
            for part in range(flat // head):
                piece = slice(part * head, (part + 1) * head)
                dq_out[piece, :] = (scale * dq_t[:, piece].T).astype(jnp.bfloat16)
        if slot == 2 * HOPS - 1:
            stats_arrive(HOPS - 1)
        if slot >= 2 * HOPS:
            far = FAR[slot - 2 * HOPS]
            queries_arrive(HOPS - 1, far)
            queries_used(HOPS - 1, far)
    rest = [chunk for chunk in range(CHUNKS) if chunk not in FAR]
    for chunk in rest + list(FAR[2 * CHUNKS - 2 * HOPS:]):
        queries_arrive(HOPS - 1, chunk)
        queries_used(HOPS - 1, chunk)

    dk_out[...] = (scale * dk_acc[...]).astype(jnp.bfloat16)
    dv_out[...] = dv_acc[...].astype(jnp.bfloat16)
    for hop in range(HOPS):
        @pl.when(sends_kv[hop])
        def _():
            for chunk in range(CHUNKS):
                kv_copy(hop, chunk).wait_send()

        @pl.when(sends_qd[hop])
        def _():
            for chunk in range(CHUNKS) if hop + 1 < HOPS else rest:
                qd_copy(hop, chunk).wait_send()
            ld_copy(hop).wait_send()

    @pl.when(sends_far | sends_via)
    def _():
        for chunk in FAR:
            far_copy(chunk).wait_send()

    @pl.when(passes)
    def _():
        for chunk in FAR:
            pass_copy(chunk).wait_send()


def store_kernel(dq_in, dk_in, dv_in, dq_hbm, dk_hbm, dv_hbm, sem):
    copies = [pltpu.make_async_copy(source, target, sem.at[index])
              for index, (source, target) in enumerate(((dq_in, dq_hbm), (dk_in, dk_hbm), (dv_in, dv_hbm)))]
    for copy in copies:
        copy.start()
    for copy in copies:
        copy.wait()


def solution(mesh):
    outer, inner = mesh.shape["cpo"], mesh.shape["cp"]
    ring = round(inner ** (1 / 3))

    def local(queries, keys, values, attn_out, logsumexp, d_out, cu_seqlens):
        rows, heads, head = queries.shape
        flat = rows * heads
        low, full = jnp.bfloat16, jnp.float32
        any_spec = pl.BlockSpec(memory_space=pl.ANY)
        vmem_spec = pl.BlockSpec(memory_space=pltpu.VMEM)
        dma = pltpu.SemaphoreType.DMA
        shapes = (jax.ShapeDtypeStruct((flat, head), low), jax.ShapeDtypeStruct((rows, head), low), jax.ShapeDtypeStruct((rows, head), low))
        grads = pl.pallas_call(
            functools.partial(backward_kernel, (outer, inner, rows, heads, head, ring)),
            out_shape=shapes,
            in_specs=[any_spec] * 7,
            out_specs=(vmem_spec,) * 3,
            scratch_shapes=[
                pltpu.VMEM((2, rows, head), low), pltpu.VMEM((HOPS, 2, rows, head), low),
                pltpu.VMEM((2, flat, head), low), pltpu.VMEM((HOPS, 2, flat, head), low), pltpu.VMEM((2, flat, head), low),
                pltpu.VMEM((flat, head), low),
                pltpu.VMEM((2, flat), full), pltpu.VMEM((HOPS, 2, flat), full),
                pltpu.VMEM((heads, rows), full), pltpu.VMEM((1, cu_seqlens.shape[0]), jnp.int32),
                pltpu.VMEM((HOPS + 1, 1, flat), full),
                pltpu.VMEM((head, rows), low), pltpu.VMEM((head, flat), full),
                pltpu.VMEM((rows, head), full), pltpu.VMEM((rows, head), full),
                dma((7,)),
                dma((HOPS, CHUNKS)), dma((HOPS, CHUNKS)), dma((HOPS, CHUNKS)), dma((HOPS, CHUNKS)),
                dma((CHUNKS,)), dma((CHUNKS,)), dma((CHUNKS,)), dma((HOPS,)), dma((HOPS,)),
            ],
            compiler_params=pltpu.CompilerParams(collective_id=0, has_side_effects=True),
        )(queries.reshape(flat, head), keys, values, attn_out.reshape(flat, head), d_out.reshape(flat, head),
          logsumexp.T, cu_seqlens.reshape(1, -1))
        d_query, d_key, d_value = pl.pallas_call(
            store_kernel, out_shape=shapes, in_specs=[vmem_spec] * 3, out_specs=(any_spec,) * 3, scratch_shapes=[dma((3,))],
        )(*grads)
        return d_query.reshape(rows, heads, head), d_key, d_value

    seq_spec = P(("dp", "cpo", "cp"))
    return jax.shard_map(local, mesh=mesh, in_specs=(seq_spec,) * 6 + (P("dp"),), out_specs=(seq_spec,) * 3, check_vma=False)
```

```python
import functools
import math

import jax
import jax.numpy as jnp
from jax import lax
from jax.experimental import pallas as pl
from jax.experimental.pallas import tpu as pltpu
from jax.sharding import PartitionSpec as P

MESH = pl.DeviceIdType.MESH
HOPS = 3
CHUNKS = 4
FAR = (0, 1, 2)
ORDER = (3, 0, 1, 2)
VIA = 2
LOG2E = math.log2(math.e)
NT = (((1,), (1,)), ((), ()))
NN = (((1,), (0,)), ((), ()))


def dot(lhs, rhs, dims):
    return lax.dot_general(lhs, rhs, dims, preferred_element_type=jnp.float32)


def backward_kernel(sizes, q_hbm, k_hbm, v_hbm, o_hbm, do_hbm, lse_hbm, cu_hbm, dq_out, dk_out, dv_out,
                    kv_own, kv_in, qd_own, qd_in, qd_via, o_buf, ld_own, ld_in, lse_buf, cu_buf, starts, key_t, dq_t, dk_acc, dv_acc,
                    load_sem, kv_send, kv_recv, qd_send, qd_recv, far_send, far_recv, via_recv, ld_send, ld_recv):
    outer, inner, rows, heads, head, ring = sizes
    group = outer * inner
    scale = head ** -0.5
    span = rows // CHUNKS
    lanes = span * heads
    flat = rows * heads
    bounds = cu_buf.shape[1]
    rank = lax.axis_index("cpo") * inner + lax.axis_index("cp")
    column = rank % ring

    def device(index):
        return (0, index // inner, index % inner)

    loads = [
        pltpu.make_async_copy(k_hbm, kv_own.at[0], load_sem.at[0]),
        pltpu.make_async_copy(v_hbm, kv_own.at[1], load_sem.at[1]),
        pltpu.make_async_copy(q_hbm, qd_own.at[0], load_sem.at[2]),
        pltpu.make_async_copy(do_hbm, qd_own.at[1], load_sem.at[3]),
        pltpu.make_async_copy(o_hbm, o_buf, load_sem.at[4]),
        pltpu.make_async_copy(lse_hbm, lse_buf, load_sem.at[5]),
        pltpu.make_async_copy(cu_hbm, cu_buf, load_sem.at[6]),
    ]
    for load in loads:
        load.start()

    barrier = pltpu.get_barrier_semaphore()
    arrivals = 0
    for step in (-4, -3, -2, -1, 1, 2, 3, 4):
        peer = rank + step
        known = (peer >= 0) & (peer < group)
        if abs(step) > HOPS:
            known = known & (column == VIA)

        @pl.when(known)
        def _():
            pl.semaphore_signal(barrier, inc=1, device_id=device(peer), device_id_type=MESH)

        arrivals = arrivals + jnp.where(known, 1, 0)
    pl.semaphore_wait(barrier, arrivals)

    def kv_copy(hop, chunk):
        source = kv_own if hop == 0 else kv_in.at[hop - 1]
        part = pl.ds(chunk * span, span)
        return pltpu.make_async_remote_copy(
            src_ref=source.at[:, part], dst_ref=kv_in.at[hop, :, part],
            send_sem=kv_send.at[hop, chunk], recv_sem=kv_recv.at[hop, chunk],
            device_id=device(rank + 1), device_id_type=MESH)

    def qd_copy(hop, chunk):
        source = qd_own if hop == 0 else qd_in.at[hop - 1]
        part = pl.ds(chunk * lanes, lanes)
        return pltpu.make_async_remote_copy(
            src_ref=source.at[:, part], dst_ref=qd_in.at[hop, :, part],
            send_sem=qd_send.at[hop, chunk], recv_sem=qd_recv.at[hop, chunk],
            device_id=device(rank - 1), device_id_type=MESH)

    def ld_copy(hop):
        return pltpu.make_async_remote_copy(
            src_ref=ld_own, dst_ref=ld_in.at[hop],
            send_sem=ld_send.at[hop], recv_sem=ld_recv.at[hop],
            device_id=device(rank - hop - 1), device_id_type=MESH)

    def far_copy(chunk):
        part = pl.ds(chunk * lanes, lanes)
        return pltpu.make_async_remote_copy(
            src_ref=qd_own.at[:, part], dst_ref=qd_in.at[HOPS - 1, :, part],
            send_sem=far_send.at[chunk], recv_sem=far_recv.at[chunk],
            device_id=device(rank - 3), device_id_type=MESH)

    def via_copy(chunk):
        part = pl.ds(chunk * lanes, lanes)
        return pltpu.make_async_remote_copy(
            src_ref=qd_own.at[:, part], dst_ref=qd_via.at[:, part],
            send_sem=far_send.at[chunk], recv_sem=via_recv.at[chunk],
            device_id=device(rank - 4), device_id_type=MESH)

    def pass_copy(chunk):
        part = pl.ds(chunk * lanes, lanes)
        return pltpu.make_async_remote_copy(
            src_ref=qd_via.at[:, part], dst_ref=qd_in.at[HOPS - 1, :, part],
            send_sem=qd_send.at[HOPS - 1, chunk], recv_sem=far_recv.at[chunk],
            device_id=device(rank + 1), device_id_type=MESH)

    sends_kv = [(rank >= hop) & (rank + 1 < group) for hop in range(HOPS)]
    gets_kv = [rank >= hop + 1 for hop in range(HOPS)]
    sends_qd = [(rank >= 1) & (rank + hop < group) for hop in range(HOPS)]
    gets_qd = [rank + hop + 1 < group for hop in range(HOPS)]
    sends_ld = [rank >= hop + 1 for hop in range(HOPS)]
    is_via = column == VIA
    sends_far = (rank >= HOPS) & ~is_via
    sends_via = (rank >= HOPS + 1) & is_via
    passes = is_via & (rank + HOPS + 1 < group)

    loads[0].wait()
    loads[1].wait()

    @pl.when(sends_kv[0])
    def _():
        for chunk in range(CHUNKS):
            kv_copy(0, chunk).start()

    loads[2].wait()
    loads[3].wait()

    @pl.when(sends_qd[0])
    def _():
        qd_copy(0, ORDER[0]).start()

    @pl.when(sends_far)
    def _():
        far_copy(FAR[0]).start()

    @pl.when(sends_via)
    def _():
        for chunk in FAR:
            via_copy(chunk).start()

    loads[4].wait()
    loads[5].wait()
    loads[6].wait()

    row_id = lax.broadcasted_iota(jnp.int32, (head, heads * head), 0)
    lane_id = lax.broadcasted_iota(jnp.int32, (head, heads * head), 1)
    for part in range(rows // head):
        piece = slice(part * head, (part + 1) * head)
        wide = jnp.zeros((head, heads * head), jnp.float32)
        for g in range(heads):
            column_g = jnp.broadcast_to(lse_buf[g:g + 1, piece], (head, head)).T
            wide = jnp.where(lane_id == row_id * heads + g, jnp.concatenate([column_g] * heads, axis=1), wide)
        ld_own[0:1, part * heads * head:(part + 1) * heads * head] = jnp.sum(wide, axis=0, keepdims=True) * LOG2E
    for part in range(flat // head):
        piece = slice(part * head, (part + 1) * head)
        prod = qd_own[1, piece, :].astype(jnp.float32) * o_buf[piece, :].astype(jnp.float32)
        ld_own[1:2, piece] = jnp.sum(prod.T, axis=0, keepdims=True)

    first = (rank * rows).astype(jnp.float32)
    cuts = cu_buf[...].astype(jnp.float32)
    cut_cols = []
    for base in range(0, bounds, head):
        width = min(head, bounds - base)
        row = cuts[:, base:base + width]
        if width < head:
            row = jnp.concatenate([row, jnp.zeros((1, head - width), jnp.float32)], axis=1)
        cut_cols.append(jnp.broadcast_to(row, (head, head)).T - first)
    lane = lax.broadcasted_iota(jnp.int32, (1, head), 1)

    def fill_starts(step, _):
        lane_base = pl.multiple_of((step % (flat // head)) * head, head)
        hop = step // (flat // head)
        token = ((lane + lane_base) // heads + hop * rows).astype(jnp.float32)
        best = jnp.full((head, head), -1e9, jnp.float32)
        for col in cut_cols:
            best = jnp.maximum(best, jnp.where(col <= token, col, -1e9))
        starts[hop, :, pl.ds(lane_base, head)] = jnp.max(best, axis=0, keepdims=True)
        return 0

    lax.fori_loop(0, (HOPS + 1) * flat // head, fill_starts, 0)

    for hop in range(HOPS):
        @pl.when(sends_ld[hop])
        def _():
            ld_copy(hop).start()

    @pl.when(sends_qd[0])
    def _():
        for chunk in ORDER[1:]:
            qd_copy(0, chunk).start()

    dk_acc[...] = jnp.zeros_like(dk_acc)
    dv_acc[...] = jnp.zeros_like(dv_acc)
    dq_t[...] = jnp.zeros_like(dq_t)

    def tile(kv, k_from, k_to, qd, ld, chunk, key_shift, start_slot, q_side, k_side):
        part = slice(chunk * lanes, (chunk + 1) * lanes)
        key_rows = slice(k_from, k_to)
        keys, vals = kv[0, key_rows, :], kv[1, key_rows, :]
        qry, dout = qd[0, part, :], qd[1, part, :]
        score = dot(keys, qry, NT)
        grad = dot(vals, dout, NT)
        lse, row_dot = ld[0:1, part], ld[1:2, part]
        start = starts[start_slot, :, part]
        key_pos = lax.broadcasted_iota(jnp.int32, (k_to - k_from, lanes), 0).astype(jnp.float32)
        keep = key_pos >= start - float(key_shift * rows + k_from)
        if q_side and k_side:
            token = lax.broadcasted_iota(jnp.int32, (1, lanes), 1) // heads + (chunk * span - k_from)
            keep = keep & (key_pos <= token.astype(jnp.float32))
        prob = jnp.where(keep, jnp.exp2(score * (scale * LOG2E) - lse), 0.0)
        dsc = (prob * (grad - row_dot)).astype(jnp.bfloat16)
        if k_side:
            dv_acc[key_rows, :] += dot(prob.astype(jnp.bfloat16), dout, NN)
            dk_acc[key_rows, :] += dot(dsc, qry, NN)
        if q_side:
            dq_t[:, part] += dot(key_t[:, key_rows], dsc, NN)

    key_t[...] = kv_own[0].T
    for chunk in range(CHUNKS):
        tile(kv_own, 0, (chunk + 1) * span, qd_own, ld_own, chunk, 0, 0, True, True)

    def keys_arrive(hop, chunks):
        @pl.when(gets_kv[hop])
        def _():
            for chunk in chunks:
                kv_copy(hop, chunk).wait_recv()

        if hop + 1 < HOPS:
            @pl.when(sends_kv[hop + 1])
            def _():
                for chunk in chunks:
                    kv_copy(hop + 1, chunk).start()

    def keys_used(hop):
        @pl.when(gets_kv[hop])
        def _():
            key_t[...] = kv_in[hop, 0].T
            for chunk in range(CHUNKS):
                k_from = chunk * span if hop + 1 == HOPS else 0
                tile(kv_in.at[hop], k_from, rows, qd_own, ld_own, chunk, -hop - 1, 0, True, False)

    def queries_arrive(hop, chunk):
        @pl.when(gets_qd[hop])
        def _():
            if hop + 1 == HOPS and chunk in FAR:
                far_copy(chunk).wait_recv()
            else:
                qd_copy(hop, chunk).wait_recv()

        if hop + 1 < HOPS and not (hop + 2 == HOPS and chunk in FAR):
            @pl.when(sends_qd[hop + 1])
            def _():
                qd_copy(hop + 1, chunk).start()

    def stats_arrive(hop):
        @pl.when(gets_qd[hop])
        def _():
            ld_copy(hop).wait_recv()

    def far_goes(index):
        @pl.when(sends_far)
        def _():
            far_copy(FAR[index]).start()

    def via_passes(index):
        @pl.when(passes)
        def _():
            via_copy(FAR[index]).wait_recv()
            pass_copy(FAR[index]).start()

    def queries_used(hop, chunk):
        @pl.when(gets_qd[hop])
        def _():
            k_from = chunk * span if hop + 1 == HOPS else 0
            tile(kv_own, k_from, rows, qd_in.at[hop], ld_in.at[hop], chunk, 0, hop + 1, False, True)

    def queries(hop, index):
        queries_arrive(hop, ORDER[index])
        if index == 0:
            stats_arrive(hop)
        queries_used(hop, ORDER[index])

    def far_queries(index):
        queries_arrive(HOPS - 1, FAR[index])
        if index == 0:
            stats_arrive(HOPS - 1)
        queries_used(HOPS - 1, FAR[index])

    keys_arrive(0, (0, 1))
    queries(0, 0)
    keys_arrive(0, (2, 3))
    far_goes(1)
    via_passes(0)
    queries(0, 1)
    keys_used(0)
    queries(0, 2)
    far_queries(0)
    keys_arrive(1, (0, 1))
    via_passes(1)
    queries(0, 3)
    keys_arrive(1, (2, 3))
    far_goes(2)
    via_passes(2)
    queries(1, 0)
    keys_used(1)
    queries(1, 1)
    far_queries(1)
    keys_arrive(2, (0, 1))
    queries(1, 2)
    keys_arrive(2, (2, 3))
    queries(1, 3)
    keys_used(2)
    for part in range(flat // head):
        piece = slice(part * head, (part + 1) * head)
        dq_out[piece, :] = (scale * dq_t[:, piece].T).astype(jnp.bfloat16)
    far_queries(2)
    queries_arrive(HOPS - 1, ORDER[0])
    queries_used(HOPS - 1, ORDER[0])

    dk_out[...] = (scale * dk_acc[...]).astype(jnp.bfloat16)
    dv_out[...] = dv_acc[...].astype(jnp.bfloat16)
    for hop in range(HOPS):
        @pl.when(sends_kv[hop])
        def _():
            for chunk in range(CHUNKS):
                kv_copy(hop, chunk).wait_send()

        @pl.when(sends_qd[hop])
        def _():
            for chunk in ORDER if hop + 1 < HOPS else ORDER[:1]:
                qd_copy(hop, chunk).wait_send()

        @pl.when(sends_ld[hop])
        def _():
            ld_copy(hop).wait_send()

    @pl.when(sends_far | sends_via)
    def _():
        for chunk in FAR:
            far_copy(chunk).wait_send()

    @pl.when(passes)
    def _():
        for chunk in FAR:
            pass_copy(chunk).wait_send()


def store_kernel(dq_in, dk_in, dv_in, dq_hbm, dk_hbm, dv_hbm, sem):
    copies = [pltpu.make_async_copy(source, target, sem.at[index])
              for index, (source, target) in enumerate(((dq_in, dq_hbm), (dk_in, dk_hbm), (dv_in, dv_hbm)))]
    for copy in copies:
        copy.start()
    for copy in copies:
        copy.wait()


def solution(mesh):
    outer, inner = mesh.shape["cpo"], mesh.shape["cp"]
    ring = round(inner ** (1 / 3))

    def local(queries, keys, values, attn_out, logsumexp, d_out, cu_seqlens):
        rows, heads, head = queries.shape
        flat = rows * heads
        low, full = jnp.bfloat16, jnp.float32
        any_spec = pl.BlockSpec(memory_space=pl.ANY)
        vmem_spec = pl.BlockSpec(memory_space=pltpu.VMEM)
        dma = pltpu.SemaphoreType.DMA
        shapes = (jax.ShapeDtypeStruct((flat, head), low), jax.ShapeDtypeStruct((rows, head), low), jax.ShapeDtypeStruct((rows, head), low))
        grads = pl.pallas_call(
            functools.partial(backward_kernel, (outer, inner, rows, heads, head, ring)),
            out_shape=tuple(pltpu.VMEM(shape.shape, low) for shape in shapes),
            in_specs=[any_spec] * 7,
            out_specs=(vmem_spec,) * 3,
            scratch_shapes=[
                pltpu.VMEM((2, rows, head), low), pltpu.VMEM((HOPS, 2, rows, head), low),
                pltpu.VMEM((2, flat, head), low), pltpu.VMEM((HOPS, 2, flat, head), low), pltpu.VMEM((2, flat, head), low),
                pltpu.VMEM((flat, head), low),
                pltpu.VMEM((2, flat), full), pltpu.VMEM((HOPS, 2, flat), full),
                pltpu.VMEM((heads, rows), full), pltpu.VMEM((1, cu_seqlens.shape[0]), jnp.int32),
                pltpu.VMEM((HOPS + 1, 1, flat), full),
                pltpu.VMEM((head, rows), low), pltpu.VMEM((head, flat), full),
                pltpu.VMEM((rows, head), full), pltpu.VMEM((rows, head), full),
                dma((7,)),
                dma((HOPS, CHUNKS)), dma((HOPS, CHUNKS)), dma((HOPS, CHUNKS)), dma((HOPS, CHUNKS)),
                dma((CHUNKS,)), dma((CHUNKS,)), dma((CHUNKS,)), dma((HOPS,)), dma((HOPS,)),
            ],
            compiler_params=pltpu.CompilerParams(collective_id=0, has_side_effects=True),
        )(queries.reshape(flat, head), keys, values, attn_out.reshape(flat, head), d_out.reshape(flat, head),
          logsumexp.T, cu_seqlens.reshape(1, -1))
        d_query, d_key, d_value = pl.pallas_call(
            store_kernel, out_shape=shapes, in_specs=[vmem_spec] * 3, out_specs=(any_spec,) * 3, scratch_shapes=[dma((3,))],
        )(*(pltpu.with_memory_space_constraint(grad, pltpu.VMEM) for grad in grads))
        return d_query.reshape(rows, heads, head), d_key, d_value

    seq_spec = P(("dp", "cpo", "cp"))
    return jax.shard_map(local, mesh=mesh, in_specs=(seq_spec,) * 6 + (P("dp"),), out_specs=(seq_spec,) * 3, check_vma=False)
```

```python
import functools
import math

import jax
import jax.numpy as jnp
from jax import lax
from jax.experimental import pallas as pl
from jax.experimental.pallas import tpu as pltpu
from jax.sharding import PartitionSpec as P

MESH = pl.DeviceIdType.MESH
SHARDS = 5
KV_CHUNKS = 2
QD_CHUNKS = 4
LOG2E = math.log2(math.e)
NT = (((1,), (1,)), ((), ()))
NN = (((1,), (0,)), ((), ()))


def dot(lhs, rhs, dims):
    return lax.dot_general(lhs, rhs, dims, preferred_element_type=jnp.float32)


def backward_kernel(sizes, q_hbm, k_hbm, v_hbm, o_hbm, do_hbm, lse_hbm, cu_hbm, dq_out, dkv_out,
                    kv_s, kv_w, qd_s, qd_w, ld_s, ld_w, o_buf, lse_buf, cu_buf, starts, key_t, dq_t, dk_acc, dv_acc, dq_fin, dkv_fin,
                    load_sem, guest_send, guest_recv, fwd_send, fwd_recv, right_send, right_recv, left_send, left_recv, back_send, back_recv):
    outer, inner, rows, heads, head = sizes
    group = outer * inner
    pairs = group // 2
    scale = head ** -0.5
    flat = rows * heads
    k_part = rows // KV_CHUNKS
    lanes = flat // QD_CHUNKS
    span = rows // QD_CHUNKS
    bounds = cu_buf.shape[1]
    rank = lax.axis_index("cpo") * inner + lax.axis_index("cp")

    def resident(pair):
        return (pair + pair // (inner // 2) + 1) % 2

    def host(pair):
        return 2 * pair + resident(pair)

    def helper(pair):
        return (host(pair) + inner) % group

    is_host = rank % 2 == resident(rank // 2)
    is_helper = rank % 2 != resident(rank // 2)
    pair = jnp.where(is_host, rank // 2, ((rank + inner) % group) // 2)
    res = resident(pair)
    gst = 1 - res
    guest = 2 * pair + gst
    own = jnp.where(is_host, res, 2)
    prev_res, next_res = resident(pair - 1), resident(pair + 1)
    has_prev, has_prev2 = pair >= 1, pair >= 2
    has_next, has_next2 = pair + 1 < pairs, pair + 2 < pairs
    my_host = 2 * (rank // 2) + resident(rank // 2)

    def device(index):
        return (0, index // inner, index % inner)

    def remote(source, target, send, recv, index):
        return pltpu.make_async_remote_copy(src_ref=source, dst_ref=target, send_sem=send, recv_sem=recv,
                                            device_id=device(index), device_id_type=MESH)

    loads = [
        pltpu.make_async_copy(k_hbm, kv_s.at[own, 0], load_sem.at[0]),
        pltpu.make_async_copy(v_hbm, kv_s.at[own, 1], load_sem.at[1]),
        pltpu.make_async_copy(q_hbm, qd_s.at[own, 0], load_sem.at[2]),
        pltpu.make_async_copy(do_hbm, qd_s.at[own, 1], load_sem.at[3]),
        pltpu.make_async_copy(o_hbm, o_buf, load_sem.at[4]),
        pltpu.make_async_copy(lse_hbm, lse_buf, load_sem.at[5]),
        pltpu.make_async_copy(cu_hbm, cu_buf, load_sem.at[6]),
    ]
    for load in loads:
        load.start()

    barrier = pltpu.get_barrier_semaphore()
    everyone = rank >= 0
    peers = [
        (is_host, helper(pair)), (is_host, guest), (is_helper, host(pair)), (is_helper, guest),
        (is_helper, my_host), (is_helper, (my_host + inner) % group),
        (everyone & has_next, host(pair + 1)), (everyone & has_next2, host(pair + 2)),
        (is_host & has_prev, host(pair - 1)), (is_host & has_prev2, host(pair - 2)),
        (is_host & has_prev, helper(pair - 1)), (is_host & has_prev2, helper(pair - 2)),
    ]
    arrivals = 0
    for known, peer in peers:
        @pl.when(known)
        def _():
            pl.semaphore_signal(barrier, inc=1, device_id=device(peer), device_id_type=MESH)

        arrivals = arrivals + jnp.where(known, 1, 0)
    pl.semaphore_wait(barrier, arrivals)

    def kv_rows(chunk):
        return pl.ds(chunk * k_part, k_part)

    def qd_rows(chunk):
        if isinstance(chunk, int):
            return pl.ds(chunk * lanes, lanes)
        return pl.ds(pl.multiple_of(chunk * lanes, lanes), lanes)

    LD = KV_CHUNKS + QD_CHUNKS

    place = jnp.where(is_host, gst, rank % 2)

    def guest_kv(chunk):
        part = kv_rows(chunk)
        return remote(kv_s.at[2, :, part], kv_s.at[place, :, part], guest_send.at[chunk], guest_recv.at[chunk], my_host)

    def guest_qd(chunk):
        part = qd_rows(chunk)
        return remote(qd_s.at[2, :, part], qd_s.at[place, :, part], guest_send.at[KV_CHUNKS + chunk], guest_recv.at[KV_CHUNKS + chunk], my_host)

    def guest_ld():
        return remote(ld_s.at[2], ld_s.at[place], guest_send.at[LD], guest_recv.at[LD], my_host)

    def fwd_kv(slot, chunk):
        part = kv_rows(chunk)
        return remote(kv_s.at[slot, :, part], kv_s.at[slot, :, part], fwd_send.at[slot, chunk], fwd_recv.at[slot, chunk], helper(pair))

    def fwd_qd(slot, chunk):
        part = qd_rows(chunk)
        return remote(qd_s.at[slot, :, part], qd_s.at[slot, :, part], fwd_send.at[slot, KV_CHUNKS + chunk], fwd_recv.at[slot, KV_CHUNKS + chunk], helper(pair))

    def fwd_ld(slot):
        return remote(ld_s.at[slot], ld_s.at[slot], fwd_send.at[slot, LD], fwd_recv.at[slot, LD], helper(pair))

    def right1(slot, chunk):
        part = kv_rows(chunk)
        return remote(kv_s.at[slot, :, part], kv_w.at[slot, :, part], right_send.at[slot, chunk], right_recv.at[slot, chunk], host(pair + 1))

    def right2(chunk):
        part = kv_rows(chunk)
        return remote(kv_s.at[1, :, part], kv_w.at[2, :, part], right_send.at[2, chunk], right_recv.at[2, chunk], host(pair + 2))

    def left1(slot, chunk):
        part = qd_rows(chunk)
        return remote(qd_s.at[slot, :, part], qd_w.at[slot, :, part], left_send.at[slot, chunk], left_recv.at[slot, chunk], helper(pair - 1))

    def left2(chunk):
        part = qd_rows(chunk)
        return remote(qd_s.at[0, :, part], qd_w.at[2, :, part], left_send.at[2, chunk], left_recv.at[2, chunk], helper(pair - 2))

    def left1_ld(slot):
        return remote(ld_s.at[slot], ld_w.at[slot], left_send.at[slot, QD_CHUNKS], left_recv.at[slot, QD_CHUNKS], helper(pair - 1))

    def left2_ld():
        return remote(ld_s.at[0], ld_w.at[2], left_send.at[2, QD_CHUNKS], left_recv.at[2, QD_CHUNKS], helper(pair - 2))

    def back_dq():
        return remote(dq_fin.at[gst], dq_out, back_send.at[0], back_recv.at[0], guest)

    def back_dkv(slot, index, target):
        return remote(dkv_fin.at[slot], dkv_out, back_send.at[index], back_recv.at[1], target)

    def when(cond, *starts_of):
        @pl.when(cond)
        def _():
            for item in starts_of:
                item().start()

    loads[0].wait()
    loads[1].wait()
    for chunk in range(KV_CHUNKS):
        when(is_helper, lambda: guest_kv(chunk))
        when(is_host & has_next, lambda: right1(res, chunk))
        when(is_host, lambda: fwd_kv(res, chunk))
        when(is_host & has_next2 & (res == 1), lambda: right2(chunk))
    loads[2].wait()
    loads[3].wait()
    for chunk in range(QD_CHUNKS):
        when(is_host, lambda: fwd_qd(res, chunk))
    for chunk in range(QD_CHUNKS // 2):
        when(is_host & has_prev2 & (res == 0), lambda: left2(chunk))
    loads[4].wait()
    loads[5].wait()
    loads[6].wait()

    row_id = lax.broadcasted_iota(jnp.int32, (head, heads * head), 0)
    lane_id = lax.broadcasted_iota(jnp.int32, (head, heads * head), 1)
    for part in range(rows // head):
        piece = slice(part * head, (part + 1) * head)
        wide = jnp.zeros((head, heads * head), jnp.float32)
        for g in range(heads):
            column_g = jnp.broadcast_to(lse_buf[g:g + 1, piece], (head, head)).T
            wide = jnp.where(lane_id == row_id * heads + g, jnp.concatenate([column_g] * heads, axis=1), wide)
        ld_s[own, 0:1, part * heads * head:(part + 1) * heads * head] = jnp.sum(wide, axis=0, keepdims=True) * LOG2E
    for part in range(flat // head):
        piece = slice(part * head, (part + 1) * head)
        prod = qd_s[own, 1, piece, :].astype(jnp.float32) * o_buf[piece, :].astype(jnp.float32)
        ld_s[own, 1:2, piece] = jnp.sum(prod.T, axis=0, keepdims=True)

    first = (pair * (2 * rows)).astype(jnp.float32)
    cuts = cu_buf[...].astype(jnp.float32)
    cut_cols = []
    for base in range(0, bounds, head):
        width = min(head, bounds - base)
        row = cuts[:, base:base + width]
        if width < head:
            row = jnp.concatenate([row, jnp.zeros((1, head - width), jnp.float32)], axis=1)
        cut_cols.append(jnp.broadcast_to(row, (head, head)).T - first)
    lane = lax.broadcasted_iota(jnp.int32, (1, head), 1)

    def fill_starts(step, _):
        lane_base = pl.multiple_of((step % (flat // head)) * head, head)
        shard = step // (flat // head)
        token = ((lane + lane_base) // heads + shard * rows).astype(jnp.float32)
        best = jnp.full((head, head), -1e9, jnp.float32)
        for col in cut_cols:
            best = jnp.maximum(best, jnp.where(col <= token, col, -1e9))
        starts[shard, :, pl.ds(lane_base, head)] = jnp.max(best, axis=0, keepdims=True)
        return 0

    lax.fori_loop(0, 2 * (flat // head), fill_starts, 0)

    when(is_helper, guest_ld)
    when(is_host, lambda: fwd_ld(res))
    when(is_host & has_prev, lambda: left1_ld(res))
    when(is_host & has_prev2 & (res == 0), left2_ld)
    for chunk in range(QD_CHUNKS):
        when(is_helper, lambda: guest_qd(chunk))
        when(is_host & has_prev, lambda: left1(res, chunk))

    def scores(kv, key_rows, key_off, qd, ld, part, start, token_off):
        keys, vals = kv[0, key_rows, :], kv[1, key_rows, :]
        qry, dout = qd[0, part, :], qd[1, part, :]
        score = dot(keys, qry, NT)
        grad = dot(vals, dout, NT)
        lse, row_dot = ld[0:1, part], ld[1:2, part]
        key_pos = lax.broadcasted_iota(jnp.int32, score.shape, 0).astype(jnp.float32)
        keep = key_pos >= start[:, part] - key_off
        if token_off is not None:
            token = lax.broadcasted_iota(jnp.int32, (1, lanes), 1) // heads + token_off
            keep = keep & (key_pos <= token.astype(jnp.float32))
        prob = jnp.where(keep, jnp.exp2(score * (scale * LOG2E) - lse), 0.0)
        dsc = (prob * (grad - row_dot)).astype(jnp.bfloat16)
        return prob, dsc, qry, dout

    def q_tile(kv, k_from, k_to, key_off, q_slot, chunk, token_off=None):
        part, key_rows = qd_rows(chunk), pl.ds(k_from, k_to - k_from)
        _, dsc, _, _ = scores(kv, key_rows, key_off + k_from, qd_s.at[q_slot], ld_s.at[q_slot], part, starts.at[q_slot], token_off)
        dq_t[q_slot, :, part] += dot(key_t[:, k_from:k_to], dsc, NN)

    def k_tile(k_slot, k_from, k_to, qd, ld, q_shard, chunk, token_off=None):
        part, key_rows = qd_rows(chunk), pl.ds(k_from, k_to - k_from)
        key_off = (k_slot * rows + k_from) * 1.0
        prob, dsc, qry, dout = scores(kv_s.at[k_slot], key_rows, key_off, qd, ld, part, starts.at[q_shard], token_off)
        dv_acc[k_slot, key_rows, :] += dot(prob.astype(jnp.bfloat16), dout, NN)
        dk_acc[k_slot, key_rows, :] += dot(dsc, qry, NN)

    def finish_dq(slot, target):
        for part in range(flat // head):
            piece = slice(part * head, (part + 1) * head)
            target[piece, :] = (scale * dq_t[slot, :, piece].T).astype(jnp.bfloat16)

    def finish_dkv(slot):
        dkv_fin[slot, 0, :, :] = (scale * dk_acc[slot, :, :]).astype(jnp.bfloat16)
        dkv_fin[slot, 1, :, :] = dv_acc[slot, :, :].astype(jnp.bfloat16)

    @pl.when(is_host)
    def _():
        dq_t[...] = jnp.zeros_like(dq_t)

        def diagonal(slot):
            key_t[...] = kv_s[slot, 0, :, :].T
            for chunk in range(QD_CHUNKS):
                q_tile(kv_s.at[slot], 0, (chunk + 1) * span, slot * rows * 1.0, slot, chunk, chunk * span)

        diagonal(res)
        for chunk in range(KV_CHUNKS):
            guest_kv(chunk).wait_recv()
            when(has_next, lambda: right1(gst, chunk))
            fwd_kv(gst, chunk).start()
            when(has_next2 & (gst == 1), lambda: right2(chunk))
        guest_ld().wait_recv()
        fwd_ld(gst).start()
        when(has_prev, lambda: left1_ld(gst))
        when(has_prev2 & (gst == 0), left2_ld)
        for chunk in range(QD_CHUNKS // 2, QD_CHUNKS):
            when(has_prev2 & (res == 0), lambda: left2(chunk))

        @pl.when(has_prev)
        def _():
            for chunk in range(KV_CHUNKS):
                right1(prev_res, chunk).wait_recv()
            key_t[...] = kv_w[prev_res, 0, :, :].T

        prev_off = (prev_res - 2) * rows * 1.0
        late_off = (-1 - prev_res) * rows * 1.0

        def pass_queries(chunk, _):
            guest_qd(chunk).wait_recv()
            when(has_prev, lambda: left1(gst, chunk))
            fwd_qd(gst, chunk).start()
            when(has_prev2 & (gst == 0), lambda: left2(chunk))

            @pl.when(has_prev)
            def _():
                q_tile(kv_w.at[prev_res], 0, rows, prev_off, res, chunk)
                q_tile(kv_w.at[prev_res], 0, rows, prev_off, gst, chunk)

            return 0

        lax.fori_loop(0, QD_CHUNKS, pass_queries, 0)
        diagonal(gst)
        key_t[...] = kv_s[0, 0, :, :].T
        for chunk in range(QD_CHUNKS):
            q_tile(kv_s.at[0], 0, rows, 0.0, 1, chunk)

        @pl.when(has_prev2)
        def _():
            for chunk in range(KV_CHUNKS):
                right2(chunk).wait_recv()
            key_t[...] = kv_w[2, 0, :, :].T
            for chunk in range(QD_CHUNKS):
                q_tile(kv_w.at[2], chunk * span, rows, -3.0 * rows, 0, chunk)

        def late_keys(slot):
            @pl.when(has_prev)
            def _():
                def two(step, _):
                    q_tile(kv_w.at[1 - prev_res], 0, rows, late_off, slot, 2 * step)
                    q_tile(kv_w.at[1 - prev_res], 0, rows, late_off, slot, 2 * step + 1)
                    return 0

                lax.fori_loop(0, QD_CHUNKS // 2, two, 0)

        @pl.when(has_prev)
        def _():
            for chunk in range(KV_CHUNKS):
                right1(1 - prev_res, chunk).wait_recv()
            key_t[...] = kv_w[1 - prev_res, 0, :, :].T

        late_keys(gst)
        finish_dq(gst, dq_fin.at[gst])
        late_keys(res)
        back_dq().start()
        finish_dq(res, dq_out)

        for chunk in range(KV_CHUNKS):
            fwd_kv(res, chunk).wait_send()
            fwd_kv(gst, chunk).wait_send()
        for chunk in range(QD_CHUNKS):
            fwd_qd(res, chunk).wait_send()
            fwd_qd(gst, chunk).wait_send()
        fwd_ld(res).wait_send()
        fwd_ld(gst).wait_send()

        @pl.when(has_next)
        def _():
            for chunk in range(KV_CHUNKS):
                right1(0, chunk).wait_send()
                right1(1, chunk).wait_send()

        @pl.when(has_next2)
        def _():
            for chunk in range(KV_CHUNKS):
                right2(chunk).wait_send()

        @pl.when(has_prev)
        def _():
            for slot in range(2):
                for chunk in range(QD_CHUNKS):
                    left1(slot, chunk).wait_send()
                left1_ld(slot).wait_send()

        @pl.when(has_prev2)
        def _():
            for chunk in range(QD_CHUNKS):
                left2(chunk).wait_send()
            left2_ld().wait_send()

        back_dq().wait_send()
        back_dkv(0, 1, guest).wait_recv()

    @pl.when(is_helper)
    def _():
        lax.fori_loop(2 * (flat // head), SHARDS * (flat // head), fill_starts, 0)
        dk_acc[...] = jnp.zeros_like(dk_acc)
        dv_acc[...] = jnp.zeros_like(dv_acc)

        def diagonal(slot):
            for chunk in range(QD_CHUNKS):
                k_tile(slot, 0, (chunk + 1) * span, qd_s.at[slot], ld_s.at[slot], slot, chunk, chunk * span)

        for chunk in range(KV_CHUNKS):
            fwd_kv(res, chunk).wait_recv()
        for chunk in range(QD_CHUNKS):
            fwd_qd(res, chunk).wait_recv()
        fwd_ld(res).wait_recv()
        diagonal(res)
        for chunk in range(KV_CHUNKS):
            fwd_kv(gst, chunk).wait_recv()

        def queries(slot):
            @pl.when(has_next)
            def _():
                left1_ld(slot).wait_recv()

                def one(chunk, _):
                    left1(slot, chunk).wait_recv()
                    k_tile(gst, 0, rows, qd_w.at[slot], ld_w.at[slot], slot + 2, chunk)
                    k_tile(res, 0, rows, qd_w.at[slot], ld_w.at[slot], slot + 2, chunk)
                    return 0

                lax.fori_loop(0, QD_CHUNKS, one, 0)

        queries(next_res)
        for chunk in range(QD_CHUNKS):
            fwd_qd(gst, chunk).wait_recv()
        fwd_ld(gst).wait_recv()
        diagonal(gst)
        for chunk in range(QD_CHUNKS):
            k_tile(0, 0, rows, qd_s.at[1], ld_s.at[1], 1, chunk)

        @pl.when(has_next2)
        def _():
            left2_ld().wait_recv()
            for chunk in range(QD_CHUNKS):
                left2(chunk).wait_recv()
                k_tile(1, chunk * span, rows, qd_w.at[2], ld_w.at[2], 4, chunk)

        queries(1 - next_res)
        finish_dkv(gst)
        finish_dkv(res)
        back_dkv(gst, 1, guest).start()
        back_dkv(res, 2, host(pair)).start()

        for chunk in range(KV_CHUNKS):
            guest_kv(chunk).wait_send()
        for chunk in range(QD_CHUNKS):
            guest_qd(chunk).wait_send()
        guest_ld().wait_send()
        back_dkv(gst, 1, guest).wait_send()
        back_dkv(res, 2, host(pair)).wait_send()
        back_dq().wait_recv()
        back_dkv(0, 1, guest).wait_recv()


def store_kernel(dq_in, dkv_in, dq_hbm, dk_hbm, dv_hbm, sem):
    copies = [pltpu.make_async_copy(source, target, sem.at[index])
              for index, (source, target) in enumerate(((dq_in, dq_hbm), (dkv_in.at[0], dk_hbm), (dkv_in.at[1], dv_hbm)))]
    for copy in copies:
        copy.start()
    for copy in copies:
        copy.wait()


def solution(mesh):
    outer, inner = mesh.shape["cpo"], mesh.shape["cp"]

    def local(queries, keys, values, attn_out, logsumexp, d_out, cu_seqlens):
        rows, heads, head = queries.shape
        flat = rows * heads
        low, full = jnp.bfloat16, jnp.float32
        any_spec = pl.BlockSpec(memory_space=pl.ANY)
        vmem_spec = pl.BlockSpec(memory_space=pltpu.VMEM)
        dma = pltpu.SemaphoreType.DMA
        moves = KV_CHUNKS + QD_CHUNKS + 1
        grads = pl.pallas_call(
            functools.partial(backward_kernel, (outer, inner, rows, heads, head)),
            out_shape=(pltpu.VMEM((flat, head), low), pltpu.VMEM((2, rows, head), low)),
            in_specs=[any_spec] * 7,
            out_specs=(vmem_spec,) * 2,
            scratch_shapes=[
                pltpu.VMEM((3, 2, rows, head), low), pltpu.VMEM((3, 2, rows, head), low),
                pltpu.VMEM((3, 2, flat, head), low), pltpu.VMEM((3, 2, flat, head), low),
                pltpu.VMEM((3, 2, flat), full), pltpu.VMEM((3, 2, flat), full),
                pltpu.VMEM((flat, head), low), pltpu.VMEM((heads, rows), full), pltpu.VMEM((1, cu_seqlens.shape[0]), jnp.int32),
                pltpu.VMEM((SHARDS, 1, flat), full), pltpu.VMEM((head, rows), low),
                pltpu.VMEM((2, head, flat), full), pltpu.VMEM((2, rows, head), full), pltpu.VMEM((2, rows, head), full),
                pltpu.VMEM((2, flat, head), low), pltpu.VMEM((2, 2, rows, head), low),
                dma((7,)), dma((moves,)), dma((moves,)), dma((2, moves)), dma((2, moves)),
                dma((3, KV_CHUNKS)), dma((3, KV_CHUNKS)), dma((3, QD_CHUNKS + 1)), dma((3, QD_CHUNKS + 1)), dma((3,)), dma((2,)),
            ],
            compiler_params=pltpu.CompilerParams(collective_id=0, has_side_effects=True),
        )(queries.reshape(flat, head), keys, values, attn_out.reshape(flat, head), d_out.reshape(flat, head),
          logsumexp.T, cu_seqlens.reshape(1, -1))
        d_query, d_key, d_value = pl.pallas_call(
            store_kernel,
            out_shape=(jax.ShapeDtypeStruct((flat, head), low), jax.ShapeDtypeStruct((rows, head), low), jax.ShapeDtypeStruct((rows, head), low)),
            in_specs=[vmem_spec] * 2, out_specs=(any_spec,) * 3, scratch_shapes=[dma((3,))],
        )(*(pltpu.with_memory_space_constraint(grad, pltpu.VMEM) for grad in grads))
        return d_query.reshape(rows, heads, head), d_key, d_value

    seq_spec = P(("dp", "cpo", "cp"))
    return jax.shard_map(local, mesh=mesh, in_specs=(seq_spec,) * 6 + (P("dp"),), out_specs=(seq_spec,) * 3, check_vma=False)
```

```python
import functools
import math

import jax
import jax.numpy as jnp
from jax import lax
from jax.experimental import pallas as pl
from jax.experimental.pallas import tpu as pltpu
from jax.sharding import PartitionSpec as P

MESH = pl.DeviceIdType.MESH
SHARDS = 5
KV_CHUNKS = 2
QD_CHUNKS = 4
LOG2E = math.log2(math.e)
NT = (((1,), (1,)), ((), ()))
NN = (((1,), (0,)), ((), ()))


def dot(lhs, rhs, dims):
    return lax.dot_general(lhs, rhs, dims, preferred_element_type=jnp.float32)


def backward_kernel(sizes, q_hbm, k_hbm, v_hbm, o_hbm, do_hbm, lse_hbm, cu_hbm, dq_out, dkv_out,
                    kv_s, kv_w, qd_s, qd_w, ld_s, ld_w, qd_via, ld_via, o_buf, lse_buf, cu_buf, starts, key_t, dq_t, dk_acc, dv_acc, dq_fin, dkv_fin,
                    load_sem, guest_send, guest_recv, fwd_send, fwd_recv, right_send, right_recv, left_send, left_recv, via_recv, back_send, back_recv):
    outer, inner, rows, heads, head = sizes
    group = outer * inner
    pairs = group // 2
    half = pairs // outer
    scale = head ** -0.5
    flat = rows * heads
    k_part = rows // KV_CHUNKS
    lanes = flat // QD_CHUNKS
    span = rows // QD_CHUNKS
    bounds = cu_buf.shape[1]
    rank = lax.axis_index("cpo") * inner + lax.axis_index("cp")

    def resident(pair):
        return (pair + pair // half + 1) % 2

    def host(pair):
        return 2 * pair + resident(pair)

    def helper(pair):
        return (host(pair) + inner) % group

    def visitor(pair):
        return 2 * pair + 1 - resident(pair)

    is_host = rank % 2 == resident(rank // 2)
    is_helper = rank % 2 != resident(rank // 2)
    pair = jnp.where(is_host, rank // 2, ((rank + inner) % group) // 2)
    res = resident(pair)
    gst = 1 - res
    guest = visitor(pair)
    mine = rank // 2
    side = rank % 2
    own = jnp.where(is_host, res, 2)
    prev_res, next_res = resident(pair - 1), resident(pair + 1)
    has_prev, has_prev2 = pair >= 1, pair >= 2
    has_next, has_next2 = pair + 1 < pairs, pair + 2 < pairs
    my_host = host(mine)

    is_carrier = is_helper & (mine == half - 1)
    goes_left1 = is_helper & (mine == half)
    goes_left2 = is_helper & (mine == half + 1)
    before_cut, at_cut, past_cut, past_cut2 = pair == half - 2, pair == half - 1, pair == half, pair == half + 1

    def device(index):
        return (0, index // inner, index % inner)

    def remote(source, target, send, recv, index):
        return pltpu.make_async_remote_copy(src_ref=source, dst_ref=target, send_sem=send, recv_sem=recv,
                                            device_id=device(index), device_id_type=MESH)

    loads = [
        pltpu.make_async_copy(k_hbm, kv_s.at[own, 0], load_sem.at[0]),
        pltpu.make_async_copy(v_hbm, kv_s.at[own, 1], load_sem.at[1]),
        pltpu.make_async_copy(q_hbm, qd_s.at[own, 0], load_sem.at[2]),
        pltpu.make_async_copy(do_hbm, qd_s.at[own, 1], load_sem.at[3]),
        pltpu.make_async_copy(o_hbm, o_buf, load_sem.at[4]),
        pltpu.make_async_copy(lse_hbm, lse_buf, load_sem.at[5]),
        pltpu.make_async_copy(cu_hbm, cu_buf, load_sem.at[6]),
    ]
    for load in loads:
        load.start()

    barrier = pltpu.get_barrier_semaphore()
    for known, peer in (
        (is_host, guest), (is_helper, host(pair)), (is_helper, my_host), (is_helper, (my_host + inner) % group), (is_host, helper(pair)),
        (is_host & has_prev & ~past_cut, host(pair - 1)), (is_host & has_prev2 & ~past_cut & ~past_cut2, host(pair - 2)),
        (is_helper & has_next & ~at_cut, host(pair + 1)), (is_helper & has_next2 & ~at_cut & ~before_cut, host(pair + 2)),
        (is_carrier, host(half - 2)), (is_host & (past_cut | past_cut2), visitor(half - 1)),
        (is_helper & at_cut, visitor(half)), (is_helper & at_cut, visitor(half + 1)),
        (is_helper & before_cut, visitor(half)),
    ):
        @pl.when(known)
        def _():
            pl.semaphore_signal(barrier, inc=1, device_id=device(peer), device_id_type=MESH)

    arrivals = jnp.where(is_host, 2, 3)
    for known, count in (
        (is_host & has_next & ~at_cut, 1), (is_host & has_next2 & ~at_cut & ~before_cut, 1),
        (is_host & has_prev & ~past_cut, 1), (is_host & has_prev2 & ~past_cut & ~past_cut2, 1),
        (is_host & before_cut, 1), (is_carrier, 2), (goes_left1, 2), (goes_left2, 1),
    ):
        arrivals = arrivals + jnp.where(known, count, 0)
    for load in loads:
        load.wait()

    row_id = lax.broadcasted_iota(jnp.int32, (head, heads * head), 0)
    lane_id = lax.broadcasted_iota(jnp.int32, (head, heads * head), 1)
    for part in range(rows // head):
        piece = slice(part * head, (part + 1) * head)
        wide = jnp.zeros((head, heads * head), jnp.float32)
        for g in range(heads):
            column_g = jnp.broadcast_to(lse_buf[g:g + 1, piece], (head, head)).T
            wide = jnp.where(lane_id == row_id * heads + g, jnp.concatenate([column_g] * heads, axis=1), wide)
        ld_s[own, 0:1, part * heads * head:(part + 1) * heads * head] = jnp.sum(wide, axis=0, keepdims=True) * LOG2E
    for part in range(flat // head):
        piece = slice(part * head, (part + 1) * head)
        prod = qd_s[own, 1, piece, :].astype(jnp.float32) * o_buf[piece, :].astype(jnp.float32)
        ld_s[own, 1:2, piece] = jnp.sum(prod.T, axis=0, keepdims=True)

    pl.semaphore_wait(barrier, arrivals)

    def kv_rows(chunk):
        return pl.ds(chunk * k_part, k_part)

    def qd_rows(chunk):
        if isinstance(chunk, int):
            return pl.ds(chunk * lanes, lanes)
        return pl.ds(pl.multiple_of(chunk * lanes, lanes), lanes)

    LD = KV_CHUNKS + QD_CHUNKS

    place = jnp.where(is_host, gst, rank % 2)

    def guest_kv(chunk):
        part = kv_rows(chunk)
        return remote(kv_s.at[2, :, part], kv_s.at[place, :, part], guest_send.at[chunk], guest_recv.at[chunk], my_host)

    def guest_qd(chunk):
        part = qd_rows(chunk)
        return remote(qd_s.at[2, :, part], qd_s.at[place, :, part], guest_send.at[KV_CHUNKS + chunk], guest_recv.at[KV_CHUNKS + chunk], my_host)

    def guest_ld():
        return remote(ld_s.at[2], ld_s.at[place], guest_send.at[LD], guest_recv.at[LD], my_host)

    def fwd_kv(slot, chunk):
        part = kv_rows(chunk)
        return remote(kv_s.at[slot, :, part], kv_s.at[slot, :, part], fwd_send.at[slot, chunk], fwd_recv.at[slot, chunk], helper(pair))

    def fwd_qd(slot, chunk):
        part = qd_rows(chunk)
        return remote(qd_s.at[slot, :, part], qd_s.at[slot, :, part], fwd_send.at[slot, KV_CHUNKS + chunk], fwd_recv.at[slot, KV_CHUNKS + chunk], helper(pair))

    def fwd_ld(slot):
        return remote(ld_s.at[slot], ld_s.at[slot], fwd_send.at[slot, LD], fwd_recv.at[slot, LD], helper(pair))

    def right1(slot, chunk):
        part = kv_rows(chunk)
        to = jnp.where(at_cut, guest, host(pair + 1))
        return remote(kv_s.at[slot, :, part], kv_w.at[slot, :, part], right_send.at[slot, chunk], right_recv.at[slot, chunk], to)

    def right2(chunk):
        part = kv_rows(chunk)
        to = jnp.where(before_cut, visitor(half - 1), host(pair + 2))
        return remote(kv_s.at[1, :, part], kv_w.at[2, :, part], right_send.at[2, chunk], right_recv.at[2, chunk], to)

    def carry1(slot, chunk):
        part = kv_rows(chunk)
        source = kv_s.at[2, :, part] if slot == 1 else kv_w.at[slot, :, part]
        return remote(source, kv_w.at[slot, :, part], right_send.at[slot, chunk], right_recv.at[slot, chunk], host(half))

    def carry2(chunk):
        part = kv_rows(chunk)
        return remote(kv_s.at[2, :, part], kv_w.at[2, :, part], left_send.at[0, chunk], right_recv.at[2, chunk], host(half + 1))

    def left1(slot, chunk, source=None, to=None):
        part = qd_rows(chunk)
        source, to = (slot, helper(pair - 1)) if source is None else (source, to)
        return remote(qd_s.at[source, :, part], qd_w.at[slot, :, part], left_send.at[slot, chunk], left_recv.at[slot, chunk], to)

    def left2(chunk, source=0, to=None):
        part = qd_rows(chunk)
        to = helper(pair - 2) if to is None else to
        return remote(qd_s.at[source, :, part], qd_w.at[2, :, part], left_send.at[2, chunk], left_recv.at[2, chunk], to)

    def left1_ld(slot, source=None, to=None):
        source, to = (slot, helper(pair - 1)) if source is None else (source, to)
        return remote(ld_s.at[source], ld_w.at[slot], left_send.at[slot, QD_CHUNKS], left_recv.at[slot, QD_CHUNKS], to)

    def left2_ld(source=0, to=None):
        to = helper(pair - 2) if to is None else to
        return remote(ld_s.at[source], ld_w.at[2], left_send.at[2, QD_CHUNKS], left_recv.at[2, QD_CHUNKS], to)

    def over_qd(chunk):
        part = qd_rows(chunk)
        return remote(qd_s.at[0, :, part], qd_via.at[:, part], left_send.at[0, chunk], via_recv.at[chunk], visitor(half))

    def over_ld():
        return remote(ld_s.at[0], ld_via, left_send.at[0, QD_CHUNKS], via_recv.at[QD_CHUNKS], visitor(half))

    def relay_qd(chunk):
        part = qd_rows(chunk)
        return remote(qd_via.at[:, part], qd_w.at[2, :, part], left_send.at[0, chunk], left_recv.at[2, chunk], helper(half - 2))

    def relay_qd1(chunk):
        part = qd_rows(chunk)
        return remote(qd_via.at[:, part], qd_w.at[0, :, part], left_send.at[2, chunk], left_recv.at[0, chunk], helper(half - 1))

    def relay_ld1():
        return remote(ld_via, ld_w.at[0], left_send.at[0, QD_CHUNKS], left_recv.at[0, QD_CHUNKS], helper(half - 1))

    def relay_ld2():
        return remote(ld_via, ld_w.at[2], left_send.at[2, QD_CHUNKS], left_recv.at[2, QD_CHUNKS], helper(half - 2))

    def back_dq():
        return remote(dq_fin.at[gst], dq_out, back_send.at[0], back_recv.at[0], guest)

    def back_dkv(slot, part, index, target):
        part_rows = pl.ds(part * (rows // 2), rows // 2)
        return remote(dkv_fin.at[slot, :, part_rows], dkv_out.at[:, part_rows], back_send.at[index + part], back_recv.at[1 + part], target)

    def when(cond, *starts_of):
        @pl.when(cond)
        def _():
            for item in starts_of:
                item().start()

    sends_right1 = is_host & has_next
    sends_right2 = is_host & has_next2 & (res == 1) & ~at_cut
    sends_left1 = is_host & has_prev & ~past_cut
    sends_left2 = is_host & has_prev2 & (res == 0) & ~past_cut & ~past_cut2
    waits_left2 = (pair // half) % 2 == res
    for chunk in range(KV_CHUNKS):
        when(is_helper, lambda: guest_kv(chunk))
        when(sends_right1, lambda: right1(res, chunk))
        when(is_host, lambda: fwd_kv(res, chunk))
        when(sends_right2, lambda: right2(chunk))
    when(is_carrier, *[lambda chunk=chunk: carry1(1, chunk) for chunk in range(KV_CHUNKS)])
    when(is_helper, guest_ld)
    when(is_host, lambda: fwd_ld(res))
    when(sends_left1, lambda: left1_ld(res))
    when(sends_left2, left2_ld)
    for chunk in range(QD_CHUNKS):
        when(is_helper & ~past_cut & ~at_cut, lambda: guest_qd(chunk))
        when(sends_left1, lambda: left1(res, chunk))
        when(is_host, lambda: fwd_qd(res, chunk))
        when(sends_left2 if chunk < QD_CHUNKS // 2 else sends_left2 & ~waits_left2, lambda: left2(chunk))
    when(is_carrier, *[lambda chunk=chunk: carry2(chunk) for chunk in range(KV_CHUNKS)])
    when(is_host & past_cut, over_ld, *[lambda chunk=chunk: over_qd(chunk) for chunk in range(QD_CHUNKS)])

    first = (pair * (2 * rows)).astype(jnp.float32)
    cuts = cu_buf[...].astype(jnp.float32)
    cut_cols = []
    for base in range(0, bounds, head):
        width = min(head, bounds - base)
        row = cuts[:, base:base + width]
        if width < head:
            row = jnp.concatenate([row, jnp.zeros((1, head - width), jnp.float32)], axis=1)
        cut_cols.append(jnp.broadcast_to(row, (head, head)).T - first)
    lane = lax.broadcasted_iota(jnp.int32, (1, head), 1)

    def fill_starts(step, _):
        lane_base = pl.multiple_of((step % (flat // head)) * head, head)
        shard = step // (flat // head)
        token = ((lane + lane_base) // heads + shard * rows).astype(jnp.float32)
        best = jnp.full((head, head), -1e9, jnp.float32)
        for col in cut_cols:
            best = jnp.maximum(best, jnp.where(col <= token, col, -1e9))
        starts[shard, :, pl.ds(lane_base, head)] = jnp.max(best, axis=0, keepdims=True)
        return 0

    lax.fori_loop(0, 2 * (flat // head), fill_starts, 0)

    def directs():
        out = [(goes_left1, left1_ld(side, 2, helper(mine - 1))), (goes_left2, left2_ld(2, helper(mine - 2)))]
        for chunk in range(QD_CHUNKS):
            out.append((goes_left1, left1(side, chunk, 2, helper(mine - 1))))
            out.append((goes_left2, left2(chunk, 2, helper(mine - 2))))
        return out

    @pl.when(goes_left1)
    def _():
        left1_ld(side, 2, helper(mine - 1)).start()
        for chunk in range(QD_CHUNKS):
            left1(side, chunk, 2, helper(mine - 1)).start()

    def scores(kv, key_rows, key_off, qd, ld, part, start, token_off):
        keys, vals = kv[0, key_rows, :], kv[1, key_rows, :]
        qry, dout = qd[0, part, :], qd[1, part, :]
        score = dot(keys, qry, NT)
        grad = dot(vals, dout, NT)
        lse, row_dot = ld[0:1, part], ld[1:2, part]
        key_pos = lax.broadcasted_iota(jnp.int32, score.shape, 0).astype(jnp.float32)
        keep = key_pos >= start[:, part] - key_off
        if token_off is not None:
            token = lax.broadcasted_iota(jnp.int32, (1, lanes), 1) // heads + token_off
            keep = keep & (key_pos <= token.astype(jnp.float32))
        prob = jnp.where(keep, jnp.exp2(score * (scale * LOG2E) - lse), 0.0)
        dsc = (prob * (grad - row_dot)).astype(jnp.bfloat16)
        return prob, dsc, qry, dout

    def q_tile(kv, key_slot, k_from, k_to, key_off, q_slot, chunk, token_off=None):
        part, key_rows = qd_rows(chunk), pl.ds(k_from, k_to - k_from)
        _, dsc, _, _ = scores(kv, key_rows, key_off + k_from, qd_s.at[q_slot], ld_s.at[q_slot], part, starts.at[q_slot], token_off)
        dq_t[q_slot, :, part] += dot(key_t[key_slot, :, k_from:k_to], dsc, NN)

    def k_tile(k_slot, k_from, k_to, qd, ld, q_shard, chunk, token_off=None):
        part, key_rows = qd_rows(chunk), pl.ds(k_from, k_to - k_from)
        key_off = (k_slot * rows + k_from) * 1.0
        prob, dsc, qry, dout = scores(kv_s.at[k_slot], key_rows, key_off, qd, ld, part, starts.at[q_shard], token_off)
        dv_acc[k_slot, key_rows, :] += dot(prob.astype(jnp.bfloat16), dout, NN)
        dk_acc[k_slot, key_rows, :] += dot(dsc, qry, NN)

    def finish_dq(slot, target):
        for part in range(flat // head):
            piece = slice(part * head, (part + 1) * head)
            target[piece, :] = (scale * dq_t[slot, :, piece].T).astype(jnp.bfloat16)

    def finish_dkv(slot, part):
        part_rows = slice(part * (rows // 2), (part + 1) * (rows // 2))
        dkv_fin[slot, 0, part_rows, :] = (scale * dk_acc[slot, part_rows, :]).astype(jnp.bfloat16)
        dkv_fin[slot, 1, part_rows, :] = dv_acc[slot, part_rows, :].astype(jnp.bfloat16)

    @pl.when(is_host)
    def _():
        dq_t[...] = jnp.zeros_like(dq_t)

        relays_right1 = has_next & ~at_cut
        relays_right2 = has_next2 & (gst == 1) & ~at_cut
        relays_left1 = has_prev & ~past_cut
        relays_left2 = has_prev2 & (gst == 0) & ~past_cut & ~past_cut2

        def diagonal(slot, chunk):
            q_tile(kv_s.at[slot], slot, 0, (chunk + 1) * span, slot * rows * 1.0, slot, chunk, chunk * span)

        key_t[res] = kv_s[res, 0, :, :].T
        for chunk in range(QD_CHUNKS):
            diagonal(res, chunk)
        for chunk in range(KV_CHUNKS):
            guest_kv(chunk).wait_recv()
            fwd_kv(gst, chunk).start()
            when(relays_right2, lambda: right2(chunk))
            when(relays_right1 & ~has_prev, lambda: right1(gst, chunk))
        guest_ld().wait_recv()
        fwd_ld(gst).start()
        when(relays_left1, lambda: left1_ld(gst))
        when(relays_left2, left2_ld)
        key_t[gst] = kv_s[gst, 0, :, :].T
        soon = jnp.where(past_cut, 1 - prev_res, prev_res)
        prev_off = (soon - 2) * rows * 1.0
        late_off = (-1 - soon) * rows * 1.0

        def early_keys():
            for chunk in range(KV_CHUNKS):
                right1(soon, chunk).wait_recv()
            key_t[2] = kv_w[soon, 0, :, :].T

        def early_tiles(chunk):
            q_tile(kv_w.at[soon], 2, 0, rows, prev_off, res, chunk)
            q_tile(kv_w.at[soon], 2, 0, rows, prev_off, gst, chunk)

        for chunk in range(QD_CHUNKS):
            guest_qd(chunk).wait_recv()
            when(relays_left1 & has_next, lambda: left1(gst, chunk))
            fwd_qd(gst, chunk).start()
            when(relays_left2 & ~waits_left2, lambda: left2(chunk))
            diagonal(gst, chunk)
            q_tile(kv_s.at[0], 0, 0, rows, 0.0, 1, chunk)

            @pl.when(has_prev & ~past_cut)
            def _():
                if chunk == 0:
                    early_keys()
                early_tiles(chunk)

        for chunk in range(KV_CHUNKS):
            when(relays_right1 & has_prev, lambda: right1(gst, chunk))
        @pl.when(past_cut)
        def _():
            early_keys()

            def both(chunk, _):
                early_tiles(chunk)
                return 0

            lax.fori_loop(0, QD_CHUNKS, both, 0)

        for chunk in range(QD_CHUNKS):
            when((relays_left2 | sends_left2 if chunk >= QD_CHUNKS // 2 else relays_left2) & waits_left2, lambda: left2(chunk))

        def far_keys():
            for chunk in range(KV_CHUNKS):
                right2(chunk).wait_recv()
            key_t[2] = kv_w[2, 0, :, :].T
            for chunk in range(QD_CHUNKS):
                q_tile(kv_w.at[2], 2, chunk * span, rows, -3.0 * rows, 0, chunk)

        @pl.when(has_prev2 & ~past_cut)
        def _():
            far_keys()

        for chunk in range(QD_CHUNKS):
            when(relays_left1 & ~has_next, lambda: left1(gst, chunk))

        def late_keys(slot, part, step):
            @pl.when(has_prev)
            def _():
                for index in range(2):
                    q_tile(kv_w.at[1 - soon], 2, part * k_part, (part + 1) * k_part, late_off, slot, 2 * step + index)

        for chunk in range(KV_CHUNKS):
            @pl.when(has_prev)
            def _():
                right1(1 - soon, chunk).wait_recv()
                key_t[2, :, chunk * k_part:(chunk + 1) * k_part] = kv_w[1 - soon, 0, chunk * k_part:(chunk + 1) * k_part, :].T

            late_keys(gst, chunk, 0)
            late_keys(gst, chunk, 1)
            if chunk == KV_CHUNKS - 1:
                finish_dq(gst, dq_fin.at[gst])
            late_keys(res, chunk, 0)
            if chunk == KV_CHUNKS - 1:
                back_dq().start()
            late_keys(res, chunk, 1)

        @pl.when(past_cut)
        def _():
            far_keys()

        finish_dq(res, dq_out)

        for chunk in range(KV_CHUNKS):
            fwd_kv(res, chunk).wait_send()
            fwd_kv(gst, chunk).wait_send()
        for chunk in range(QD_CHUNKS):
            fwd_qd(res, chunk).wait_send()
            fwd_qd(gst, chunk).wait_send()
        fwd_ld(res).wait_send()
        fwd_ld(gst).wait_send()

        @pl.when(has_next)
        def _():
            for chunk in range(KV_CHUNKS):
                right1(res, chunk).wait_send()

        @pl.when(relays_right1)
        def _():
            for chunk in range(KV_CHUNKS):
                right1(gst, chunk).wait_send()

        @pl.when(sends_right2 | relays_right2)
        def _():
            for chunk in range(KV_CHUNKS):
                right2(chunk).wait_send()

        @pl.when(sends_left1)
        def _():
            for slot in range(2):
                for chunk in range(QD_CHUNKS):
                    left1(slot, chunk).wait_send()
                left1_ld(slot).wait_send()

        @pl.when(past_cut)
        def _():
            over_ld().wait_send()
            for chunk in range(QD_CHUNKS):
                over_qd(chunk).wait_send()

        @pl.when(sends_left2 | relays_left2)
        def _():
            for chunk in range(QD_CHUNKS):
                left2(chunk).wait_send()
            left2_ld().wait_send()

        back_dq().wait_send()
        for part in range(2):
            back_dkv(0, part, 1, guest).wait_recv()

    @pl.when(is_helper)
    def _():
        lax.fori_loop(2 * (flat // head), SHARDS * (flat // head), fill_starts, 0)
        dk_acc[...] = jnp.zeros_like(dk_acc)
        dv_acc[...] = jnp.zeros_like(dv_acc)

        def diagonal(slot, chunk):
            k_tile(slot, 0, (chunk + 1) * span, qd_s.at[slot], ld_s.at[slot], slot, chunk, chunk * span)

        def carry(slot):
            @pl.when(is_carrier)
            def _():
                for chunk in range(KV_CHUNKS):
                    carry1(slot, chunk).wait_recv()
                    carry1(slot, chunk).start()

        carry(0)
        for chunk in range(KV_CHUNKS):
            fwd_kv(res, chunk).wait_recv()
        fwd_ld(res).wait_recv()
        for chunk in range(QD_CHUNKS):
            fwd_qd(res, chunk).wait_recv()
            diagonal(res, chunk)
        for chunk in range(QD_CHUNKS):
            when(past_cut | at_cut, lambda: guest_qd(chunk))
        carry(2)
        for chunk in range(KV_CHUNKS):
            fwd_kv(gst, chunk).wait_recv()
        fwd_ld(gst).wait_recv()

        def next_queries(slot, chunk):
            left1(slot, chunk).wait_recv()
            k_tile(res, 0, rows, qd_w.at[slot], ld_w.at[slot], slot + 2, chunk)
            k_tile(gst, 0, rows, qd_w.at[slot], ld_w.at[slot], slot + 2, chunk)

        soon_next = jnp.where(at_cut, 1 - next_res, next_res)

        @pl.when(has_next & ~at_cut)
        def _():
            left1_ld(soon_next).wait_recv()

        @pl.when(goes_left1)
        def _():
            over_ld().wait_recv()
            relay_ld1().start()
            relay_ld2().start()
            for chunk in range(QD_CHUNKS):
                over_qd(chunk).wait_recv()
                relay_qd1(chunk).start()
                relay_qd(chunk).start()

        for chunk in range(QD_CHUNKS):
            @pl.when(has_next & ~at_cut)
            def _():
                next_queries(soon_next, chunk)

            fwd_qd(gst, chunk).wait_recv()
            diagonal(gst, chunk)
            k_tile(0, 0, rows, qd_s.at[1], ld_s.at[1], 1, chunk)
            if chunk == 0:
                @pl.when(goes_left2)
                def _():
                    left2_ld(2, helper(mine - 2)).start()
                    for far in range(QD_CHUNKS):
                        left2(far, 2, helper(mine - 2)).start()

        def all_queries(slot):
            left1_ld(slot).wait_recv()

            def one(chunk, _):
                next_queries(slot, chunk)
                return 0

            lax.fori_loop(0, QD_CHUNKS, one, 0)

        @pl.when(at_cut)
        def _():
            all_queries(soon_next)

        @pl.when(has_next)
        def _():
            all_queries(1 - soon_next)


        @pl.when(gst == 0)
        def _():
            finish_dkv(0, 0)
            finish_dkv(0, 1)

        for part in range(2):
            @pl.when(has_next2)
            def _():
                if part == 0:
                    left2_ld().wait_recv()
                for chunk in range(part * QD_CHUNKS // 2, (part + 1) * QD_CHUNKS // 2):
                    left2(chunk).wait_recv()
                    k_tile(1, chunk * span, rows, qd_w.at[2], ld_w.at[2], 4, chunk)

            finish_dkv(1, part)

            @pl.when(gst == 1)
            def _():
                finish_dkv(0, part)
                back_dkv(1, part, 1, guest).start()
                back_dkv(0, part, 3, host(pair)).start()

            @pl.when(gst == 0)
            def _():
                if part == 0:
                    back_dkv(0, 0, 1, guest).start()
                    back_dkv(0, 1, 1, guest).start()
                back_dkv(1, part, 3, host(pair)).start()

        @pl.when(goes_left1)
        def _():
            relay_ld1().wait_send()
            relay_ld2().wait_send()
            for chunk in range(QD_CHUNKS):
                relay_qd1(chunk).wait_send()
                relay_qd(chunk).wait_send()

        @pl.when(is_carrier)
        def _():
            for chunk in range(KV_CHUNKS):
                for slot in range(3):
                    carry1(slot, chunk).wait_send()
                carry2(chunk).wait_send()

        for chunk in range(KV_CHUNKS):
            guest_kv(chunk).wait_send()
        for chunk in range(QD_CHUNKS):
            guest_qd(chunk).wait_send()
        guest_ld().wait_send()
        for cond, copy in directs():
            @pl.when(cond)
            def _():
                copy.wait_send()

        for part in range(2):
            back_dkv(gst, part, 1, guest).wait_send()
            back_dkv(res, part, 3, host(pair)).wait_send()
            back_dkv(0, part, 1, guest).wait_recv()
        back_dq().wait_recv()


def store_kernel(dq_in, dkv_in, dq_hbm, dk_hbm, dv_hbm, sem):
    copies = [pltpu.make_async_copy(source, target, sem.at[index])
              for index, (source, target) in enumerate(((dq_in, dq_hbm), (dkv_in.at[0], dk_hbm), (dkv_in.at[1], dv_hbm)))]
    for copy in copies:
        copy.start()
    for copy in copies:
        copy.wait()


def solution(mesh):
    outer, inner = mesh.shape["cpo"], mesh.shape["cp"]

    def local(queries, keys, values, attn_out, logsumexp, d_out, cu_seqlens):
        rows, heads, head = queries.shape
        flat = rows * heads
        low, full = jnp.bfloat16, jnp.float32
        any_spec = pl.BlockSpec(memory_space=pl.ANY)
        vmem_spec = pl.BlockSpec(memory_space=pltpu.VMEM)
        dma = pltpu.SemaphoreType.DMA
        moves = KV_CHUNKS + QD_CHUNKS + 1
        grads = pl.pallas_call(
            functools.partial(backward_kernel, (outer, inner, rows, heads, head)),
            out_shape=(pltpu.VMEM((flat, head), low), pltpu.VMEM((2, rows, head), low)),
            in_specs=[any_spec] * 7,
            out_specs=(vmem_spec,) * 2,
            scratch_shapes=[
                pltpu.VMEM((3, 2, rows, head), low), pltpu.VMEM((3, 2, rows, head), low),
                pltpu.VMEM((3, 2, flat, head), low), pltpu.VMEM((3, 2, flat, head), low),
                pltpu.VMEM((3, 2, flat), full), pltpu.VMEM((3, 2, flat), full), pltpu.VMEM((2, flat, head), low), pltpu.VMEM((2, flat), full),
                pltpu.VMEM((flat, head), low), pltpu.VMEM((heads, rows), full), pltpu.VMEM((1, cu_seqlens.shape[0]), jnp.int32),
                pltpu.VMEM((SHARDS, 1, flat), full), pltpu.VMEM((3, head, rows), low),
                pltpu.VMEM((2, head, flat), full), pltpu.VMEM((2, rows, head), full), pltpu.VMEM((2, rows, head), full),
                pltpu.VMEM((2, flat, head), low), pltpu.VMEM((2, 2, rows, head), low),
                dma((7,)), dma((moves,)), dma((moves,)), dma((2, moves)), dma((2, moves)),
                dma((3, KV_CHUNKS)), dma((3, KV_CHUNKS)), dma((3, QD_CHUNKS + 1)), dma((3, QD_CHUNKS + 1)), dma((QD_CHUNKS + 1,)), dma((5,)), dma((3,)),
            ],
            compiler_params=pltpu.CompilerParams(collective_id=0, has_side_effects=True),
        )(queries.reshape(flat, head), keys, values, attn_out.reshape(flat, head), d_out.reshape(flat, head),
          logsumexp.T, cu_seqlens.reshape(1, -1))
        d_query, d_key, d_value = pl.pallas_call(
            store_kernel,
            out_shape=(jax.ShapeDtypeStruct((flat, head), low), jax.ShapeDtypeStruct((rows, head), low), jax.ShapeDtypeStruct((rows, head), low)),
            in_specs=[vmem_spec] * 2, out_specs=(any_spec,) * 3, scratch_shapes=[dma((3,))],
        )(*(pltpu.with_memory_space_constraint(grad, pltpu.VMEM) for grad in grads))
        return d_query.reshape(rows, heads, head), d_key, d_value

    seq_spec = P(("dp", "cpo", "cp"))
    return jax.shard_map(local, mesh=mesh, in_specs=(seq_spec,) * 6 + (P("dp"),), out_specs=(seq_spec,) * 3, check_vma=False)
```

```python
import functools
import math

import jax
import jax.numpy as jnp
from jax import lax
from jax.experimental import pallas as pl
from jax.experimental.pallas import tpu as pltpu
from jax.sharding import PartitionSpec as P

MESH = pl.DeviceIdType.MESH
SHARDS = 5
KV_CHUNKS = 2
QD_CHUNKS = 4
LOG2E = math.log2(math.e)
NT = (((1,), (1,)), ((), ()))
NN = (((1,), (0,)), ((), ()))


def dot(lhs, rhs, dims):
    return lax.dot_general(lhs, rhs, dims, preferred_element_type=jnp.float32)


def backward_kernel(sizes, q_hbm, k_hbm, v_hbm, o_hbm, do_hbm, lse_hbm, cu_hbm, dq_out, dkv_out,
                    kv_s, kv_w, qd_s, qd_w, ld_s, ld_w, qd_via, ld_via, o_buf, lse_buf, cu_buf, starts, key_t, dq_t, dk_acc, dv_acc, dq_fin, dkv_fin,
                    load_sem, guest_send, guest_recv, fwd_send, fwd_recv, right_send, right_recv, left_send, left_recv, via_recv, back_send, back_recv):
    outer, inner, rows, heads, head = sizes
    group = outer * inner
    pairs = group // 2
    half = pairs // outer
    scale = head ** -0.5
    flat = rows * heads
    k_part = rows // KV_CHUNKS
    lanes = flat // QD_CHUNKS
    span = rows // QD_CHUNKS
    bounds = cu_buf.shape[1]
    rank = lax.axis_index("cpo") * inner + lax.axis_index("cp")

    def resident(pair):
        return (pair + pair // half + 1) % 2

    def host(pair):
        return 2 * pair + resident(pair)

    def helper(pair):
        return (host(pair) + inner) % group

    def visitor(pair):
        return 2 * pair + 1 - resident(pair)

    is_host = rank % 2 == resident(rank // 2)
    is_helper = rank % 2 != resident(rank // 2)
    pair = jnp.where(is_host, rank // 2, ((rank + inner) % group) // 2)
    res = resident(pair)
    gst = 1 - res
    guest = visitor(pair)
    mine = rank // 2
    side = rank % 2
    own = jnp.where(is_host, res, 2)
    prev_res, next_res = resident(pair - 1), resident(pair + 1)
    has_prev, has_prev2 = pair >= 1, pair >= 2
    has_next, has_next2 = pair + 1 < pairs, pair + 2 < pairs
    my_host = host(mine)

    is_carrier = is_helper & (mine == half - 1)
    goes_left1 = is_helper & (mine == half)
    goes_left2 = is_helper & (mine == half + 1)
    before_cut, at_cut, past_cut, past_cut2 = pair == half - 2, pair == half - 1, pair == half, pair == half + 1

    def device(index):
        return (0, index // inner, index % inner)

    def remote(source, target, send, recv, index):
        return pltpu.make_async_remote_copy(src_ref=source, dst_ref=target, send_sem=send, recv_sem=recv,
                                            device_id=device(index), device_id_type=MESH)

    loads = [
        pltpu.make_async_copy(k_hbm, kv_s.at[own, 0], load_sem.at[0]),
        pltpu.make_async_copy(v_hbm, kv_s.at[own, 1], load_sem.at[1]),
        pltpu.make_async_copy(q_hbm, qd_s.at[own, 0], load_sem.at[2]),
        pltpu.make_async_copy(do_hbm, qd_s.at[own, 1], load_sem.at[3]),
        pltpu.make_async_copy(o_hbm, o_buf, load_sem.at[4]),
        pltpu.make_async_copy(lse_hbm, lse_buf, load_sem.at[5]),
        pltpu.make_async_copy(cu_hbm, cu_buf, load_sem.at[6]),
    ]
    for load in loads:
        load.start()

    barrier = pltpu.get_barrier_semaphore()
    for known, peer in (
        (is_host, guest), (is_helper, host(pair)), (is_helper, my_host), (is_helper, (my_host + inner) % group), (is_host, helper(pair)),
        (is_host & has_prev & ~past_cut, host(pair - 1)), (is_host & has_prev2 & ~past_cut & ~past_cut2, host(pair - 2)),
        (is_helper & has_next & ~at_cut, host(pair + 1)), (is_helper & has_next2 & ~at_cut & ~before_cut, host(pair + 2)),
        (is_carrier, host(half - 2)), (is_host & (past_cut | past_cut2), visitor(half - 1)),
        (is_helper & at_cut, visitor(half)), (is_helper & at_cut, visitor(half + 1)),
        (is_helper & before_cut, visitor(half)),
    ):
        @pl.when(known)
        def _():
            pl.semaphore_signal(barrier, inc=1, device_id=device(peer), device_id_type=MESH)

    arrivals = jnp.where(is_host, 2, 3)
    for known, count in (
        (is_host & has_next & ~at_cut, 1), (is_host & has_next2 & ~at_cut & ~before_cut, 1),
        (is_host & has_prev & ~past_cut, 1), (is_host & has_prev2 & ~past_cut & ~past_cut2, 1),
        (is_host & before_cut, 1), (is_carrier, 2), (goes_left1, 2), (goes_left2, 1),
    ):
        arrivals = arrivals + jnp.where(known, count, 0)
    for load in loads:
        load.wait()

    pl.semaphore_wait(barrier, arrivals)

    def kv_rows(chunk):
        return pl.ds(chunk * k_part, k_part)

    def qd_rows(chunk):
        if isinstance(chunk, int):
            return pl.ds(chunk * lanes, lanes)
        return pl.ds(pl.multiple_of(chunk * lanes, lanes), lanes)

    LD = KV_CHUNKS + QD_CHUNKS

    place = jnp.where(is_host, gst, rank % 2)

    def guest_kv(chunk):
        part = kv_rows(chunk)
        return remote(kv_s.at[2, :, part], kv_s.at[place, :, part], guest_send.at[chunk], guest_recv.at[chunk], my_host)

    def guest_qd(chunk):
        part = qd_rows(chunk)
        return remote(qd_s.at[2, :, part], qd_s.at[place, :, part], guest_send.at[KV_CHUNKS + chunk], guest_recv.at[KV_CHUNKS + chunk], my_host)

    def guest_ld():
        return remote(ld_s.at[2], ld_s.at[place], guest_send.at[LD], guest_recv.at[LD], my_host)

    def fwd_kv(slot, chunk):
        part = kv_rows(chunk)
        return remote(kv_s.at[slot, :, part], kv_s.at[slot, :, part], fwd_send.at[slot, chunk], fwd_recv.at[slot, chunk], helper(pair))

    def fwd_qd(slot, chunk):
        part = qd_rows(chunk)
        return remote(qd_s.at[slot, :, part], qd_s.at[slot, :, part], fwd_send.at[slot, KV_CHUNKS + chunk], fwd_recv.at[slot, KV_CHUNKS + chunk], helper(pair))

    def fwd_ld(slot):
        return remote(ld_s.at[slot], ld_s.at[slot], fwd_send.at[slot, LD], fwd_recv.at[slot, LD], helper(pair))

    def right1(slot, chunk):
        part = kv_rows(chunk)
        to = jnp.where(at_cut, guest, host(pair + 1))
        return remote(kv_s.at[slot, :, part], kv_w.at[slot, :, part], right_send.at[slot, chunk], right_recv.at[slot, chunk], to)

    def right2(chunk):
        part = kv_rows(chunk)
        to = jnp.where(before_cut, visitor(half - 1), host(pair + 2))
        return remote(kv_s.at[1, :, part], kv_w.at[2, :, part], right_send.at[2, chunk], right_recv.at[2, chunk], to)

    def carry1(slot, chunk):
        part = kv_rows(chunk)
        source = kv_s.at[2, :, part] if slot == 1 else kv_w.at[slot, :, part]
        return remote(source, kv_w.at[slot, :, part], right_send.at[slot, chunk], right_recv.at[slot, chunk], host(half))

    def carry2(chunk):
        part = kv_rows(chunk)
        return remote(kv_s.at[2, :, part], kv_w.at[2, :, part], left_send.at[0, chunk], right_recv.at[2, chunk], host(half + 1))

    def left1(slot, chunk, source=None, to=None):
        part = qd_rows(chunk)
        source, to = (slot, helper(pair - 1)) if source is None else (source, to)
        return remote(qd_s.at[source, :, part], qd_w.at[slot, :, part], left_send.at[slot, chunk], left_recv.at[slot, chunk], to)

    def left2(chunk, source=0, to=None):
        part = qd_rows(chunk)
        to = helper(pair - 2) if to is None else to
        return remote(qd_s.at[source, :, part], qd_w.at[2, :, part], left_send.at[2, chunk], left_recv.at[2, chunk], to)

    def left1_ld(slot, source=None, to=None):
        source, to = (slot, helper(pair - 1)) if source is None else (source, to)
        return remote(ld_s.at[source], ld_w.at[slot], left_send.at[slot, QD_CHUNKS], left_recv.at[slot, QD_CHUNKS], to)

    def left2_ld(source=0, to=None):
        to = helper(pair - 2) if to is None else to
        return remote(ld_s.at[source], ld_w.at[2], left_send.at[2, QD_CHUNKS], left_recv.at[2, QD_CHUNKS], to)

    def over_qd(chunk):
        part = qd_rows(chunk)
        return remote(qd_s.at[0, :, part], qd_via.at[:, part], left_send.at[0, chunk], via_recv.at[chunk], visitor(half))

    def over_ld():
        return remote(ld_s.at[0], ld_via, left_send.at[0, QD_CHUNKS], via_recv.at[QD_CHUNKS], visitor(half))

    def relay_qd(chunk):
        part = qd_rows(chunk)
        return remote(qd_via.at[:, part], qd_w.at[2, :, part], left_send.at[0, chunk], left_recv.at[2, chunk], helper(half - 2))

    def relay_qd1(chunk):
        part = qd_rows(chunk)
        return remote(qd_via.at[:, part], qd_w.at[0, :, part], left_send.at[2, chunk], left_recv.at[0, chunk], helper(half - 1))

    def relay_ld1():
        return remote(ld_via, ld_w.at[0], left_send.at[0, QD_CHUNKS], left_recv.at[0, QD_CHUNKS], helper(half - 1))

    def relay_ld2():
        return remote(ld_via, ld_w.at[2], left_send.at[2, QD_CHUNKS], left_recv.at[2, QD_CHUNKS], helper(half - 2))

    def back_dq(part):
        part_rows = pl.ds(part * (flat // 2), flat // 2)
        return remote(dq_fin.at[gst, part_rows], dq_out.at[part_rows], back_send.at[5 * part], back_recv.at[3 * part], guest)

    def back_dkv(slot, part, index, target):
        part_rows = pl.ds(part * (rows // 2), rows // 2)
        return remote(dkv_fin.at[slot, :, part_rows], dkv_out.at[:, part_rows], back_send.at[index + part], back_recv.at[1 + part], target)

    def when(cond, *starts_of):
        @pl.when(cond)
        def _():
            for item in starts_of:
                item().start()

    sends_right1 = is_host & has_next
    sends_right2 = is_host & has_next2 & (res == 1) & ~at_cut
    sends_left1 = is_host & has_prev & ~past_cut
    sends_left2 = is_host & has_prev2 & (res == 0) & ~past_cut & ~past_cut2
    waits_left2 = (pair // half) % 2 == res
    for chunk in range(KV_CHUNKS):
        when(is_helper, lambda: guest_kv(chunk))
        when(sends_right1, lambda: right1(res, chunk))
        when(is_host, lambda: fwd_kv(res, chunk))
        when(sends_right2, lambda: right2(chunk))
    when(is_carrier, *[lambda chunk=chunk: carry1(1, chunk) for chunk in range(KV_CHUNKS)])
    row_id = lax.broadcasted_iota(jnp.int32, (head, heads * head), 0)
    lane_id = lax.broadcasted_iota(jnp.int32, (head, heads * head), 1)
    for part in range(rows // head):
        piece = slice(part * head, (part + 1) * head)
        wide = jnp.zeros((head, heads * head), jnp.float32)
        for g in range(heads):
            column_g = jnp.broadcast_to(lse_buf[g:g + 1, piece], (head, head)).T
            wide = jnp.where(lane_id == row_id * heads + g, jnp.concatenate([column_g] * heads, axis=1), wide)
        ld_s[own, 0:1, part * heads * head:(part + 1) * heads * head] = jnp.sum(wide, axis=0, keepdims=True) * LOG2E
    for part in range(flat // head):
        piece = slice(part * head, (part + 1) * head)
        prod = qd_s[own, 1, piece, :].astype(jnp.float32) * o_buf[piece, :].astype(jnp.float32)
        ld_s[own, 1:2, piece] = jnp.sum(prod.T, axis=0, keepdims=True)

    when(is_helper, guest_ld)
    when(is_host, lambda: fwd_ld(res))
    when(sends_left1, lambda: left1_ld(res))
    when(sends_left2, left2_ld)
    for chunk in range(QD_CHUNKS):
        when(is_helper & ~past_cut & ~at_cut, lambda: guest_qd(chunk))
        when(sends_left1, lambda: left1(res, chunk))
        when(is_host, lambda: fwd_qd(res, chunk))
        when(sends_left2 if chunk < QD_CHUNKS // 2 else sends_left2 & ~waits_left2, lambda: left2(chunk))
    when(is_carrier, *[lambda chunk=chunk: carry2(chunk) for chunk in range(KV_CHUNKS)])
    when(is_host & past_cut, over_ld, *[lambda chunk=chunk: over_qd(chunk) for chunk in range(QD_CHUNKS)])

    first = (pair * (2 * rows)).astype(jnp.float32)
    cuts = cu_buf[...].astype(jnp.float32)
    cut_cols = []
    for base in range(0, bounds, head):
        width = min(head, bounds - base)
        row = cuts[:, base:base + width]
        if width < head:
            row = jnp.concatenate([row, jnp.zeros((1, head - width), jnp.float32)], axis=1)
        cut_cols.append(jnp.broadcast_to(row, (head, head)).T - first)
    lane = lax.broadcasted_iota(jnp.int32, (1, head), 1)

    def fill_starts(step, _):
        lane_base = pl.multiple_of((step % (flat // head)) * head, head)
        shard = step // (flat // head)
        token = ((lane + lane_base) // heads + shard * rows).astype(jnp.float32)
        best = jnp.full((head, head), -1e9, jnp.float32)
        for col in cut_cols:
            best = jnp.maximum(best, jnp.where(col <= token, col, -1e9))
        starts[shard, :, pl.ds(lane_base, head)] = jnp.max(best, axis=0, keepdims=True)
        return 0

    lax.fori_loop(0, 2 * (flat // head), fill_starts, 0)

    def directs():
        out = [(goes_left1, left1_ld(side, 2, helper(mine - 1))), (goes_left2, left2_ld(2, helper(mine - 2)))]
        for chunk in range(QD_CHUNKS):
            out.append((goes_left1, left1(side, chunk, 2, helper(mine - 1))))
            out.append((goes_left2, left2(chunk, 2, helper(mine - 2))))
        return out

    @pl.when(goes_left1)
    def _():
        left1_ld(side, 2, helper(mine - 1)).start()
        for chunk in range(QD_CHUNKS):
            left1(side, chunk, 2, helper(mine - 1)).start()

    def scores(kv, key_rows, key_off, qd, ld, part, start, token_off):
        keys, vals = kv[0, key_rows, :], kv[1, key_rows, :]
        qry, dout = qd[0, part, :], qd[1, part, :]
        score = dot(keys, qry, NT)
        grad = dot(vals, dout, NT)
        lse, row_dot = ld[0:1, part], ld[1:2, part]
        key_pos = lax.broadcasted_iota(jnp.int32, score.shape, 0).astype(jnp.float32)
        keep = key_pos >= start[:, part] - key_off
        if token_off is not None:
            token = lax.broadcasted_iota(jnp.int32, (1, lanes), 1) // heads + token_off
            keep = keep & (key_pos <= token.astype(jnp.float32))
        prob = jnp.where(keep, jnp.exp2(score * (scale * LOG2E) - lse), 0.0)
        dsc = (prob * (grad - row_dot)).astype(jnp.bfloat16)
        return prob, dsc, qry, dout

    def q_tile(kv, key_slot, k_from, k_to, key_off, q_slot, chunk, token_off=None):
        part, key_rows = qd_rows(chunk), pl.ds(k_from, k_to - k_from)
        _, dsc, _, _ = scores(kv, key_rows, key_off + k_from, qd_s.at[q_slot], ld_s.at[q_slot], part, starts.at[q_slot], token_off)
        dq_t[q_slot, :, part] += dot(key_t[key_slot, :, k_from:k_to], dsc, NN)

    def k_tile(k_slot, k_from, k_to, qd, ld, q_shard, chunk, token_off=None):
        part, key_rows = qd_rows(chunk), pl.ds(k_from, k_to - k_from)
        key_off = (k_slot * rows + k_from) * 1.0
        prob, dsc, qry, dout = scores(kv_s.at[k_slot], key_rows, key_off, qd, ld, part, starts.at[q_shard], token_off)
        dv_acc[k_slot, key_rows, :] += dot(prob.astype(jnp.bfloat16), dout, NN)
        dk_acc[k_slot, key_rows, :] += dot(dsc, qry, NN)

    def finish_dq(slot, target, half_rows):
        for part in range(half_rows * flat // head // 2, (half_rows + 1) * flat // head // 2):
            piece = slice(part * head, (part + 1) * head)
            target[piece, :] = (scale * dq_t[slot, :, piece].T).astype(jnp.bfloat16)

    def finish_dkv(slot, part):
        part_rows = slice(part * (rows // 2), (part + 1) * (rows // 2))
        dkv_fin[slot, 0, part_rows, :] = (scale * dk_acc[slot, part_rows, :]).astype(jnp.bfloat16)
        dkv_fin[slot, 1, part_rows, :] = dv_acc[slot, part_rows, :].astype(jnp.bfloat16)

    @pl.when(is_host)
    def _():
        dq_t[...] = jnp.zeros_like(dq_t)

        relays_right1 = has_next & ~at_cut
        relays_right2 = has_next2 & (gst == 1) & ~at_cut
        relays_left1 = has_prev & ~past_cut
        relays_left2 = has_prev2 & (gst == 0) & ~past_cut & ~past_cut2

        def diagonal(slot, chunk):
            q_tile(kv_s.at[slot], slot, 0, (chunk + 1) * span, slot * rows * 1.0, slot, chunk, chunk * span)

        key_t[res] = kv_s[res, 0, :, :].T
        for chunk in range(QD_CHUNKS):
            diagonal(res, chunk)
        for chunk in range(KV_CHUNKS):
            guest_kv(chunk).wait_recv()
            fwd_kv(gst, chunk).start()
            when(relays_right2, lambda: right2(chunk))
            when(relays_right1, lambda: right1(gst, chunk))
        guest_ld().wait_recv()
        fwd_ld(gst).start()
        when(relays_left1, lambda: left1_ld(gst))
        when(relays_left2, left2_ld)
        key_t[gst] = kv_s[gst, 0, :, :].T
        soon = jnp.where(past_cut, 1 - prev_res, prev_res)
        prev_off = (soon - 2) * rows * 1.0
        late_off = (-1 - soon) * rows * 1.0

        def early_keys():
            for chunk in range(KV_CHUNKS):
                right1(soon, chunk).wait_recv()
            key_t[2] = kv_w[soon, 0, :, :].T

        def early_tiles(chunk):
            q_tile(kv_w.at[soon], 2, 0, rows, prev_off, res, chunk)
            q_tile(kv_w.at[soon], 2, 0, rows, prev_off, gst, chunk)

        for chunk in range(QD_CHUNKS):
            guest_qd(chunk).wait_recv()
            when(relays_left1 & has_next, lambda: left1(gst, chunk))
            fwd_qd(gst, chunk).start()
            when(relays_left2 & ~waits_left2, lambda: left2(chunk))
            if chunk >= QD_CHUNKS // 2:
                when(relays_left2 & waits_left2, lambda: left2(chunk - QD_CHUNKS // 2))
                when(sends_left2 & waits_left2, lambda: left2(chunk))
            diagonal(gst, chunk)
            q_tile(kv_s.at[0], 0, 0, rows, 0.0, 1, chunk)

            @pl.when(has_prev & ~past_cut)
            def _():
                if chunk == 0:
                    early_keys()
                early_tiles(chunk)

        for chunk in range(QD_CHUNKS // 2):
            when(relays_left1 & ~has_next, lambda: left1(gst, chunk))
        @pl.when(past_cut)
        def _():
            early_keys()

            def both(chunk, _):
                early_tiles(chunk)
                return 0

            lax.fori_loop(0, QD_CHUNKS, both, 0)

        for chunk in range(QD_CHUNKS // 2, QD_CHUNKS):
            when(relays_left2 & waits_left2, lambda: left2(chunk))

        def far_keys():
            for chunk in range(KV_CHUNKS):
                right2(chunk).wait_recv()
            key_t[2] = kv_w[2, 0, :, :].T
            for chunk in range(QD_CHUNKS):
                q_tile(kv_w.at[2], 2, chunk * span, rows, -3.0 * rows, 0, chunk)

        @pl.when(has_prev2 & ~past_cut)
        def _():
            far_keys()

        for chunk in range(QD_CHUNKS // 2, QD_CHUNKS):
            when(relays_left1 & ~has_next, lambda: left1(gst, chunk))

        def late_keys(slot, part, step):
            @pl.when(has_prev)
            def _():
                for index in range(2):
                    q_tile(kv_w.at[1 - soon], 2, part * k_part, (part + 1) * k_part, late_off, slot, 2 * step + index)

        for chunk in range(KV_CHUNKS):
            @pl.when(has_prev)
            def _():
                right1(1 - soon, chunk).wait_recv()
                key_t[2, :, chunk * k_part:(chunk + 1) * k_part] = kv_w[1 - soon, 0, chunk * k_part:(chunk + 1) * k_part, :].T

            last = chunk == KV_CHUNKS - 1
            late_keys(gst, chunk, 0)
            if last:
                finish_dq(gst, dq_fin.at[gst], 0)
            late_keys(gst, chunk, 1)
            if last:
                back_dq(0).start()
                finish_dq(gst, dq_fin.at[gst], 1)
            late_keys(res, chunk, 0)
            if last:
                back_dq(1).start()
            late_keys(res, chunk, 1)

        @pl.when(past_cut)
        def _():
            far_keys()

        finish_dq(res, dq_out, 0)
        finish_dq(res, dq_out, 1)

        for chunk in range(KV_CHUNKS):
            fwd_kv(res, chunk).wait_send()
            fwd_kv(gst, chunk).wait_send()
        for chunk in range(QD_CHUNKS):
            fwd_qd(res, chunk).wait_send()
            fwd_qd(gst, chunk).wait_send()
        fwd_ld(res).wait_send()
        fwd_ld(gst).wait_send()

        @pl.when(has_next)
        def _():
            for chunk in range(KV_CHUNKS):
                right1(res, chunk).wait_send()

        @pl.when(relays_right1)
        def _():
            for chunk in range(KV_CHUNKS):
                right1(gst, chunk).wait_send()

        @pl.when(sends_right2 | relays_right2)
        def _():
            for chunk in range(KV_CHUNKS):
                right2(chunk).wait_send()

        @pl.when(sends_left1)
        def _():
            for slot in range(2):
                for chunk in range(QD_CHUNKS):
                    left1(slot, chunk).wait_send()
                left1_ld(slot).wait_send()

        @pl.when(past_cut)
        def _():
            over_ld().wait_send()
            for chunk in range(QD_CHUNKS):
                over_qd(chunk).wait_send()

        @pl.when(sends_left2 | relays_left2)
        def _():
            for chunk in range(QD_CHUNKS):
                left2(chunk).wait_send()
            left2_ld().wait_send()

        back_dq(0).wait_send()
        back_dq(1).wait_send()
        for part in range(2):
            back_dkv(0, part, 1, guest).wait_recv()

    @pl.when(is_helper)
    def _():
        lax.fori_loop(2 * (flat // head), SHARDS * (flat // head), fill_starts, 0)
        dk_acc[...] = jnp.zeros_like(dk_acc)
        dv_acc[...] = jnp.zeros_like(dv_acc)

        def diagonal(slot, chunk):
            k_tile(slot, 0, (chunk + 1) * span, qd_s.at[slot], ld_s.at[slot], slot, chunk, chunk * span)

        def carry(slot):
            @pl.when(is_carrier)
            def _():
                for chunk in range(KV_CHUNKS):
                    carry1(slot, chunk).wait_recv()
                    carry1(slot, chunk).start()

        carry(0)
        for chunk in range(KV_CHUNKS):
            fwd_kv(res, chunk).wait_recv()
        fwd_ld(res).wait_recv()
        for chunk in range(QD_CHUNKS):
            fwd_qd(res, chunk).wait_recv()
            diagonal(res, chunk)
        for chunk in range(QD_CHUNKS):
            when(past_cut | at_cut, lambda: guest_qd(chunk))
        carry(2)
        for chunk in range(KV_CHUNKS):
            fwd_kv(gst, chunk).wait_recv()
        fwd_ld(gst).wait_recv()

        def next_queries(slot, chunk):
            left1(slot, chunk).wait_recv()
            k_tile(res, 0, rows, qd_w.at[slot], ld_w.at[slot], slot + 2, chunk)
            k_tile(gst, 0, rows, qd_w.at[slot], ld_w.at[slot], slot + 2, chunk)

        soon_next = jnp.where(at_cut, 1 - next_res, next_res)

        @pl.when(has_next & ~at_cut)
        def _():
            left1_ld(soon_next).wait_recv()

        @pl.when(goes_left1)
        def _():
            over_ld().wait_recv()
            relay_ld1().start()
            relay_ld2().start()
            for chunk in range(QD_CHUNKS):
                over_qd(chunk).wait_recv()
                relay_qd1(chunk).start()
                relay_qd(chunk).start()

        for chunk in range(QD_CHUNKS):
            @pl.when(has_next & ~at_cut)
            def _():
                next_queries(soon_next, chunk)

            fwd_qd(gst, chunk).wait_recv()
            diagonal(gst, chunk)
            k_tile(0, 0, rows, qd_s.at[1], ld_s.at[1], 1, chunk)
            if chunk == 0:
                @pl.when(goes_left2)
                def _():
                    left2_ld(2, helper(mine - 2)).start()
                    for far in range(QD_CHUNKS):
                        left2(far, 2, helper(mine - 2)).start()

        def all_queries(slot):
            left1_ld(slot).wait_recv()

            def one(chunk, _):
                next_queries(slot, chunk)
                return 0

            lax.fori_loop(0, QD_CHUNKS, one, 0)

        @pl.when(at_cut)
        def _():
            all_queries(soon_next)

        late = 1 - soon_next
        is_early = has_next & (gst == 0)

        @pl.when(is_early)
        def _():
            left1_ld(late).wait_recv()
            for chunk in range(QD_CHUNKS):
                left1(late, chunk).wait_recv()
                k_tile(0, chunk * span, rows, qd_w.at[1], ld_w.at[1], 3, chunk)
                if chunk == QD_CHUNKS // 2 - 1:
                    finish_dkv(0, 0)
                k_tile(1, 0, rows, qd_w.at[1], ld_w.at[1], 3, chunk)
                if chunk == QD_CHUNKS // 2 - 1:
                    back_dkv(0, 0, 1, guest).start()

        @pl.when(has_next & ~is_early)
        def _():
            all_queries(late)


        @pl.when(gst == 0)
        def _():
            @pl.when(~is_early)
            def _():
                finish_dkv(0, 0)
                back_dkv(0, 0, 1, guest).start()

            finish_dkv(0, 1)

        for part in range(2):
            @pl.when(has_next2)
            def _():
                if part == 0:
                    left2_ld().wait_recv()
                for chunk in range(part * QD_CHUNKS // 2, (part + 1) * QD_CHUNKS // 2):
                    left2(chunk).wait_recv()
                    k_tile(1, chunk * span, rows, qd_w.at[2], ld_w.at[2], 4, chunk)

            finish_dkv(1, part)

            @pl.when(gst == 1)
            def _():
                finish_dkv(0, part)
                back_dkv(1, part, 1, guest).start()
                back_dkv(0, part, 3, host(pair)).start()

            @pl.when(gst == 0)
            def _():
                if part == 0:
                    back_dkv(0, 1, 1, guest).start()
                back_dkv(1, part, 3, host(pair)).start()

        @pl.when(goes_left1)
        def _():
            relay_ld1().wait_send()
            relay_ld2().wait_send()
            for chunk in range(QD_CHUNKS):
                relay_qd1(chunk).wait_send()
                relay_qd(chunk).wait_send()

        @pl.when(is_carrier)
        def _():
            for chunk in range(KV_CHUNKS):
                for slot in range(3):
                    carry1(slot, chunk).wait_send()
                carry2(chunk).wait_send()

        for chunk in range(KV_CHUNKS):
            guest_kv(chunk).wait_send()
        for chunk in range(QD_CHUNKS):
            guest_qd(chunk).wait_send()
        guest_ld().wait_send()
        for cond, copy in directs():
            @pl.when(cond)
            def _():
                copy.wait_send()

        for part in range(2):
            back_dkv(gst, part, 1, guest).wait_send()
            back_dkv(res, part, 3, host(pair)).wait_send()
            back_dkv(0, part, 1, guest).wait_recv()
        back_dq(0).wait_recv()
        back_dq(1).wait_recv()


def store_kernel(dq_in, dkv_in, dq_hbm, dk_hbm, dv_hbm, sem):
    copies = [pltpu.make_async_copy(source, target, sem.at[index])
              for index, (source, target) in enumerate(((dq_in, dq_hbm), (dkv_in.at[0], dk_hbm), (dkv_in.at[1], dv_hbm)))]
    for copy in copies:
        copy.start()
    for copy in copies:
        copy.wait()


def solution(mesh):
    outer, inner = mesh.shape["cpo"], mesh.shape["cp"]

    def local(queries, keys, values, attn_out, logsumexp, d_out, cu_seqlens):
        rows, heads, head = queries.shape
        flat = rows * heads
        low, full = jnp.bfloat16, jnp.float32
        any_spec = pl.BlockSpec(memory_space=pl.ANY)
        vmem_spec = pl.BlockSpec(memory_space=pltpu.VMEM)
        dma = pltpu.SemaphoreType.DMA
        moves = KV_CHUNKS + QD_CHUNKS + 1
        grads = pl.pallas_call(
            functools.partial(backward_kernel, (outer, inner, rows, heads, head)),
            out_shape=(pltpu.VMEM((flat, head), low), pltpu.VMEM((2, rows, head), low)),
            in_specs=[any_spec] * 7,
            out_specs=(vmem_spec,) * 2,
            scratch_shapes=[
                pltpu.VMEM((3, 2, rows, head), low), pltpu.VMEM((3, 2, rows, head), low),
                pltpu.VMEM((3, 2, flat, head), low), pltpu.VMEM((3, 2, flat, head), low),
                pltpu.VMEM((3, 2, flat), full), pltpu.VMEM((3, 2, flat), full), pltpu.VMEM((2, flat, head), low), pltpu.VMEM((2, flat), full),
                pltpu.VMEM((flat, head), low), pltpu.VMEM((heads, rows), full), pltpu.VMEM((1, cu_seqlens.shape[0]), jnp.int32),
                pltpu.VMEM((SHARDS, 1, flat), full), pltpu.VMEM((3, head, rows), low),
                pltpu.VMEM((2, head, flat), full), pltpu.VMEM((2, rows, head), full), pltpu.VMEM((2, rows, head), full),
                pltpu.VMEM((2, flat, head), low), pltpu.VMEM((2, 2, rows, head), low),
                dma((7,)), dma((moves,)), dma((moves,)), dma((2, moves)), dma((2, moves)),
                dma((3, KV_CHUNKS)), dma((3, KV_CHUNKS)), dma((3, QD_CHUNKS + 1)), dma((3, QD_CHUNKS + 1)), dma((QD_CHUNKS + 1,)), dma((6,)), dma((4,)),
            ],
            compiler_params=pltpu.CompilerParams(collective_id=0, has_side_effects=True),
        )(queries.reshape(flat, head), keys, values, attn_out.reshape(flat, head), d_out.reshape(flat, head),
          logsumexp.T, cu_seqlens.reshape(1, -1))
        d_query, d_key, d_value = pl.pallas_call(
            store_kernel,
            out_shape=(jax.ShapeDtypeStruct((flat, head), low), jax.ShapeDtypeStruct((rows, head), low), jax.ShapeDtypeStruct((rows, head), low)),
            in_specs=[vmem_spec] * 2, out_specs=(any_spec,) * 3, scratch_shapes=[dma((3,))],
        )(*(pltpu.with_memory_space_constraint(grad, pltpu.VMEM) for grad in grads))
        return d_query.reshape(rows, heads, head), d_key, d_value

    seq_spec = P(("dp", "cpo", "cp"))
    return jax.shard_map(local, mesh=mesh, in_specs=(seq_spec,) * 6 + (P("dp"),), out_specs=(seq_spec,) * 3, check_vma=False)
```

```python
import functools
import math

import jax
import jax.numpy as jnp
from jax import lax
from jax.experimental import pallas as pl
from jax.experimental.pallas import tpu as pltpu
from jax.sharding import PartitionSpec as P

MESH = pl.DeviceIdType.MESH
SHARDS = 5
KV_CHUNKS = 2
QD_CHUNKS = 4
LOG2E = math.log2(math.e)
NT = (((1,), (1,)), ((), ()))
NN = (((1,), (0,)), ((), ()))


def dot(lhs, rhs, dims):
    return lax.dot_general(lhs, rhs, dims, preferred_element_type=jnp.float32)


def backward_kernel(sizes, q_hbm, k_hbm, v_hbm, o_hbm, do_hbm, lse_hbm, cu_hbm, dq_out, dkv_out,
                    kv_s, kv_w, qd_s, qd_w, ld_s, ld_w, qd_via, ld_via, o_buf, lse_buf, cu_buf, starts, key_t, dq_t, dk_acc, dv_acc, dq_fin, dkv_fin,
                    load_sem, guest_send, guest_recv, fwd_send, fwd_recv, right_send, right_recv, left_send, left_recv, via_recv, back_send, back_recv):
    outer, inner, rows, heads, head = sizes
    group = outer * inner
    pairs = group // 2
    half = pairs // outer
    scale = head ** -0.5
    flat = rows * heads
    k_part = rows // KV_CHUNKS
    lanes = flat // QD_CHUNKS
    span = rows // QD_CHUNKS
    bounds = cu_buf.shape[1]
    rank = lax.axis_index("cpo") * inner + lax.axis_index("cp")

    def resident(pair):
        return (pair + pair // half + 1) % 2

    def host(pair):
        return 2 * pair + resident(pair)

    def helper(pair):
        return (host(pair) + inner) % group

    def visitor(pair):
        return 2 * pair + 1 - resident(pair)

    is_host = rank % 2 == resident(rank // 2)
    is_helper = rank % 2 != resident(rank // 2)
    pair = jnp.where(is_host, rank // 2, ((rank + inner) % group) // 2)
    res = resident(pair)
    gst = 1 - res
    guest = visitor(pair)
    mine = rank // 2
    side = rank % 2
    own = jnp.where(is_host, res, 2)
    prev_res, next_res = resident(pair - 1), resident(pair + 1)
    has_prev, has_prev2 = pair >= 1, pair >= 2
    has_next, has_next2 = pair + 1 < pairs, pair + 2 < pairs
    my_host = host(mine)

    is_carrier = is_helper & (mine == half - 1)
    goes_left1 = is_helper & (mine == half)
    goes_left2 = is_helper & (mine == half + 1)
    before_cut, at_cut, past_cut, past_cut2 = pair == half - 2, pair == half - 1, pair == half, pair == half + 1

    def device(index):
        return (0, index // inner, index % inner)

    def remote(source, target, send, recv, index):
        return pltpu.make_async_remote_copy(src_ref=source, dst_ref=target, send_sem=send, recv_sem=recv,
                                            device_id=device(index), device_id_type=MESH)

    loads = [
        pltpu.make_async_copy(k_hbm, kv_s.at[own, 0], load_sem.at[0]),
        pltpu.make_async_copy(v_hbm, kv_s.at[own, 1], load_sem.at[1]),
        pltpu.make_async_copy(q_hbm, qd_s.at[own, 0], load_sem.at[2]),
        pltpu.make_async_copy(do_hbm, qd_s.at[own, 1], load_sem.at[3]),
        pltpu.make_async_copy(o_hbm, o_buf, load_sem.at[4]),
        pltpu.make_async_copy(lse_hbm, lse_buf, load_sem.at[5]),
        pltpu.make_async_copy(cu_hbm, cu_buf, load_sem.at[6]),
    ]
    for load in loads:
        load.start()

    barrier = pltpu.get_barrier_semaphore()
    for known, peer in (
        (is_host, guest), (is_helper, host(pair)), (is_helper, my_host), (is_helper, (my_host + inner) % group), (is_host, helper(pair)),
        (is_host & has_prev & ~past_cut, host(pair - 1)), (is_host & has_prev2 & ~past_cut & ~past_cut2, host(pair - 2)),
        (is_helper & has_next & ~at_cut, host(pair + 1)), (is_helper & has_next2 & ~at_cut & ~before_cut, host(pair + 2)),
        (is_host & past_cut, helper(half - 2)), (is_host & (past_cut | past_cut2), visitor(half - 1)),
        (is_helper & at_cut, visitor(half)), (is_helper & at_cut, visitor(half + 1)),
        (is_helper & before_cut, visitor(half)),
    ):
        @pl.when(known)
        def _():
            pl.semaphore_signal(barrier, inc=1, device_id=device(peer), device_id_type=MESH)

    arrivals = jnp.where(is_host, 2, 3)
    for known, count in (
        (is_host & has_next & ~at_cut, 1), (is_host & has_next2 & ~at_cut & ~before_cut, 1),
        (is_host & has_prev & ~past_cut, 1), (is_host & has_prev2 & ~past_cut & ~past_cut2, 1),
        (is_helper & before_cut, 1), (is_carrier, 2), (goes_left1, 2), (goes_left2, 1),
    ):
        arrivals = arrivals + jnp.where(known, count, 0)
    for load in loads:
        load.wait()

    pl.semaphore_wait(barrier, arrivals)

    def kv_rows(chunk):
        return pl.ds(chunk * k_part, k_part)

    def qd_rows(chunk):
        if isinstance(chunk, int):
            return pl.ds(chunk * lanes, lanes)
        return pl.ds(pl.multiple_of(chunk * lanes, lanes), lanes)

    LD = KV_CHUNKS + QD_CHUNKS

    place = jnp.where(is_host, gst, rank % 2)

    def guest_kv(chunk):
        part = kv_rows(chunk)
        return remote(kv_s.at[2, :, part], kv_s.at[place, :, part], guest_send.at[chunk], guest_recv.at[chunk], my_host)

    def guest_qd(chunk):
        part = qd_rows(chunk)
        return remote(qd_s.at[2, :, part], qd_s.at[place, :, part], guest_send.at[KV_CHUNKS + chunk], guest_recv.at[KV_CHUNKS + chunk], my_host)

    def guest_ld():
        return remote(ld_s.at[2], ld_s.at[place], guest_send.at[LD], guest_recv.at[LD], my_host)

    def fwd_kv(slot, chunk):
        part = kv_rows(chunk)
        return remote(kv_s.at[slot, :, part], kv_s.at[slot, :, part], fwd_send.at[slot, chunk], fwd_recv.at[slot, chunk], helper(pair))

    def fwd_qd(slot, chunk):
        part = qd_rows(chunk)
        return remote(qd_s.at[slot, :, part], qd_s.at[slot, :, part], fwd_send.at[slot, KV_CHUNKS + chunk], fwd_recv.at[slot, KV_CHUNKS + chunk], helper(pair))

    def fwd_ld(slot):
        return remote(ld_s.at[slot], ld_s.at[slot], fwd_send.at[slot, LD], fwd_recv.at[slot, LD], helper(pair))

    def right1(slot, chunk):
        part = kv_rows(chunk)
        to = jnp.where(at_cut, guest, host(pair + 1))
        return remote(kv_s.at[slot, :, part], kv_w.at[slot, :, part], right_send.at[slot, chunk], right_recv.at[slot, chunk], to)

    def right2(chunk):
        part = kv_rows(chunk)
        return remote(kv_s.at[1, :, part], kv_w.at[2, :, part], right_send.at[2, chunk], right_recv.at[2, chunk], host(pair + 2))

    def carry1(slot, chunk):
        part = kv_rows(chunk)
        source = kv_s.at[2, :, part] if slot == 1 else kv_w.at[slot, :, part]
        return remote(source, kv_w.at[slot, :, part], right_send.at[slot, chunk], right_recv.at[slot, chunk], host(half))

    def carry2(chunk):
        part = kv_rows(chunk)
        return remote(kv_s.at[2, :, part], kv_w.at[2, :, part], left_send.at[0, chunk], right_recv.at[2, chunk], host(half + 1))

    def left1(slot, chunk, source=None, to=None):
        part = qd_rows(chunk)
        source, to = (slot, helper(pair - 1)) if source is None else (source, to)
        return remote(qd_s.at[source, :, part], qd_w.at[slot, :, part], left_send.at[slot, chunk], left_recv.at[slot, chunk], to)

    def left2(chunk, source=0, to=None):
        part = qd_rows(chunk)
        to = helper(pair - 2) if to is None else to
        return remote(qd_s.at[source, :, part], qd_w.at[2, :, part], left_send.at[2, chunk], left_recv.at[2, chunk], to)

    def left1_ld(slot, source=None, to=None):
        source, to = (slot, helper(pair - 1)) if source is None else (source, to)
        return remote(ld_s.at[source], ld_w.at[slot], left_send.at[slot, QD_CHUNKS], left_recv.at[slot, QD_CHUNKS], to)

    def left2_ld(source=0, to=None):
        to = helper(pair - 2) if to is None else to
        return remote(ld_s.at[source], ld_w.at[2], left_send.at[2, QD_CHUNKS], left_recv.at[2, QD_CHUNKS], to)

    def over_qd(chunk):
        part = qd_rows(chunk)
        return remote(qd_s.at[0, :, part], qd_via.at[:, part], left_send.at[0, chunk], via_recv.at[chunk], visitor(half))

    def over_ld():
        return remote(ld_s.at[0], ld_via, left_send.at[0, QD_CHUNKS], via_recv.at[QD_CHUNKS], visitor(half))

    def relay_qd(chunk):
        part = qd_rows(chunk)
        return remote(qd_via.at[:, part], qd_w.at[2, :, part], left_send.at[0, chunk], left_recv.at[2, chunk], helper(half - 2))

    def relay_qd1(chunk):
        part = qd_rows(chunk)
        return remote(qd_via.at[:, part], qd_w.at[0, :, part], left_send.at[2, chunk], left_recv.at[0, chunk], helper(half - 1))

    def relay_ld1():
        return remote(ld_via, ld_w.at[0], left_send.at[0, QD_CHUNKS], left_recv.at[0, QD_CHUNKS], helper(half - 1))

    def relay_ld2():
        return remote(ld_via, ld_w.at[2], left_send.at[2, QD_CHUNKS], left_recv.at[2, QD_CHUNKS], helper(half - 2))

    def back_dq(part):
        part_rows = pl.ds(part * (flat // 2), flat // 2)
        return remote(dq_fin.at[gst, part_rows], dq_out.at[part_rows], back_send.at[5 * part], back_recv.at[3 * part], guest)

    def back_dkv(slot, part, index, target):
        part_rows = pl.ds(part * (rows // 2), rows // 2)
        return remote(dkv_fin.at[slot, :, part_rows], dkv_out.at[:, part_rows], back_send.at[index + part], back_recv.at[1 + part], target)

    def when(cond, *starts_of):
        @pl.when(cond)
        def _():
            for item in starts_of:
                item().start()

    sends_right1 = is_host & has_next
    sends_right2 = is_host & has_next2 & (res == 1) & ~at_cut & ~before_cut
    sends_left1 = is_host & has_prev & ~past_cut
    sends_left2 = is_host & has_prev2 & (res == 0) & ~past_cut & ~past_cut2
    waits_left2 = (pair // half) % 2 == res
    for chunk in range(KV_CHUNKS):
        when(is_helper, lambda: guest_kv(chunk))
        when(sends_right1, lambda: right1(res, chunk))
        when(is_host, lambda: fwd_kv(res, chunk))
        when(sends_right2, lambda: right2(chunk))
    when(is_carrier, *[lambda chunk=chunk: carry1(1, chunk) for chunk in range(KV_CHUNKS)])
    row_id = lax.broadcasted_iota(jnp.int32, (head, heads * head), 0)
    lane_id = lax.broadcasted_iota(jnp.int32, (head, heads * head), 1)
    for part in range(rows // head):
        piece = slice(part * head, (part + 1) * head)
        wide = jnp.zeros((head, heads * head), jnp.float32)
        for g in range(heads):
            column_g = jnp.broadcast_to(lse_buf[g:g + 1, piece], (head, head)).T
            wide = jnp.where(lane_id == row_id * heads + g, jnp.concatenate([column_g] * heads, axis=1), wide)
        ld_s[own, 0:1, part * heads * head:(part + 1) * heads * head] = jnp.sum(wide, axis=0, keepdims=True) * LOG2E
    for part in range(flat // head):
        piece = slice(part * head, (part + 1) * head)
        prod = qd_s[own, 1, piece, :].astype(jnp.float32) * o_buf[piece, :].astype(jnp.float32)
        ld_s[own, 1:2, piece] = jnp.sum(prod.T, axis=0, keepdims=True)

    when(is_helper, guest_ld)
    when(is_host, lambda: fwd_ld(res))
    when(sends_left1, lambda: left1_ld(res))
    when(sends_left2, left2_ld)
    for chunk in range(QD_CHUNKS):
        when(is_helper & ~past_cut & ~at_cut, lambda: guest_qd(chunk))
        when(sends_left1, lambda: left1(res, chunk))
        when(is_host, lambda: fwd_qd(res, chunk))
        when(sends_left2 if chunk < QD_CHUNKS // 2 else sends_left2 & ~waits_left2, lambda: left2(chunk))
    when(is_carrier, *[lambda chunk=chunk: carry2(chunk) for chunk in range(KV_CHUNKS)])
    when(is_host & past_cut, over_ld, *[lambda chunk=chunk: over_qd(chunk) for chunk in range(QD_CHUNKS)])

    first = (pair * (2 * rows)).astype(jnp.float32)
    cuts = cu_buf[...].astype(jnp.float32)
    cut_cols = []
    for base in range(0, bounds, head):
        width = min(head, bounds - base)
        row = cuts[:, base:base + width]
        if width < head:
            row = jnp.concatenate([row, jnp.zeros((1, head - width), jnp.float32)], axis=1)
        cut_cols.append(jnp.broadcast_to(row, (head, head)).T - first)
    lane = lax.broadcasted_iota(jnp.int32, (1, head), 1)

    def fill_starts(step, _):
        lane_base = pl.multiple_of((step % (flat // head)) * head, head)
        shard = step // (flat // head)
        token = ((lane + lane_base) // heads + shard * rows).astype(jnp.float32)
        best = jnp.full((head, head), -1e9, jnp.float32)
        for col in cut_cols:
            best = jnp.maximum(best, jnp.where(col <= token, col, -1e9))
        starts[shard, :, pl.ds(lane_base, head)] = jnp.max(best, axis=0, keepdims=True)
        return 0

    lax.fori_loop(0, 2 * (flat // head), fill_starts, 0)

    def directs():
        out = [(goes_left1, left1_ld(side, 2, helper(mine - 1))), (goes_left2, left2_ld(2, helper(mine - 2)))]
        for chunk in range(QD_CHUNKS):
            out.append((goes_left1, left1(side, chunk, 2, helper(mine - 1))))
            out.append((goes_left2, left2(chunk, 2, helper(mine - 2))))
        return out

    @pl.when(goes_left1)
    def _():
        left1_ld(side, 2, helper(mine - 1)).start()
        for chunk in range(QD_CHUNKS):
            left1(side, chunk, 2, helper(mine - 1)).start()

    def scores(kv, key_rows, key_off, qd, ld, part, start, token_off):
        keys, vals = kv[0, key_rows, :], kv[1, key_rows, :]
        qry, dout = qd[0, part, :], qd[1, part, :]
        score = dot(keys, qry, NT)
        grad = dot(vals, dout, NT)
        lse, row_dot = ld[0:1, part], ld[1:2, part]
        key_pos = lax.broadcasted_iota(jnp.int32, score.shape, 0).astype(jnp.float32)
        keep = key_pos >= start[:, part] - key_off
        if token_off is not None:
            token = lax.broadcasted_iota(jnp.int32, (1, lanes), 1) // heads + token_off
            keep = keep & (key_pos <= token.astype(jnp.float32))
        prob = jnp.where(keep, jnp.exp2(score * (scale * LOG2E) - lse), 0.0)
        dsc = (prob * (grad - row_dot)).astype(jnp.bfloat16)
        return prob, dsc, qry, dout

    def q_tile(kv, key_slot, k_from, k_to, key_off, q_slot, chunk, token_off=None):
        part, key_rows = qd_rows(chunk), pl.ds(k_from, k_to - k_from)
        _, dsc, _, _ = scores(kv, key_rows, key_off + k_from, qd_s.at[q_slot], ld_s.at[q_slot], part, starts.at[q_slot], token_off)
        dq_t[q_slot, :, part] += dot(key_t[key_slot, :, k_from:k_to], dsc, NN)

    def k_tile(k_slot, k_from, k_to, qd, ld, q_shard, chunk, token_off=None):
        part, key_rows = qd_rows(chunk), pl.ds(k_from, k_to - k_from)
        key_off = (k_slot * rows + k_from) * 1.0
        prob, dsc, qry, dout = scores(kv_s.at[k_slot], key_rows, key_off, qd, ld, part, starts.at[q_shard], token_off)
        dv_acc[k_slot, key_rows, :] += dot(prob.astype(jnp.bfloat16), dout, NN)
        dk_acc[k_slot, key_rows, :] += dot(dsc, qry, NN)

    def finish_dq(slot, target, half_rows):
        for part in range(half_rows * flat // head // 2, (half_rows + 1) * flat // head // 2):
            piece = slice(part * head, (part + 1) * head)
            target[piece, :] = (scale * dq_t[slot, :, piece].T).astype(jnp.bfloat16)

    def finish_dkv(slot, part):
        part_rows = slice(part * (rows // 2), (part + 1) * (rows // 2))
        dkv_fin[slot, 0, part_rows, :] = (scale * dk_acc[slot, part_rows, :]).astype(jnp.bfloat16)
        dkv_fin[slot, 1, part_rows, :] = dv_acc[slot, part_rows, :].astype(jnp.bfloat16)

    @pl.when(is_host)
    def _():
        dq_t[...] = jnp.zeros_like(dq_t)

        relays_right1 = has_next & ~at_cut
        relays_right2 = has_next2 & (gst == 1) & ~at_cut
        relays_left1 = has_prev & ~past_cut
        relays_left2 = has_prev2 & (gst == 0) & ~past_cut & ~past_cut2

        def diagonal(slot, chunk):
            q_tile(kv_s.at[slot], slot, 0, (chunk + 1) * span, slot * rows * 1.0, slot, chunk, chunk * span)

        key_t[res] = kv_s[res, 0, :, :].T
        for chunk in range(QD_CHUNKS):
            diagonal(res, chunk)
        for chunk in range(KV_CHUNKS):
            guest_kv(chunk).wait_recv()
            fwd_kv(gst, chunk).start()
            when(relays_right2, lambda: right2(chunk))
            when(relays_right1, lambda: right1(gst, chunk))
        guest_ld().wait_recv()
        fwd_ld(gst).start()
        when(relays_left1, lambda: left1_ld(gst))
        when(relays_left2, left2_ld)
        key_t[gst] = kv_s[gst, 0, :, :].T
        soon = jnp.where(past_cut, 1 - prev_res, prev_res)
        prev_off = (soon - 2) * rows * 1.0
        late_off = (-1 - soon) * rows * 1.0

        def early_keys():
            for chunk in range(KV_CHUNKS):
                right1(soon, chunk).wait_recv()
            key_t[2] = kv_w[soon, 0, :, :].T

        def early_tiles(chunk):
            q_tile(kv_w.at[soon], 2, 0, rows, prev_off, res, chunk)
            q_tile(kv_w.at[soon], 2, 0, rows, prev_off, gst, chunk)

        for chunk in range(QD_CHUNKS):
            guest_qd(chunk).wait_recv()
            when(relays_left1, lambda: left1(gst, chunk))
            fwd_qd(gst, chunk).start()
            when(relays_left2 & ~waits_left2, lambda: left2(chunk))
            if chunk >= QD_CHUNKS // 2:
                when(relays_left2 & waits_left2, lambda: left2(chunk - QD_CHUNKS // 2))
                when(sends_left2 & waits_left2, lambda: left2(chunk))
            diagonal(gst, chunk)
            q_tile(kv_s.at[0], 0, 0, rows, 0.0, 1, chunk)

            @pl.when(has_prev & ~past_cut)
            def _():
                if chunk == 0:
                    early_keys()
                early_tiles(chunk)

        @pl.when(past_cut)
        def _():
            early_keys()

            for chunk in range(QD_CHUNKS):
                q_tile(kv_w.at[soon], 2, 0, rows, prev_off, gst, chunk)

        for chunk in range(QD_CHUNKS // 2, QD_CHUNKS):
            when(relays_left2 & waits_left2, lambda: left2(chunk))

        def far_keys():
            for chunk in range(KV_CHUNKS):
                right2(chunk).wait_recv()
            key_t[2] = kv_w[2, 0, :, :].T
            for chunk in range(QD_CHUNKS):
                q_tile(kv_w.at[2], 2, chunk * span, rows, -3.0 * rows, 0, chunk)

        @pl.when(has_prev2 & ~past_cut)
        def _():
            far_keys()

        def late_keys(slot, part, step):
            @pl.when(has_prev)
            def _():
                for index in range(2):
                    q_tile(kv_w.at[1 - soon], 2, part * k_part, (part + 1) * k_part, late_off, slot, 2 * step + index)

        for chunk in range(KV_CHUNKS):
            @pl.when(has_prev)
            def _():
                right1(1 - soon, chunk).wait_recv()
                key_t[2, :, chunk * k_part:(chunk + 1) * k_part] = kv_w[1 - soon, 0, chunk * k_part:(chunk + 1) * k_part, :].T

            last = chunk == KV_CHUNKS - 1
            late_keys(gst, chunk, 0)
            if last:
                finish_dq(gst, dq_fin.at[gst], 0)
            late_keys(gst, chunk, 1)
            if last:
                back_dq(0).start()
                finish_dq(gst, dq_fin.at[gst], 1)
            late_keys(res, chunk, 0)
            if last:
                back_dq(1).start()
            late_keys(res, chunk, 1)

        @pl.when(past_cut)
        def _():
            key_t[2] = kv_w[soon, 0, :, :].T
            for chunk in range(QD_CHUNKS):
                q_tile(kv_w.at[soon], 2, 0, rows, prev_off, res, chunk)
            far_keys()

        finish_dq(res, dq_out, 0)
        finish_dq(res, dq_out, 1)

        for chunk in range(KV_CHUNKS):
            fwd_kv(res, chunk).wait_send()
            fwd_kv(gst, chunk).wait_send()
        for chunk in range(QD_CHUNKS):
            fwd_qd(res, chunk).wait_send()
            fwd_qd(gst, chunk).wait_send()
        fwd_ld(res).wait_send()
        fwd_ld(gst).wait_send()

        @pl.when(has_next)
        def _():
            for chunk in range(KV_CHUNKS):
                right1(res, chunk).wait_send()

        @pl.when(relays_right1)
        def _():
            for chunk in range(KV_CHUNKS):
                right1(gst, chunk).wait_send()

        @pl.when(sends_right2 | relays_right2)
        def _():
            for chunk in range(KV_CHUNKS):
                right2(chunk).wait_send()

        @pl.when(sends_left1)
        def _():
            for slot in range(2):
                for chunk in range(QD_CHUNKS):
                    left1(slot, chunk).wait_send()
                left1_ld(slot).wait_send()

        @pl.when(past_cut)
        def _():
            over_ld().wait_send()
            for chunk in range(QD_CHUNKS):
                over_qd(chunk).wait_send()

        @pl.when(sends_left2 | relays_left2)
        def _():
            for chunk in range(QD_CHUNKS):
                left2(chunk).wait_send()
            left2_ld().wait_send()

        back_dq(0).wait_send()
        back_dq(1).wait_send()
        for part in range(2):
            back_dkv(0, part, 1, guest).wait_recv()

    @pl.when(is_helper)
    def _():
        lax.fori_loop(2 * (flat // head), SHARDS * (flat // head), fill_starts, 0)
        dk_acc[...] = jnp.zeros_like(dk_acc)
        dv_acc[...] = jnp.zeros_like(dv_acc)

        def diagonal(slot, chunk):
            k_tile(slot, 0, (chunk + 1) * span, qd_s.at[slot], ld_s.at[slot], slot, chunk, chunk * span)

        def carry(slot):
            @pl.when(is_carrier)
            def _():
                for chunk in range(KV_CHUNKS):
                    carry1(slot, chunk).wait_recv()
                    carry1(slot, chunk).start()

        carry(0)
        for chunk in range(KV_CHUNKS):
            fwd_kv(res, chunk).wait_recv()
        when(before_cut, *[lambda chunk=chunk: right2(chunk) for chunk in range(KV_CHUNKS)])
        fwd_ld(res).wait_recv()
        for chunk in range(QD_CHUNKS):
            fwd_qd(res, chunk).wait_recv()
            diagonal(res, chunk)
        for chunk in range(QD_CHUNKS):
            when(past_cut | at_cut, lambda: guest_qd(chunk))
        for chunk in range(KV_CHUNKS):
            fwd_kv(gst, chunk).wait_recv()
        fwd_ld(gst).wait_recv()

        def next_queries(slot, chunk):
            left1(slot, chunk).wait_recv()
            k_tile(res, 0, rows, qd_w.at[slot], ld_w.at[slot], slot + 2, chunk)
            k_tile(gst, 0, rows, qd_w.at[slot], ld_w.at[slot], slot + 2, chunk)

        soon_next = jnp.where(at_cut, 1 - next_res, next_res)

        @pl.when(has_next & ~at_cut)
        def _():
            left1_ld(soon_next).wait_recv()

        @pl.when(goes_left1)
        def _():
            over_ld().wait_recv()
            relay_ld1().start()
            relay_ld2().start()
            for chunk in range(QD_CHUNKS):
                over_qd(chunk).wait_recv()
                relay_qd1(chunk).start()
                relay_qd(chunk).start()

        for chunk in range(QD_CHUNKS):
            @pl.when(has_next & ~at_cut)
            def _():
                next_queries(soon_next, chunk)

            fwd_qd(gst, chunk).wait_recv()
            diagonal(gst, chunk)
            k_tile(0, 0, rows, qd_s.at[1], ld_s.at[1], 1, chunk)
            if chunk == 0:
                @pl.when(goes_left2)
                def _():
                    left2_ld(2, helper(mine - 2)).start()
                    for far in range(QD_CHUNKS):
                        left2(far, 2, helper(mine - 2)).start()

        def all_queries(slot):
            left1_ld(slot).wait_recv()

            def one(chunk, _):
                next_queries(slot, chunk)
                return 0

            lax.fori_loop(0, QD_CHUNKS, one, 0)

        @pl.when(at_cut)
        def _():
            all_queries(soon_next)

        late = 1 - soon_next
        is_early = has_next & (gst == 0)

        @pl.when(is_early)
        def _():
            left1_ld(late).wait_recv()
            for chunk in range(QD_CHUNKS):
                left1(late, chunk).wait_recv()
                k_tile(0, chunk * span, rows, qd_w.at[1], ld_w.at[1], 3, chunk)
                if chunk == QD_CHUNKS // 2 - 1:
                    finish_dkv(0, 0)
                k_tile(1, 0, rows, qd_w.at[1], ld_w.at[1], 3, chunk)
                if chunk == QD_CHUNKS // 2 - 1:
                    back_dkv(0, 0, 1, guest).start()

        @pl.when(has_next & ~is_early)
        def _():
            all_queries(late)


        @pl.when(gst == 0)
        def _():
            @pl.when(~is_early)
            def _():
                finish_dkv(0, 0)
                back_dkv(0, 0, 1, guest).start()

            finish_dkv(0, 1)

        for part in range(2):
            @pl.when(has_next2)
            def _():
                if part == 0:
                    left2_ld().wait_recv()
                for chunk in range(part * QD_CHUNKS // 2, (part + 1) * QD_CHUNKS // 2):
                    left2(chunk).wait_recv()
                    k_tile(1, chunk * span, rows, qd_w.at[2], ld_w.at[2], 4, chunk)

            finish_dkv(1, part)

            @pl.when(gst == 1)
            def _():
                finish_dkv(0, part)
                back_dkv(1, part, 1, guest).start()
                back_dkv(0, part, 3, host(pair)).start()

            @pl.when(gst == 0)
            def _():
                if part == 0:
                    back_dkv(0, 1, 1, guest).start()
                back_dkv(1, part, 3, host(pair)).start()

        @pl.when(goes_left1)
        def _():
            relay_ld1().wait_send()
            relay_ld2().wait_send()
            for chunk in range(QD_CHUNKS):
                relay_qd1(chunk).wait_send()
                relay_qd(chunk).wait_send()

        @pl.when(before_cut)
        def _():
            for chunk in range(KV_CHUNKS):
                right2(chunk).wait_send()

        @pl.when(is_carrier)
        def _():
            for chunk in range(KV_CHUNKS):
                for slot in range(2):
                    carry1(slot, chunk).wait_send()
                carry2(chunk).wait_send()

        for chunk in range(KV_CHUNKS):
            guest_kv(chunk).wait_send()
        for chunk in range(QD_CHUNKS):
            guest_qd(chunk).wait_send()
        guest_ld().wait_send()
        for cond, copy in directs():
            @pl.when(cond)
            def _():
                copy.wait_send()

        for part in range(2):
            back_dkv(gst, part, 1, guest).wait_send()
            back_dkv(res, part, 3, host(pair)).wait_send()
            back_dkv(0, part, 1, guest).wait_recv()
        back_dq(0).wait_recv()
        back_dq(1).wait_recv()


def store_kernel(dq_in, dkv_in, dq_hbm, dk_hbm, dv_hbm, sem):
    copies = [pltpu.make_async_copy(source, target, sem.at[index])
              for index, (source, target) in enumerate(((dq_in, dq_hbm), (dkv_in.at[0], dk_hbm), (dkv_in.at[1], dv_hbm)))]
    for copy in copies:
        copy.start()
    for copy in copies:
        copy.wait()


def solution(mesh):
    outer, inner = mesh.shape["cpo"], mesh.shape["cp"]

    def local(queries, keys, values, attn_out, logsumexp, d_out, cu_seqlens):
        rows, heads, head = queries.shape
        flat = rows * heads
        low, full = jnp.bfloat16, jnp.float32
        any_spec = pl.BlockSpec(memory_space=pl.ANY)
        vmem_spec = pl.BlockSpec(memory_space=pltpu.VMEM)
        dma = pltpu.SemaphoreType.DMA
        moves = KV_CHUNKS + QD_CHUNKS + 1
        grads = pl.pallas_call(
            functools.partial(backward_kernel, (outer, inner, rows, heads, head)),
            out_shape=(pltpu.VMEM((flat, head), low), pltpu.VMEM((2, rows, head), low)),
            in_specs=[any_spec] * 7,
            out_specs=(vmem_spec,) * 2,
            scratch_shapes=[
                pltpu.VMEM((3, 2, rows, head), low), pltpu.VMEM((3, 2, rows, head), low),
                pltpu.VMEM((3, 2, flat, head), low), pltpu.VMEM((3, 2, flat, head), low),
                pltpu.VMEM((3, 2, flat), full), pltpu.VMEM((3, 2, flat), full), pltpu.VMEM((2, flat, head), low), pltpu.VMEM((2, flat), full),
                pltpu.VMEM((flat, head), low), pltpu.VMEM((heads, rows), full), pltpu.VMEM((1, cu_seqlens.shape[0]), jnp.int32),
                pltpu.VMEM((SHARDS, 1, flat), full), pltpu.VMEM((3, head, rows), low),
                pltpu.VMEM((2, head, flat), full), pltpu.VMEM((2, rows, head), full), pltpu.VMEM((2, rows, head), full),
                pltpu.VMEM((2, flat, head), low), pltpu.VMEM((2, 2, rows, head), low),
                dma((7,)), dma((moves,)), dma((moves,)), dma((2, moves)), dma((2, moves)),
                dma((3, KV_CHUNKS)), dma((3, KV_CHUNKS)), dma((3, QD_CHUNKS + 1)), dma((3, QD_CHUNKS + 1)), dma((QD_CHUNKS + 1,)), dma((6,)), dma((4,)),
            ],
            compiler_params=pltpu.CompilerParams(collective_id=0, has_side_effects=True),
        )(queries.reshape(flat, head), keys, values, attn_out.reshape(flat, head), d_out.reshape(flat, head),
          logsumexp.T, cu_seqlens.reshape(1, -1))
        d_query, d_key, d_value = pl.pallas_call(
            store_kernel,
            out_shape=(jax.ShapeDtypeStruct((flat, head), low), jax.ShapeDtypeStruct((rows, head), low), jax.ShapeDtypeStruct((rows, head), low)),
            in_specs=[vmem_spec] * 2, out_specs=(any_spec,) * 3, scratch_shapes=[dma((3,))],
        )(*(pltpu.with_memory_space_constraint(grad, pltpu.VMEM) for grad in grads))
        return d_query.reshape(rows, heads, head), d_key, d_value

    seq_spec = P(("dp", "cpo", "cp"))
    return jax.shard_map(local, mesh=mesh, in_specs=(seq_spec,) * 6 + (P("dp"),), out_specs=(seq_spec,) * 3, check_vma=False)
```

```python
import functools
import math

import jax
import jax.numpy as jnp
from jax import lax
from jax.experimental import pallas as pl
from jax.experimental.pallas import tpu as pltpu
from jax.sharding import PartitionSpec as P

MESH = pl.DeviceIdType.MESH
SHARDS = 5
KV_CHUNKS = 2
QD_CHUNKS = 4
LOG2E = math.log2(math.e)
NT = (((1,), (1,)), ((), ()))
NN = (((1,), (0,)), ((), ()))


def dot(lhs, rhs, dims):
    return lax.dot_general(lhs, rhs, dims, preferred_element_type=jnp.float32)


def backward_kernel(sizes, q_hbm, k_hbm, v_hbm, o_hbm, do_hbm, lse_hbm, cu_hbm, dq_out, dkv_out,
                    kv_s, kv_w, qd_s, qd_w, ld_s, ld_w, qd_via, ld_via, o_buf, lse_buf, cu_buf, starts, key_t, dq_t, dk_acc, dv_acc, dq_fin, dkv_fin,
                    load_sem, guest_send, guest_recv, fwd_send, fwd_recv, right_send, right_recv, left_send, left_recv, via_recv, back_send, back_recv):
    outer, inner, rows, heads, head = sizes
    group = outer * inner
    pairs = group // 2
    half = pairs // outer
    scale = head ** -0.5
    flat = rows * heads
    k_part = rows // KV_CHUNKS
    lanes = flat // QD_CHUNKS
    span = rows // QD_CHUNKS
    bounds = cu_buf.shape[1]
    rank = lax.axis_index("cpo") * inner + lax.axis_index("cp")

    def resident(pair):
        return (pair + pair // half + 1) % 2

    def host(pair):
        return 2 * pair + resident(pair)

    def helper(pair):
        return (host(pair) + inner) % group

    def visitor(pair):
        return 2 * pair + 1 - resident(pair)

    is_host = rank % 2 == resident(rank // 2)
    is_helper = rank % 2 != resident(rank // 2)
    pair = jnp.where(is_host, rank // 2, ((rank + inner) % group) // 2)
    res = resident(pair)
    gst = 1 - res
    guest = visitor(pair)
    mine = rank // 2
    side = rank % 2
    own = jnp.where(is_host, res, 2)
    prev_res, next_res = resident(pair - 1), resident(pair + 1)
    has_prev, has_prev2 = pair >= 1, pair >= 2
    has_next, has_next2 = pair + 1 < pairs, pair + 2 < pairs
    my_host = host(mine)

    is_carrier = is_helper & (mine == half - 1)
    goes_left1 = is_helper & (mine == half)
    goes_left2 = is_helper & (mine == half + 1)
    before_cut, at_cut, past_cut, past_cut2 = pair == half - 2, pair == half - 1, pair == half, pair == half + 1

    def device(index):
        return (0, index // inner, index % inner)

    def remote(source, target, send, recv, index):
        return pltpu.make_async_remote_copy(src_ref=source, dst_ref=target, send_sem=send, recv_sem=recv,
                                            device_id=device(index), device_id_type=MESH)

    loads = [
        pltpu.make_async_copy(k_hbm, kv_s.at[own, 0], load_sem.at[0]),
        pltpu.make_async_copy(v_hbm, kv_s.at[own, 1], load_sem.at[1]),
        pltpu.make_async_copy(q_hbm, qd_s.at[own, 0], load_sem.at[2]),
        pltpu.make_async_copy(do_hbm, qd_s.at[own, 1], load_sem.at[3]),
        pltpu.make_async_copy(o_hbm, o_buf, load_sem.at[4]),
        pltpu.make_async_copy(lse_hbm, lse_buf, load_sem.at[5]),
        pltpu.make_async_copy(cu_hbm, cu_buf, load_sem.at[6]),
    ]
    for load in loads:
        load.start()

    barrier = pltpu.get_barrier_semaphore()
    for known, peer in (
        (is_host, guest), (is_helper, host(pair)), (is_helper, my_host), (is_helper, (my_host + inner) % group), (is_host, helper(pair)),
        (is_host & has_prev & ~past_cut, host(pair - 1)), (is_host & has_prev2 & ~past_cut & ~past_cut2, host(pair - 2)),
        (is_helper & has_next & ~at_cut, host(pair + 1)), (is_helper & has_next2 & ~at_cut & ~before_cut, host(pair + 2)),
        (is_host & past_cut, helper(half - 2)), (is_host & (past_cut | past_cut2), visitor(half - 1)),
        (is_helper & at_cut, visitor(half)), (is_helper & at_cut, visitor(half + 1)),
        (is_helper & before_cut, visitor(half)),
    ):
        @pl.when(known)
        def _():
            pl.semaphore_signal(barrier, inc=1, device_id=device(peer), device_id_type=MESH)

    arrivals = jnp.where(is_host, 2, 3)
    for known, count in (
        (is_host & has_next & ~at_cut, 1), (is_host & has_next2 & ~at_cut & ~before_cut, 1),
        (is_host & has_prev & ~past_cut, 1), (is_host & has_prev2 & ~past_cut & ~past_cut2, 1),
        (is_helper & before_cut, 1), (is_carrier, 2), (goes_left1, 2), (goes_left2, 1),
    ):
        arrivals = arrivals + jnp.where(known, count, 0)
    for load in loads:
        load.wait()

    pl.semaphore_wait(barrier, arrivals)

    def kv_rows(chunk):
        return pl.ds(chunk * k_part, k_part)

    def qd_rows(chunk):
        if isinstance(chunk, int):
            return pl.ds(chunk * lanes, lanes)
        return pl.ds(pl.multiple_of(chunk * lanes, lanes), lanes)

    LD = KV_CHUNKS + QD_CHUNKS

    place = jnp.where(is_host, gst, rank % 2)

    def guest_kv(chunk):
        part = kv_rows(chunk)
        return remote(kv_s.at[2, :, part], kv_s.at[place, :, part], guest_send.at[chunk], guest_recv.at[chunk], my_host)

    def guest_qd(chunk):
        part = qd_rows(chunk)
        return remote(qd_s.at[2, :, part], qd_s.at[place, :, part], guest_send.at[KV_CHUNKS + chunk], guest_recv.at[KV_CHUNKS + chunk], my_host)

    def guest_ld():
        return remote(ld_s.at[2], ld_s.at[place], guest_send.at[LD], guest_recv.at[LD], my_host)

    def fwd_kv(slot, chunk):
        part = kv_rows(chunk)
        return remote(kv_s.at[slot, :, part], kv_s.at[slot, :, part], fwd_send.at[slot, chunk], fwd_recv.at[slot, chunk], helper(pair))

    def fwd_qd(slot, chunk):
        part = qd_rows(chunk)
        return remote(qd_s.at[slot, :, part], qd_s.at[slot, :, part], fwd_send.at[slot, KV_CHUNKS + chunk], fwd_recv.at[slot, KV_CHUNKS + chunk], helper(pair))

    def fwd_ld(slot):
        return remote(ld_s.at[slot], ld_s.at[slot], fwd_send.at[slot, LD], fwd_recv.at[slot, LD], helper(pair))

    def right1(slot, chunk):
        part = kv_rows(chunk)
        to = jnp.where(at_cut, guest, host(pair + 1))
        return remote(kv_s.at[slot, :, part], kv_w.at[slot, :, part], right_send.at[slot, chunk], right_recv.at[slot, chunk], to)

    def right2(chunk):
        part = kv_rows(chunk)
        return remote(kv_s.at[1, :, part], kv_w.at[2, :, part], right_send.at[2, chunk], right_recv.at[2, chunk], host(pair + 2))

    def carry1(slot, chunk):
        part = kv_rows(chunk)
        source = kv_s.at[2, :, part] if slot == 1 else kv_w.at[slot, :, part]
        return remote(source, kv_w.at[slot, :, part], right_send.at[slot, chunk], right_recv.at[slot, chunk], host(half))

    def carry2(chunk):
        part = kv_rows(chunk)
        return remote(kv_s.at[2, :, part], kv_w.at[2, :, part], left_send.at[0, chunk], right_recv.at[2, chunk], host(half + 1))

    def left1(slot, chunk, source=None, to=None):
        part = qd_rows(chunk)
        source, to = (slot, helper(pair - 1)) if source is None else (source, to)
        return remote(qd_s.at[source, :, part], qd_w.at[slot, :, part], left_send.at[slot, chunk], left_recv.at[slot, chunk], to)

    def left2(chunk, source=0, to=None):
        part = qd_rows(chunk)
        to = helper(pair - 2) if to is None else to
        return remote(qd_s.at[source, :, part], qd_w.at[2, :, part], left_send.at[2, chunk], left_recv.at[2, chunk], to)

    def left1_ld(slot, source=None, to=None):
        source, to = (slot, helper(pair - 1)) if source is None else (source, to)
        return remote(ld_s.at[source], ld_w.at[slot], left_send.at[slot, QD_CHUNKS], left_recv.at[slot, QD_CHUNKS], to)

    def left2_ld(source=0, to=None):
        to = helper(pair - 2) if to is None else to
        return remote(ld_s.at[source], ld_w.at[2], left_send.at[2, QD_CHUNKS], left_recv.at[2, QD_CHUNKS], to)

    def over_qd(chunk):
        part = qd_rows(chunk)
        return remote(qd_s.at[0, :, part], qd_via.at[:, part], left_send.at[0, chunk], via_recv.at[chunk], visitor(half))

    def over_ld():
        return remote(ld_s.at[0], ld_via, left_send.at[0, QD_CHUNKS], via_recv.at[QD_CHUNKS], visitor(half))

    def relay_qd(chunk):
        part = qd_rows(chunk)
        return remote(qd_via.at[:, part], qd_w.at[2, :, part], left_send.at[0, chunk], left_recv.at[2, chunk], helper(half - 2))

    def relay_qd1(chunk):
        part = qd_rows(chunk)
        return remote(qd_via.at[:, part], qd_w.at[0, :, part], left_send.at[2, chunk], left_recv.at[0, chunk], helper(half - 1))

    def relay_ld1():
        return remote(ld_via, ld_w.at[0], left_send.at[0, QD_CHUNKS], left_recv.at[0, QD_CHUNKS], helper(half - 1))

    def relay_ld2():
        return remote(ld_via, ld_w.at[2], left_send.at[2, QD_CHUNKS], left_recv.at[2, QD_CHUNKS], helper(half - 2))

    def back_dq(part):
        part_rows = pl.ds(part * (flat // 2), flat // 2)
        return remote(dq_fin.at[gst, part_rows], dq_out.at[part_rows], back_send.at[5 * part], back_recv.at[3 * part], guest)

    def back_dkv(slot, part, index, target):
        part_rows = pl.ds(part * (rows // 2), rows // 2)
        return remote(dkv_fin.at[slot, :, part_rows], dkv_out.at[:, part_rows], back_send.at[index + part], back_recv.at[1 + part], target)

    def when(cond, *starts_of):
        @pl.when(cond)
        def _():
            for item in starts_of:
                item().start()

    sends_right1 = is_host & has_next
    sends_right2 = is_host & has_next2 & (res == 1) & ~at_cut & ~before_cut
    sends_left1 = is_host & has_prev & ~past_cut
    sends_left2 = is_host & has_prev2 & (res == 0) & ~past_cut & ~past_cut2
    waits_left2 = (pair // half) % 2 == res
    for chunk in range(KV_CHUNKS):
        when(is_helper, lambda: guest_kv(chunk))
        when(sends_right1, lambda: right1(res, chunk))
        when(is_host, lambda: fwd_kv(res, chunk))
        when(sends_right2, lambda: right2(chunk))
    when(is_carrier, *[lambda chunk=chunk: carry1(1, chunk) for chunk in range(KV_CHUNKS)])
    row_id = lax.broadcasted_iota(jnp.int32, (head, heads * head), 0)
    lane_id = lax.broadcasted_iota(jnp.int32, (head, heads * head), 1)
    for part in range(rows // head):
        piece = slice(part * head, (part + 1) * head)
        wide = jnp.zeros((head, heads * head), jnp.float32)
        for g in range(heads):
            column_g = jnp.broadcast_to(lse_buf[g:g + 1, piece], (head, head)).T
            wide = jnp.where(lane_id == row_id * heads + g, jnp.concatenate([column_g] * heads, axis=1), wide)
        ld_s[own, 0:1, part * heads * head:(part + 1) * heads * head] = jnp.sum(wide, axis=0, keepdims=True) * LOG2E
    for part in range(flat // head):
        piece = slice(part * head, (part + 1) * head)
        prod = qd_s[own, 1, piece, :].astype(jnp.float32) * o_buf[piece, :].astype(jnp.float32)
        ld_s[own, 1:2, piece] = jnp.sum(prod.T, axis=0, keepdims=True)

    when(is_helper, guest_ld)
    when(is_host, lambda: fwd_ld(res))
    when(sends_left1, lambda: left1_ld(res))
    when(sends_left2, left2_ld)
    for chunk in range(QD_CHUNKS):
        when(is_helper & ~past_cut & ~at_cut, lambda: guest_qd(chunk))
        when(sends_left1, lambda: left1(res, chunk))
        when(is_host, lambda: fwd_qd(res, chunk))
        when(sends_left2 if chunk < QD_CHUNKS // 2 else sends_left2 & ~waits_left2, lambda: left2(chunk))
    when(is_carrier, *[lambda chunk=chunk: carry2(chunk) for chunk in range(KV_CHUNKS)])
    when(is_host & past_cut, over_ld, *[lambda chunk=chunk: over_qd(chunk) for chunk in range(QD_CHUNKS)])

    first = (pair * (2 * rows)).astype(jnp.float32)
    cuts = cu_buf[...].astype(jnp.float32)
    cut_cols = []
    for base in range(0, bounds, head):
        width = min(head, bounds - base)
        row = cuts[:, base:base + width]
        if width < head:
            row = jnp.concatenate([row, jnp.zeros((1, head - width), jnp.float32)], axis=1)
        cut_cols.append(jnp.broadcast_to(row, (head, head)).T - first)
    lane = lax.broadcasted_iota(jnp.int32, (1, head), 1)

    def fill_starts(step, _):
        lane_base = pl.multiple_of((step % (flat // head)) * head, head)
        shard = step // (flat // head)
        token = ((lane + lane_base) // heads + shard * rows).astype(jnp.float32)
        best = jnp.full((head, head), -1e9, jnp.float32)
        for col in cut_cols:
            best = jnp.maximum(best, jnp.where(col <= token, col, -1e9))
        starts[shard, :, pl.ds(lane_base, head)] = jnp.max(best, axis=0, keepdims=True)
        return 0

    lax.fori_loop(0, 2 * (flat // head), fill_starts, 0)

    def directs():
        out = [(goes_left1, left1_ld(side, 2, helper(mine - 1))), (goes_left2, left2_ld(2, helper(mine - 2)))]
        for chunk in range(QD_CHUNKS):
            out.append((goes_left1, left1(side, chunk, 2, helper(mine - 1))))
            out.append((goes_left2, left2(chunk, 2, helper(mine - 2))))
        return out

    @pl.when(goes_left1)
    def _():
        left1_ld(side, 2, helper(mine - 1)).start()
        for chunk in range(QD_CHUNKS):
            left1(side, chunk, 2, helper(mine - 1)).start()

    def scores(kv, key_rows, key_off, qd, ld, part, start, token_off):
        keys, vals = kv[0, key_rows, :], kv[1, key_rows, :]
        qry, dout = qd[0, part, :], qd[1, part, :]
        score = dot(keys, qry, NT)
        grad = dot(vals, dout, NT)
        lse, row_dot = ld[0:1, part], ld[1:2, part]
        key_pos = lax.broadcasted_iota(jnp.int32, score.shape, 0).astype(jnp.float32)
        keep = key_pos >= start[:, part] - key_off
        if token_off is not None:
            token = lax.broadcasted_iota(jnp.int32, (1, lanes), 1) // heads + token_off
            keep = keep & (key_pos <= token.astype(jnp.float32))
        prob = jnp.where(keep, jnp.exp2(score * (scale * LOG2E) - lse), 0.0)
        dsc = (prob * (grad - row_dot)).astype(jnp.bfloat16)
        return prob, dsc, qry, dout

    def q_tile(kv, key_slot, k_from, k_to, key_off, q_slot, chunk, token_off=None):
        part, key_rows = qd_rows(chunk), pl.ds(k_from, k_to - k_from)
        _, dsc, _, _ = scores(kv, key_rows, key_off + k_from, qd_s.at[q_slot], ld_s.at[q_slot], part, starts.at[q_slot], token_off)
        dq_t[q_slot, :, part] += dot(key_t[key_slot, :, k_from:k_to], dsc, NN)

    def k_tile(k_slot, k_from, k_to, qd, ld, q_shard, chunk, token_off=None):
        part, key_rows = qd_rows(chunk), pl.ds(k_from, k_to - k_from)
        key_off = (k_slot * rows + k_from) * 1.0
        prob, dsc, qry, dout = scores(kv_s.at[k_slot], key_rows, key_off, qd, ld, part, starts.at[q_shard], token_off)
        dv_acc[k_slot, key_rows, :] += dot(prob.astype(jnp.bfloat16), dout, NN)
        dk_acc[k_slot, key_rows, :] += dot(dsc, qry, NN)

    def finish_dq(slot, target, half_rows):
        for part in range(half_rows * flat // head // 2, (half_rows + 1) * flat // head // 2):
            piece = slice(part * head, (part + 1) * head)
            target[piece, :] = (scale * dq_t[slot, :, piece].T).astype(jnp.bfloat16)

    def finish_dkv(slot, part):
        part_rows = slice(part * (rows // 2), (part + 1) * (rows // 2))
        dkv_fin[slot, 0, part_rows, :] = (scale * dk_acc[slot, part_rows, :]).astype(jnp.bfloat16)
        dkv_fin[slot, 1, part_rows, :] = dv_acc[slot, part_rows, :].astype(jnp.bfloat16)

    @pl.when(is_host)
    def _():
        dq_t[...] = jnp.zeros_like(dq_t)

        relays_right1 = has_next & ~at_cut
        relays_right2 = has_next2 & (gst == 1) & ~at_cut
        relays_left1 = has_prev & ~past_cut
        relays_left2 = has_prev2 & (gst == 0) & ~past_cut & ~past_cut2

        def diagonal(slot, chunk):
            q_tile(kv_s.at[slot], slot, 0, (chunk + 1) * span, slot * rows * 1.0, slot, chunk, chunk * span)

        key_t[res] = kv_s[res, 0, :, :].T
        for chunk in range(QD_CHUNKS):
            diagonal(res, chunk)
        for chunk in range(KV_CHUNKS):
            guest_kv(chunk).wait_recv()
            fwd_kv(gst, chunk).start()
            when(relays_right2, lambda: right2(chunk))
            when(relays_right1, lambda: right1(gst, chunk))
        guest_ld().wait_recv()
        fwd_ld(gst).start()
        when(relays_left1, lambda: left1_ld(gst))
        when(relays_left2, left2_ld)
        key_t[gst] = kv_s[gst, 0, :, :].T
        soon = jnp.where(past_cut, 1 - prev_res, prev_res)
        prev_off = (soon - 2) * rows * 1.0
        late_off = (-1 - soon) * rows * 1.0

        def early_keys():
            for chunk in range(KV_CHUNKS):
                right1(soon, chunk).wait_recv()
            key_t[2] = kv_w[soon, 0, :, :].T

        def early_tiles(chunk):
            q_tile(kv_w.at[soon], 2, 0, rows, prev_off, res, chunk)
            q_tile(kv_w.at[soon], 2, 0, rows, prev_off, gst, chunk)

        for chunk in range(QD_CHUNKS):
            guest_qd(chunk).wait_recv()
            when(relays_left1, lambda: left1(gst, chunk))
            fwd_qd(gst, chunk).start()
            when(relays_left2 & ~waits_left2, lambda: left2(chunk))
            if chunk >= QD_CHUNKS // 2:
                when(relays_left2 & waits_left2, lambda: left2(chunk - QD_CHUNKS // 2))
                when(sends_left2 & waits_left2, lambda: left2(chunk))
            diagonal(gst, chunk)
            q_tile(kv_s.at[0], 0, 0, rows, 0.0, 1, chunk)

            @pl.when(has_prev & ~past_cut)
            def _():
                if chunk == 0:
                    early_keys()
                early_tiles(chunk)

        @pl.when(past_cut)
        def _():
            early_keys()

            for chunk in range(QD_CHUNKS):
                q_tile(kv_w.at[soon], 2, 0, rows, prev_off, gst, chunk)

        for chunk in range(QD_CHUNKS // 2, QD_CHUNKS):
            when(relays_left2 & waits_left2, lambda: left2(chunk))

        def far_keys():
            for chunk in range(KV_CHUNKS):
                right2(chunk).wait_recv()
            key_t[2] = kv_w[2, 0, :, :].T
            for chunk in range(QD_CHUNKS):
                q_tile(kv_w.at[2], 2, chunk * span, rows, -3.0 * rows, 0, chunk)

        @pl.when(has_prev2 & ~past_cut)
        def _():
            far_keys()

        def late_keys(slot, part, step, cond=True):
            @pl.when(has_prev & cond)
            def _():
                for index in range(2):
                    q_tile(kv_w.at[1 - soon], 2, part * k_part, (part + 1) * k_part, late_off, slot, 2 * step + index)

        for chunk in range(KV_CHUNKS):
            @pl.when(has_prev)
            def _():
                right1(1 - soon, chunk).wait_recv()
                key_t[2, :, chunk * k_part:(chunk + 1) * k_part] = kv_w[1 - soon, 0, chunk * k_part:(chunk + 1) * k_part, :].T

            last = chunk == KV_CHUNKS - 1
            late_keys(gst, chunk, 0)
            if last:
                finish_dq(gst, dq_fin.at[gst], 0)
            late_keys(gst, chunk, 1)
            if last:
                back_dq(0).start()
                finish_dq(gst, dq_fin.at[gst], 1)
            late_keys(res, chunk, 0, last | ~past_cut)
            if last:
                back_dq(1).start()
            late_keys(res, chunk, 1, last | ~past_cut)

        @pl.when(past_cut)
        def _():
            late_keys(res, 0, 0)
            late_keys(res, 0, 1)
            key_t[2] = kv_w[soon, 0, :, :].T
            for chunk in range(QD_CHUNKS):
                q_tile(kv_w.at[soon], 2, 0, rows, prev_off, res, chunk)
            far_keys()

        finish_dq(res, dq_out, 0)
        finish_dq(res, dq_out, 1)

        for chunk in range(KV_CHUNKS):
            fwd_kv(res, chunk).wait_send()
            fwd_kv(gst, chunk).wait_send()
        for chunk in range(QD_CHUNKS):
            fwd_qd(res, chunk).wait_send()
            fwd_qd(gst, chunk).wait_send()
        fwd_ld(res).wait_send()
        fwd_ld(gst).wait_send()

        @pl.when(has_next)
        def _():
            for chunk in range(KV_CHUNKS):
                right1(res, chunk).wait_send()

        @pl.when(relays_right1)
        def _():
            for chunk in range(KV_CHUNKS):
                right1(gst, chunk).wait_send()

        @pl.when(sends_right2 | relays_right2)
        def _():
            for chunk in range(KV_CHUNKS):
                right2(chunk).wait_send()

        @pl.when(sends_left1)
        def _():
            for slot in range(2):
                for chunk in range(QD_CHUNKS):
                    left1(slot, chunk).wait_send()
                left1_ld(slot).wait_send()

        @pl.when(past_cut)
        def _():
            over_ld().wait_send()
            for chunk in range(QD_CHUNKS):
                over_qd(chunk).wait_send()

        @pl.when(sends_left2 | relays_left2)
        def _():
            for chunk in range(QD_CHUNKS):
                left2(chunk).wait_send()
            left2_ld().wait_send()

        back_dq(0).wait_send()
        back_dq(1).wait_send()
        for part in range(2):
            back_dkv(0, part, 1, guest).wait_recv()

    @pl.when(is_helper)
    def _():
        lax.fori_loop(2 * (flat // head), SHARDS * (flat // head), fill_starts, 0)
        dk_acc[...] = jnp.zeros_like(dk_acc)
        dv_acc[...] = jnp.zeros_like(dv_acc)

        def diagonal(slot, chunk):
            k_tile(slot, 0, (chunk + 1) * span, qd_s.at[slot], ld_s.at[slot], slot, chunk, chunk * span)

        def carry(slot):
            @pl.when(is_carrier)
            def _():
                for chunk in range(KV_CHUNKS):
                    carry1(slot, chunk).wait_recv()
                    carry1(slot, chunk).start()

        carry(0)
        for chunk in range(KV_CHUNKS):
            fwd_kv(res, chunk).wait_recv()
        when(before_cut, *[lambda chunk=chunk: right2(chunk) for chunk in range(KV_CHUNKS)])
        fwd_ld(res).wait_recv()
        for chunk in range(QD_CHUNKS):
            fwd_qd(res, chunk).wait_recv()
            diagonal(res, chunk)
        for chunk in range(QD_CHUNKS):
            when(past_cut | at_cut, lambda: guest_qd(chunk))
        for chunk in range(KV_CHUNKS):
            fwd_kv(gst, chunk).wait_recv()
        fwd_ld(gst).wait_recv()

        def next_queries(slot, chunk):
            left1(slot, chunk).wait_recv()
            k_tile(res, 0, rows, qd_w.at[slot], ld_w.at[slot], slot + 2, chunk)
            k_tile(gst, 0, rows, qd_w.at[slot], ld_w.at[slot], slot + 2, chunk)

        soon_next = jnp.where(at_cut, 1 - next_res, next_res)

        @pl.when(has_next & ~at_cut)
        def _():
            left1_ld(soon_next).wait_recv()

        @pl.when(goes_left1)
        def _():
            over_ld().wait_recv()
            relay_ld1().start()
            relay_ld2().start()
            for chunk in range(QD_CHUNKS):
                over_qd(chunk).wait_recv()
                relay_qd1(chunk).start()
                relay_qd(chunk).start()

        for chunk in range(QD_CHUNKS):
            @pl.when(has_next & ~at_cut)
            def _():
                next_queries(soon_next, chunk)

            fwd_qd(gst, chunk).wait_recv()
            diagonal(gst, chunk)
            k_tile(0, 0, rows, qd_s.at[1], ld_s.at[1], 1, chunk)
            if chunk == 0:
                @pl.when(goes_left2)
                def _():
                    left2_ld(2, helper(mine - 2)).start()
                    for far in range(QD_CHUNKS):
                        left2(far, 2, helper(mine - 2)).start()

        def all_queries(slot):
            left1_ld(slot).wait_recv()

            def one(chunk, _):
                next_queries(slot, chunk)
                return 0

            lax.fori_loop(0, QD_CHUNKS, one, 0)

        @pl.when(at_cut)
        def _():
            all_queries(soon_next)

        late = 1 - soon_next
        is_early = has_next & (gst == 0)

        @pl.when(is_early)
        def _():
            left1_ld(late).wait_recv()
            for chunk in range(QD_CHUNKS):
                left1(late, chunk).wait_recv()
                k_tile(0, chunk * span, rows, qd_w.at[1], ld_w.at[1], 3, chunk)
                if chunk == QD_CHUNKS // 2 - 1:
                    finish_dkv(0, 0)
                k_tile(1, 0, rows, qd_w.at[1], ld_w.at[1], 3, chunk)
                if chunk == QD_CHUNKS // 2 - 1:
                    back_dkv(0, 0, 1, guest).start()

        @pl.when(has_next & ~is_early)
        def _():
            all_queries(late)


        @pl.when(gst == 0)
        def _():
            @pl.when(~is_early)
            def _():
                finish_dkv(0, 0)
                back_dkv(0, 0, 1, guest).start()

            finish_dkv(0, 1)

        for part in range(2):
            @pl.when(has_next2)
            def _():
                if part == 0:
                    left2_ld().wait_recv()
                for chunk in range(part * QD_CHUNKS // 2, (part + 1) * QD_CHUNKS // 2):
                    left2(chunk).wait_recv()
                    k_tile(1, chunk * span, rows, qd_w.at[2], ld_w.at[2], 4, chunk)

            finish_dkv(1, part)

            @pl.when(gst == 1)
            def _():
                finish_dkv(0, part)
                back_dkv(1, part, 1, guest).start()
                back_dkv(0, part, 3, host(pair)).start()

            @pl.when(gst == 0)
            def _():
                if part == 0:
                    back_dkv(0, 1, 1, guest).start()
                back_dkv(1, part, 3, host(pair)).start()

        @pl.when(goes_left1)
        def _():
            relay_ld1().wait_send()
            relay_ld2().wait_send()
            for chunk in range(QD_CHUNKS):
                relay_qd1(chunk).wait_send()
                relay_qd(chunk).wait_send()

        @pl.when(before_cut)
        def _():
            for chunk in range(KV_CHUNKS):
                right2(chunk).wait_send()

        @pl.when(is_carrier)
        def _():
            for chunk in range(KV_CHUNKS):
                for slot in range(2):
                    carry1(slot, chunk).wait_send()
                carry2(chunk).wait_send()

        for chunk in range(KV_CHUNKS):
            guest_kv(chunk).wait_send()
        for chunk in range(QD_CHUNKS):
            guest_qd(chunk).wait_send()
        guest_ld().wait_send()
        for cond, copy in directs():
            @pl.when(cond)
            def _():
                copy.wait_send()

        for part in range(2):
            back_dkv(gst, part, 1, guest).wait_send()
            back_dkv(res, part, 3, host(pair)).wait_send()
            back_dkv(0, part, 1, guest).wait_recv()
        back_dq(0).wait_recv()
        back_dq(1).wait_recv()


def store_kernel(dq_in, dkv_in, dq_hbm, dk_hbm, dv_hbm, sem):
    copies = [pltpu.make_async_copy(source, target, sem.at[index])
              for index, (source, target) in enumerate(((dq_in, dq_hbm), (dkv_in.at[0], dk_hbm), (dkv_in.at[1], dv_hbm)))]
    for copy in copies:
        copy.start()
    for copy in copies:
        copy.wait()


def solution(mesh):
    outer, inner = mesh.shape["cpo"], mesh.shape["cp"]

    def local(queries, keys, values, attn_out, logsumexp, d_out, cu_seqlens):
        rows, heads, head = queries.shape
        flat = rows * heads
        low, full = jnp.bfloat16, jnp.float32
        any_spec = pl.BlockSpec(memory_space=pl.ANY)
        vmem_spec = pl.BlockSpec(memory_space=pltpu.VMEM)
        dma = pltpu.SemaphoreType.DMA
        moves = KV_CHUNKS + QD_CHUNKS + 1
        grads = pl.pallas_call(
            functools.partial(backward_kernel, (outer, inner, rows, heads, head)),
            out_shape=(pltpu.VMEM((flat, head), low), pltpu.VMEM((2, rows, head), low)),
            in_specs=[any_spec] * 7,
            out_specs=(vmem_spec,) * 2,
            scratch_shapes=[
                pltpu.VMEM((3, 2, rows, head), low), pltpu.VMEM((3, 2, rows, head), low),
                pltpu.VMEM((3, 2, flat, head), low), pltpu.VMEM((3, 2, flat, head), low),
                pltpu.VMEM((3, 2, flat), full), pltpu.VMEM((3, 2, flat), full), pltpu.VMEM((2, flat, head), low), pltpu.VMEM((2, flat), full),
                pltpu.VMEM((flat, head), low), pltpu.VMEM((heads, rows), full), pltpu.VMEM((1, cu_seqlens.shape[0]), jnp.int32),
                pltpu.VMEM((SHARDS, 1, flat), full), pltpu.VMEM((3, head, rows), low),
                pltpu.VMEM((2, head, flat), full), pltpu.VMEM((2, rows, head), full), pltpu.VMEM((2, rows, head), full),
                pltpu.VMEM((2, flat, head), low), pltpu.VMEM((2, 2, rows, head), low),
                dma((7,)), dma((moves,)), dma((moves,)), dma((2, moves)), dma((2, moves)),
                dma((3, KV_CHUNKS)), dma((3, KV_CHUNKS)), dma((3, QD_CHUNKS + 1)), dma((3, QD_CHUNKS + 1)), dma((QD_CHUNKS + 1,)), dma((6,)), dma((4,)),
            ],
            compiler_params=pltpu.CompilerParams(collective_id=0, has_side_effects=True),
        )(queries.reshape(flat, head), keys, values, attn_out.reshape(flat, head), d_out.reshape(flat, head),
          logsumexp.T, cu_seqlens.reshape(1, -1))
        d_query, d_key, d_value = pl.pallas_call(
            store_kernel,
            out_shape=(jax.ShapeDtypeStruct((flat, head), low), jax.ShapeDtypeStruct((rows, head), low), jax.ShapeDtypeStruct((rows, head), low)),
            in_specs=[vmem_spec] * 2, out_specs=(any_spec,) * 3, scratch_shapes=[dma((3,))],
        )(*(pltpu.with_memory_space_constraint(grad, pltpu.VMEM) for grad in grads))
        return d_query.reshape(rows, heads, head), d_key, d_value

    seq_spec = P(("dp", "cpo", "cp"))
    return jax.shard_map(local, mesh=mesh, in_specs=(seq_spec,) * 6 + (P("dp"),), out_specs=(seq_spec,) * 3, check_vma=False)
```
